32 devices in a mesh: dp: 4 (over x, y), tp: 8 (over z, core).
Axes of the slice: x: 2, y: 2, z: 4, core: 2. Of those that a mesh axis runs over, the one named last changes fastest.
Arguments:
- x: bfloat16 [8192, 7168], P('dp'), parts along dimension 0
- gain: bfloat16 [7168], replicated
- wq: bfloat16 [7168, 7168], P(None, 'tp')
- wk: bfloat16 [7168, 7168], P(None, 'tp')
- wv: bfloat16 [7168, 7168], P(None, 'tp')
- wo: bfloat16 [7168, 7168], P('tp')
Outputs:
- output: bfloat16 [8192, 7168], P('dp'), parts along dimension 0
There are 4 independent parts. The reference program is written for one: setup_inputs(seed, part) draws one part's arguments, and reference() takes and returns one part's arrays. A program takes and returns all parts, laid end to end along the dimension named above; an argument that names none is the same for every part.
All inputs are finite; a program needn't handle non-finite values.
Results may differ from the reference program's by a relative error of at most 0.012.
Values are sent between devices in bfloat16 or wider.
A program may use at most 2 GiB of HBM per device.

```python
import jax
import jax.numpy as jnp
from jax import lax

ROWS = 2048
D = 7168
HEADS = 56
KV_HEADS = 56
HEAD = 128
THETA = 10000


def setup_inputs(seed: int = 0, part: int = 0) -> dict:
    kx, kn, kq, kk, kv, ko = jax.random.split(jax.random.key(seed), 6)

    def weights(key, rows, columns):
        return jax.random.normal(key, (rows, columns), jnp.float32) * rows**-0.5

    drawn = {
        "x": jax.random.normal(jax.random.fold_in(kx, part), (ROWS, D), jnp.float32),
        "gain": 1 + 0.1 * jax.random.normal(kn, (D,), jnp.float32),
        "wq": 2 * weights(kq, D, HEADS * HEAD),
        "wk": 2 * weights(kk, D, KV_HEADS * HEAD),
        "wv": 4 * weights(kv, D, KV_HEADS * HEAD),
        "wo": weights(ko, HEADS * HEAD, D),
    }
    return {k: v.astype(jnp.bfloat16) for k, v in drawn.items()}


def normed(x, gain):
    wide = x.astype(jnp.float32)
    scale = lax.rsqrt(jnp.mean(wide * wide, -1, keepdims=True) + 1e-6)
    return (wide * scale * gain.astype(jnp.float32)).astype(jnp.bfloat16)


def turned(t, place, theta):
    half = t.shape[-1] // 2
    angle = place.astype(jnp.float32)[:, None] * theta ** (-jnp.arange(half, dtype=jnp.float32) / half)
    cos, sin = jnp.cos(angle)[:, None], jnp.sin(angle)[:, None]
    a, b = t[..., :half].astype(jnp.float32), t[..., half:].astype(jnp.float32)
    return jnp.concatenate([a * cos - b * sin, b * cos + a * sin], -1).astype(jnp.bfloat16)


def matmul(a, w):
    return jnp.dot(a, w, preferred_element_type=jnp.float32).astype(jnp.bfloat16)


def einsum(form, a, b):
    return jnp.einsum(form, a.astype(jnp.float32), b.astype(jnp.float32))


def attention(q, k, v):
    scores = einsum("tgsd,ugd->gstu", q, k) * q.shape[-1] ** -0.5
    token = jnp.arange(q.shape[0])
    scores = jnp.where(token[:, None] >= token, scores, -jnp.inf)
    weights = jax.nn.softmax(scores, -1).astype(jnp.bfloat16)
    return einsum("gstu,ugd->tgsd", weights, v).astype(jnp.bfloat16)


def reference(x, gain, wq, wk, wv, wo):
    a, place = normed(x, gain), jnp.arange(ROWS)
    q = turned(matmul(a, wq).reshape(ROWS, HEADS, HEAD), place, THETA).reshape(ROWS, KV_HEADS, -1, HEAD)
    k = turned(matmul(a, wk).reshape(ROWS, KV_HEADS, HEAD), place, THETA)
    v = matmul(a, wv).reshape(ROWS, KV_HEADS, HEAD)
    seen = attention(q, k, v).reshape(ROWS, HEADS * HEAD)
    return (x.astype(jnp.float32) + jnp.dot(seen, wo, preferred_element_type=jnp.float32)).astype(jnp.bfloat16)
```

```python
import functools

import jax
import jax.numpy as jnp
import numpy as np
from jax import lax
from jax.experimental import pallas as pl
from jax.experimental.pallas import tpu as pltpu
from jax.sharding import PartitionSpec as P

HEAD = 128
THETA = 10000
LOG2E = 1.4426950408889634
HIDDEN = -2e30
MESH = pl.DeviceIdType.MESH
BF16, F32 = jnp.bfloat16, jnp.float32


def _dot(a, b, ca, cb):
    return lax.dot_general(a, b, (((ca,), (cb,)), ((), ())), preferred_element_type=F32)


def _kernel(cfg, x_hbm, gain_ref, base_ref, fine_ref, wq_hbm, wk_hbm, wv_hbm, wo_hbm, y_hbm,
            keys, vals, wo, wbuf, xbuf, abuf, acc, stage, seen, d2d, up, dn, sendb, xres, rotc, rots,
            w_sem, wo_sem, x_sem, xres_sem, d2d_send, d2d_recv, up_recv, dn_recv, res_recv,
            send_a, send_b, send_c, send_l, fwd_send, part_send, part_recv):
    ch, sub, heads, nc, half, zs, tile, names = (cfg[k] for k in ("ch", "sub", "heads", "nc", "half", "zs", "tile", "names"))
    per = heads + 1
    pieces = nc * per
    e = HEAD**-0.5 * LOG2E
    lag1, lag2, lag3, lag4, lag5 = per, per + 2, per + 4, per + 6, per + 8
    ring, nb = up.shape[0], sendb.shape[0]

    dpi, t = lax.axis_index(names[0]), lax.axis_index(names[1])
    core, z = lax.rem(t, 2), lax.div(t, 2)
    p = jnp.where(core == 0, z, zs - 1 - z)
    step = 2 - 4 * core
    partner, upper, lower = (dpi, t + 1 - 2 * core), (dpi, t + step), (dpi, t - step)
    mine = pl.multiple_of(core * half, 128)
    other = pl.multiple_of((1 - core) * half, 128)

    def rows(s):
        return pl.ds(pl.multiple_of(s * sub, sub), sub)

    def finished(s):
        return y_hbm.at[rows(s), pl.ds(mine, half)]

    def remote(src, dst, send, recv, device):
        return pltpu.make_async_remote_copy(src_ref=src, dst_ref=dst, send_sem=send, recv_sem=recv, device_id=device, device_id_type=MESH)

    def x_copy(i):
        return pltpu.make_async_copy(x_hbm.at[pl.ds(pl.multiple_of(i * ch, ch), ch), :], xbuf, x_sem)

    def w_copies(n):
        h, par = lax.rem(n, heads), lax.rem(n, 2)
        cols = pl.ds(pl.multiple_of(h * HEAD, HEAD), HEAD)
        return [
            pltpu.make_async_copy(w.at[:, cols], wbuf.at[par, :, m * HEAD : (m + 1) * HEAD], w_sem.at[par, m])
            for m, w in enumerate((wq_hbm, wk_hbm, wv_hbm))
        ]

    def wo_copy(h):
        part = pl.ds(pl.multiple_of(h * HEAD, HEAD), HEAD)
        return pltpu.make_async_copy(wo_hbm.at[part, :], wo.at[part, :], wo_sem.at[h])

    def xres_copy(s):
        b = lax.rem(s, nb)
        return pltpu.make_async_copy(x_hbm.at[rows(s), pl.ds(mine, half)], xres.at[b], xres_sem.at[b])

    def d2d_copy(c, k):
        at = lax.rem(c, 2) * per + k
        return remote(stage.at[k], d2d.at[at], d2d_send.at[k], d2d_recv.at[at], partner)

    def term_copy(s, to, ref, recv):
        b, r = lax.rem(s, nb), lax.rem(s, ring)
        return remote(sendb.at[b], ref.at[r], send_a.at[b], recv.at[r], to)

    def root_copies(s):
        b, r = lax.rem(s, nb), lax.rem(s, ring)
        return [
            remote(sendb.at[b], finished(s), send_a.at[b], res_recv.at[r], lower),
            remote(sendb.at[b], finished(s), send_b.at[b], res_recv.at[r], upper),
            remote(sendb.at[b], finished(s), send_c.at[b], part_recv, partner),
        ]

    def root_local(s):
        b = lax.rem(s, nb)
        return pltpu.make_async_copy(sendb.at[b], finished(s), send_l.at[b])

    def forward_copy(s):
        return remote(finished(s), finished(s), fwd_send, res_recv.at[lax.rem(s, ring)], upper)

    def part_copy(s):
        return remote(finished(s), finished(s), part_send, part_recv, partner)

    def norm(i):
        bc, bs = base_ref[0, pl.ds(i, 1), :], base_ref[1, pl.ds(i, 1), :]
        rotc[...] = bc * fine_ref[0] - bs * fine_ref[1]
        rots[...] = bs * fine_ref[0] + bc * fine_ref[1]

        def group(r, _):
            at = pl.ds(pl.multiple_of(r * 16, 16), 16)
            wide = xbuf[at, :].astype(F32)
            scale = lax.rsqrt(jnp.mean(wide * wide, -1, keepdims=True) + 1e-6)
            abuf[at, :] = (wide * scale * gain_ref[...]).astype(BF16)

        lax.fori_loop(0, ch // 16, group, None)

    def turned(v):
        v = v.astype(BF16).astype(F32)
        return (v * rotc[...] + pltpu.roll(v, HEAD // 2, 1) * rots[...]).astype(BF16)

    def head(i, h):
        n = i * heads + h

        @pl.when(n + 1 < nc * heads)
        def _():
            for copy in w_copies(n + 1):
                copy.start()

        @pl.when(i == 0)
        def _():
            wo_copy(h).start()

        @pl.when((h == 0) & (i + 1 < nc))
        def _():
            x_copy(i + 1).start()

        for copy in w_copies(n):
            copy.wait()
        qkv = _dot(abuf[...], wbuf[lax.rem(n, 2)], 1, 0)
        here = pl.ds(pl.multiple_of(i * ch, ch), ch)
        q = turned(qkv[:, :HEAD])
        keys[h, here, :] = turned(qkv[:, HEAD : 2 * HEAD])
        vals[h, :HEAD, here] = qkv[:, 2 * HEAD :].astype(BF16).T
        wide = 2 * ch

        def block(jb, masked):
            at = pl.ds(pl.multiple_of(jb * wide, wide), wide)
            s = _dot(keys[h, at, :], q, 1, 1)
            if masked:
                query = i * ch + lax.broadcasted_iota(jnp.int32, (wide, ch), 1)
                key = jb * wide + lax.broadcasted_iota(jnp.int32, (wide, ch), 0)
                s = jnp.where(key <= query, s, HIDDEN)
            return s, s.max(axis=0, keepdims=True), vals[h, :, at]

        last = lax.div(i, 2)
        s, top, values = block(last, True)
        mix = _dot(values, jnp.exp2((s - top) * e).astype(BF16), 1, 0)

        def whole(jb, carry):
            old, mix = carry
            s, top, values = block(jb, False)
            top = jnp.maximum(old, top)
            weights = jnp.exp2((s - top) * e).astype(BF16)
            return top, mix * jnp.exp2((old - top) * e) + _dot(values, weights, 1, 0)

        top, mix = lax.fori_loop(0, last, whole, (top, mix))
        out = mix[:HEAD] * (1 / mix[HEAD : HEAD + 1])
        seen[:, pl.ds(pl.multiple_of(h * HEAD, HEAD), HEAD)] = out.T.astype(BF16)

    def project(i):
        @pl.when(i == 0)
        def _():
            for h in range(heads):
                wo_copy(h).wait()

        @pl.when(i > 0)
        def _():
            for k in range(per):
                d2d_copy(i - 1, k).wait_send()

        def theirs(n, _):
            at = pl.multiple_of(n * tile, tile)
            part = _dot(seen[...], wo[:, pl.ds(pl.multiple_of(other + at, 128), tile)], 1, 0)
            stage[:, :, pl.ds(at, tile)] = part.astype(BF16).reshape(per, sub, tile)

        def ours(n, _):
            at = pl.multiple_of(n * tile, tile)
            part = _dot(seen[...], wo[:, pl.ds(pl.multiple_of(mine + at, 128), tile)], 1, 0)
            acc[lax.rem(i, 2), :, :, pl.ds(at, tile)] = part.reshape(per, sub, tile)

        lax.fori_loop(0, half // tile, theirs, None)
        for k in range(per):
            d2d_copy(i, k).start()
        lax.fori_loop(0, half // tile, ours, None)

        @pl.when(i + 1 < nc)
        def _():
            x_copy(i + 1).wait()
            norm(i + 1)

    def valid(s):
        return (s >= 0) & (s < pieces)

    def sum_of(s):
        return acc.at[lax.rem(lax.div(s, per), 2), lax.rem(s, per)]

    def pair(s):
        at = lax.rem(s, 2 * per)
        d2d_copy(lax.div(s, per), lax.rem(s, per)).wait_recv()
        ours = sum_of(s)

        @pl.when((p == 1) | (p == 2))
        def _():
            ours[...] = ours[...] + d2d[at].astype(F32)

        @pl.when((p == 0) | (p == 3))
        def _():
            @pl.when(s >= nb)
            def _():
                term_copy(s - nb, lower, up, up_recv).wait_send()

            sendb[lax.rem(s, nb)] = (ours[...] + d2d[at].astype(F32)).astype(BF16)

        @pl.when(p == 3)
        def _():
            term_copy(s, lower, up, up_recv).start()

        @pl.when(p == 0)
        def _():
            term_copy(s, upper, dn, dn_recv).start()

    def relay(s):
        copy = term_copy(s, lower, up, up_recv)
        copy.wait_recv()

        @pl.when(s >= nb)
        def _():
            term_copy(s - nb, lower, up, up_recv).wait_send()

        sendb[lax.rem(s, nb)] = (sum_of(s)[...] + up[lax.rem(s, ring)].astype(F32)).astype(BF16)
        copy.start()

    def root(s):
        r = lax.rem(s, ring)
        term_copy(s, lower, up, up_recv).wait_recv()
        term_copy(s, upper, dn, dn_recv).wait_recv()
        xres_copy(s).wait()

        @pl.when(s >= nb)
        def _():
            for copy in root_copies(s - nb):
                copy.wait_send()
            root_local(s - nb).wait()

        total = sum_of(s)[...] + up[r].astype(F32) + dn[r].astype(F32)
        sendb[lax.rem(s, nb)] = (xres[lax.rem(s, nb)].astype(F32) + total).astype(BF16)
        for copy in root_copies(s):
            copy.start()
        root_local(s).start()

    def arrived(s):
        forward_copy(s).wait_recv()

        @pl.when(p == 2)
        def _():
            forward_copy(s).start()

        part_copy(s).start()

    x_copy(0).start()
    for copy in w_copies(0):
        copy.start()
    barrier = pltpu.get_barrier_semaphore()
    pl.semaphore_signal(barrier, inc=1, device_id=partner, device_id_type=MESH)

    @pl.when(p < zs - 1)
    def _():
        pl.semaphore_signal(barrier, inc=1, device_id=upper, device_id_type=MESH)

    @pl.when(p > 0)
    def _():
        pl.semaphore_signal(barrier, inc=1, device_id=lower, device_id_type=MESH)

    pl.semaphore_wait(barrier, 1 + jnp.where(p < zs - 1, 1, 0) + jnp.where(p > 0, 1, 0))

    def clear(h, _):
        keys[h] = jnp.zeros(keys.shape[1:], BF16)
        vals[h, :HEAD, :] = jnp.zeros((HEAD, vals.shape[2]), BF16)
        vals[h, HEAD:, :] = jnp.ones((vals.shape[1] - HEAD, vals.shape[2]), BF16)

    lax.fori_loop(0, heads, clear, None)
    x_copy(0).wait()
    norm(0)

    def slot(g, _):
        i, j = lax.div(g, per), lax.rem(g, per)

        @pl.when((p == 3) & valid(g - lag5))
        def _():
            arrived(g - lag5)

        @pl.when(((p == 0) | (p == 2)) & valid(g - lag4))
        def _():
            arrived(g - lag4)

        @pl.when((p == 1) & valid(g - lag3))
        def _():
            root(g - lag3)

        @pl.when((p == 1) & valid(g - lag3 + 2))
        def _():
            xres_copy(g - lag3 + 2).start()

        @pl.when((p == 2) & valid(g - lag2))
        def _():
            relay(g - lag2)

        @pl.when(valid(g - lag1))
        def _():
            pair(g - lag1)

        @pl.when((i < nc) & (j < heads))
        def _():
            head(i, j)

        @pl.when((i < nc) & (j == heads))
        def _():
            project(i)

    lax.fori_loop(0, pieces + lag5, slot, None)

    for k in range(per):
        d2d_copy(nc - 1, k).wait_send()
    for s in range(pieces - nb, pieces):
        term_copy(s, lower, up, up_recv).wait_send()

    @pl.when(p == 1)
    def _():
        for s in range(pieces - nb, pieces):
            for copy in root_copies(s)[1:]:
                copy.wait_send()
            root_local(s).wait()

    everything, theirs = y_hbm.at[:, pl.ds(mine, half)], y_hbm.at[:, pl.ds(other, half)]

    @pl.when(p == 2)
    def _():
        remote(everything, everything, fwd_send, res_recv.at[0], upper).wait_send()

    @pl.when(p != 1)
    def _():
        remote(everything, everything, part_send, part_recv, partner).wait_send()

    remote(theirs, theirs, part_send, part_recv, partner).wait_recv()


def _tables(nc, ch):
    rate = THETA ** (-np.arange(HEAD // 2) / (HEAD // 2))
    sign = np.repeat([-1.0, 1.0], HEAD // 2)

    def both(place):
        angle = np.tile(place[:, None] * rate, (1, 2))
        return np.stack([np.cos(angle), np.sin(angle) * sign]).astype(np.float32)

    return both(np.arange(nc) * ch), both(np.arange(ch))


def solution(mesh, ch=256, tile=512):
    names = mesh.axis_names
    zs = mesh.shape["tp"] // 2

    def step(x, gain, wq, wk, wv, wo):
        n, d = x.shape
        heads = wq.shape[1] // HEAD
        nc, half, per = n // ch, d // 2, heads + 1
        sub = ch // per
        base, fine = _tables(nc, ch)
        cfg = dict(ch=ch, sub=sub, heads=heads, nc=nc, half=half, zs=zs, tile=min(tile, half), names=names)
        nb, ring = 4, 8
        dma = pltpu.SemaphoreType.DMA
        hbm, vmem = pl.BlockSpec(memory_space=pl.ANY), pl.BlockSpec(memory_space=pltpu.VMEM)
        return pl.pallas_call(
            functools.partial(_kernel, cfg),
            out_shape=jax.ShapeDtypeStruct((n, d), BF16),
            in_specs=[hbm, vmem, vmem, vmem, hbm, hbm, hbm, hbm],
            out_specs=hbm,
            scratch_shapes=[
                pltpu.VMEM((heads, n, HEAD), BF16),
                pltpu.VMEM((heads, HEAD + 8, n), BF16),
                pltpu.VMEM((heads * HEAD, d), BF16),
                pltpu.VMEM((2, d, 3 * HEAD), BF16),
                pltpu.VMEM((ch, d), BF16),
                pltpu.VMEM((ch, d), BF16),
                pltpu.VMEM((2, per, sub, half), F32),
                pltpu.VMEM((per, sub, half), BF16),
                pltpu.VMEM((ch, heads * HEAD), BF16),
                pltpu.VMEM((2 * per, sub, half), BF16),
                pltpu.VMEM((ring, sub, half), BF16),
                pltpu.VMEM((ring, sub, half), BF16),
                pltpu.VMEM((nb, sub, half), BF16),
                pltpu.VMEM((nb, sub, half), BF16),
                pltpu.VMEM((ch, HEAD), F32),
                pltpu.VMEM((ch, HEAD), F32),
                dma((2, 3)), dma((heads,)), dma, dma((nb,)),
                dma((per,)), dma((2 * per,)), dma((ring,)), dma((ring,)), dma((ring,)),
                dma((nb,)), dma((nb,)), dma((nb,)), dma((nb,)), dma, dma, dma,
            ],
            compiler_params=pltpu.CompilerParams(collective_id=0, has_side_effects=True, vmem_limit_bytes=67043328),
            name="attention_half",
        )(x, gain.astype(F32).reshape(1, d), jnp.asarray(base), jnp.asarray(fine), wq, wk, wv, wo)

    tokens, columns = P("dp", None), P(None, "tp")
    return jax.shard_map(
        step,
        mesh=mesh,
        in_specs=(tokens, P(None), columns, columns, columns, P("tp", None)),
        out_specs=tokens,
        check_vma=False,
    )
```

```python
import functools

import jax
import jax.numpy as jnp
import numpy as np
from jax import lax
from jax.experimental import pallas as pl
from jax.experimental.pallas import tpu as pltpu
from jax.sharding import PartitionSpec as P

HEAD = 128
THETA = 10000
LOG2E = 1.4426950408889634
HIDDEN = -2e30
MESH = pl.DeviceIdType.MESH
BF16, F32 = jnp.bfloat16, jnp.float32
LAGS = (3, 3, 3)
GROUP = 64


def _dot(a, b, ca, cb):
    return lax.dot_general(a, b, (((ca,), (cb,)), ((), ())), preferred_element_type=F32)


def _kernel(cfg, x_hbm, gain_ref, base_ref, fine_ref, wq_hbm, wk_hbm, wv_hbm, wo_hbm, y_hbm,
            keys, vals, wo, wbuf, zbuf, xbuf, abuf, acc, stage, seen, d2d, up, cross, sendb, resb, xres, rotc, rots, gain,
            w_sem, wo_sem, x_sem, xres_sem, d2d_send, d2d_recv, up_recv, cross_recv, res_recv,
            send_a, send_b, send_c, send_l, part_send, part_recv):
    ch, sub, per, heads, nc, half, zs, tile, names = (cfg[k] for k in ("ch", "sub", "per", "heads", "nc", "half", "zs", "tile", "names"))
    depth = 2 * half
    units = 3 * (heads // 2) + 2
    pieces = nc * per
    e = HEAD**-0.5 * LOG2E
    lag1 = units + 3
    lag2 = lag1 + LAGS[0]
    lag3 = lag2 + LAGS[1]
    lag4 = lag3 + LAGS[2]
    ring, cring, nb, nx = up.shape[0], cross.shape[0], sendb.shape[0], xres.shape[0]

    dpi, t = lax.axis_index(names[0]), lax.axis_index(names[1])
    core, z = lax.rem(t, 2), lax.div(t, 2)
    inner = (z > 0) & (z < zs - 1)
    partner, above, below = (dpi, t + 1 - 2 * core), (dpi, t + 2), (dpi, t - 2)
    toward = (dpi, jnp.where(z < zs // 2, t + 2, t - 2))
    away = (dpi, jnp.where(z < zs // 2, t - 2, t + 2))
    mine = pl.multiple_of(core * half, 128)
    other = pl.multiple_of((1 - core) * half, 128)

    def rows(s):
        return pl.ds(pl.multiple_of(s * sub, sub), sub)

    def finished(s):
        return y_hbm.at[rows(s), pl.ds(mine, half)]

    def remote(src, dst, send, recv, device):
        return pltpu.make_async_remote_copy(src_ref=src, dst_ref=dst, send_sem=send, recv_sem=recv, device_id=device, device_id_type=MESH)

    def x_copy(i, r):
        at = pl.ds(r * GROUP, GROUP)
        return pltpu.make_async_copy(x_hbm.at[pl.ds(pl.multiple_of(i * ch + r * GROUP, GROUP), GROUP), :], xbuf.at[at, :], x_sem.at[r])

    def for_unit(n, act):
        k, at = lax.rem(n, units), lax.rem(n, 3)
        group, kind = lax.div(k, 3), lax.rem(k, 3)

        def columns(w, h, wide):
            return w.at[:, pl.ds(pl.multiple_of(h * HEAD, HEAD), wide * HEAD)]

        @pl.when((kind == 0) & (2 * group + 1 < heads))
        def _():
            act(pltpu.make_async_copy(columns(wv_hbm, 2 * group, 2), wbuf.at[at], w_sem.at[at, 0]))

        @pl.when((kind == 0) & (2 * group + 1 == heads))
        def _():
            act(pltpu.make_async_copy(columns(wv_hbm, 2 * group, 1), wbuf.at[at, :, :HEAD], w_sem.at[at, 0]))

        @pl.when(kind > 0)
        def _():
            h = 2 * group + kind - 1
            act(pltpu.make_async_copy(columns(wq_hbm, h, 1), wbuf.at[at, :, :HEAD], w_sem.at[at, 0]))
            act(pltpu.make_async_copy(columns(wk_hbm, h, 1), wbuf.at[at, :, HEAD:], w_sem.at[at, 1]))

    def wo_copy(h):
        part = pl.ds(pl.multiple_of(h * HEAD, HEAD), HEAD)
        return pltpu.make_async_copy(wo_hbm.at[part, :], wo.at[part, :], wo_sem.at[h])

    def xres_copy(s):
        b = lax.rem(s, nx)
        return pltpu.make_async_copy(x_hbm.at[rows(s), pl.ds(mine, half)], xres.at[b], xres_sem.at[b])

    def d2d_copy(c, k):
        at = lax.rem(c, 2) * per + k
        return remote(stage.at[k], d2d.at[at], d2d_send.at[k], d2d_recv.at[at], partner)

    def up_copy(s):
        b, r = lax.rem(s, nb), lax.rem(s, ring)
        return remote(sendb.at[b], up.at[r], send_a.at[b], up_recv.at[r], toward)

    def cross_copy(s):
        b, r = lax.rem(s, nb), lax.rem(s, cring)
        return remote(sendb.at[b], cross.at[r], send_a.at[b], cross_recv.at[r], toward)

    def out_copy(s):
        b = lax.rem(s, nb)
        return remote(resb.at[b], finished(s), send_b.at[b], res_recv.at[lax.rem(s, ring)], away)

    def part_copy(s):
        b = lax.rem(s, nb)
        return remote(resb.at[b], finished(s), send_c.at[b], part_recv, partner)

    def local_copy(s):
        b = lax.rem(s, nb)
        return pltpu.make_async_copy(resb.at[b], finished(s), send_l.at[b])

    def onward_copy(s):
        return remote(finished(s), finished(s), part_send, part_recv, partner)

    def norm(i):
        bc, bs = base_ref[0, pl.ds(i, 1), :], base_ref[1, pl.ds(i, 1), :]
        rotc[...] = bc * fine_ref[0] - bs * fine_ref[1]
        rots[...] = bs * fine_ref[0] + bc * fine_ref[1]

        def group(r, _):
            x_copy(i, r).wait()
            at = pl.ds(pl.multiple_of(r * GROUP, GROUP), GROUP)
            cols = [slice(c, c + 128) for c in range(0, depth, 128)]
            sums = [None] * 4
            for n, c in enumerate(cols):
                wide = xbuf[at, c].astype(F32)
                sums[n % 4] = wide * wide if sums[n % 4] is None else sums[n % 4] + wide * wide
            total = functools.reduce(jnp.add, [s for s in sums if s is not None])
            scale = lax.rsqrt(jnp.sum(total, -1, keepdims=True) * (1 / depth) + 1e-6)
            scale = jnp.broadcast_to(scale, (GROUP, 128))
            for n, c in enumerate(cols):
                abuf[at, c] = (xbuf[at, c].astype(F32) * scale * gain[n : n + 1, :]).astype(BF16)

        lax.fori_loop(0, ch // GROUP, group, None)

    def turned(v):
        v = v.astype(BF16).astype(F32)
        return (v * rotc[...] + pltpu.roll(v, HEAD // 2, 1) * rots[...]).astype(BF16)

    def product(n, k, cuts, between):
        if n is None:
            for do in between:
                do()
            return
        at, total = lax.rem(n, 3), None
        for lo, hi, do in zip(cuts, cuts[1:], between):
            if lo < hi:
                part = _dot(abuf[:, lo:hi], wbuf[at, lo:hi, :], 1, 0)
                total = part if total is None else total + part
            do()
        zbuf[lax.rem(k, 2)] = total

    def cut(parts):
        lead = 1 / 7 if parts > 1 else 1
        ends = [0, lead] + [lead + (1 - lead) * (j + 1) / max(parts - 1, 1) for j in range(parts - 1)]
        return [min(round(f * depth / 256) * 256, depth) for f in ends]

    def attention(n, i, k, blocks):
        h = jnp.where(lax.rem(k, 3) == 2, 2 * lax.div(k, 3), 2 * lax.div(k, 3) - 1)
        here = pl.ds(pl.multiple_of(i * ch, ch), ch)
        wide, last = 2 * ch, blocks - 1
        state = {}

        def scores(j):
            at = slice((last - j) * wide, (last - j + 1) * wide)
            s = _dot(keys[h, at, :], state["q"], 1, 1)
            if j == 0:
                gap = lax.broadcasted_iota(jnp.int32, (wide, ch), 1) - lax.broadcasted_iota(jnp.int32, (wide, ch), 0)
                s = jnp.where(gap >= last * wide - i * ch, s, HIDDEN)
            state["s", j], state["v", j] = s, vals[h, :, at]

        def lead():
            z = zbuf[lax.rem(k + 1, 2)]
            state["q"] = turned(z[:, :HEAD])
            keys[h, here, :] = turned(z[:, HEAD:])
            scores(0)

        def block(j):
            if j + 1 < blocks:
                scores(j + 1)
            s = state.pop(("s", j))
            top = s.max(axis=0, keepdims=True)
            if j:
                top = jnp.maximum(state["top"], top)
            weights = jnp.exp2((s - top) * e).astype(BF16)
            mix = _dot(state.pop(("v", j)), weights, 1, 0)
            if j:
                mix = state["mix"] * jnp.exp2((state["top"] - top) * e) + mix
            state["top"], state["mix"] = top, mix
            if j == last:
                out = mix[:HEAD] * (1 / mix[HEAD : HEAD + 1])
                seen[:, pl.ds(pl.multiple_of(h * HEAD, HEAD), HEAD)] = out.T.astype(BF16)

        product(n, k, cut(blocks + 1), [lead, *(functools.partial(block, j) for j in range(blocks))])

    def values(n, i, k):
        def post():
            z, here = zbuf[lax.rem(k + 1, 2)], pl.ds(pl.multiple_of(i * ch, ch), ch)
            for m in range(2):
                vals[2 * lax.div(k, 3) + m, :HEAD, here] = z[:, m * HEAD : (m + 1) * HEAD].astype(BF16).T

        product(n, k, [0, depth], [post])

    def compute(i, k):
        n = i * units + k
        follows = (k > 1) & (lax.rem(k, 3) != 1)

        @pl.when(k < units)
        def _():
            @pl.when(n + 2 < nc * units)
            def _():
                for_unit(n + 2, lambda copy: copy.start())

            @pl.when((i == 0) & (k < heads))
            def _():
                wo_copy(k).start()

            for_unit(n, lambda copy: copy.wait())

            @pl.when(k == 0)
            def _():
                product(n, k, [0, depth], [lambda: None])

            @pl.when(lax.rem(k, 3) == 1)
            def _():
                values(n, i, k)

            for blocks in range(1, (nc + 1) // 2 + 1):
                pl.when(follows & (lax.div(i, 2) == blocks - 1))(functools.partial(attention, n, i, k, blocks))

        for blocks in range(1, (nc + 1) // 2 + 1):
            pl.when((k == units) & (lax.div(i, 2) == blocks - 1))(functools.partial(attention, None, i, k, blocks))

        @pl.when(k == units + 1)
        def _():
            @pl.when(i == 0)
            def _():
                for h in range(heads):
                    wo_copy(h).wait()

            @pl.when(i > 0)
            def _():
                for j in range(per):
                    d2d_copy(i - 1, j).wait_send()

            def theirs(n, _):
                at = pl.multiple_of(n * tile, tile)
                part = _dot(seen[...], wo[:, pl.ds(pl.multiple_of(other + at, 128), tile)], 1, 0)
                stage[:, :, pl.ds(at, tile)] = part.astype(BF16).reshape(per, sub, tile)

            lax.fori_loop(0, half // tile, theirs, None)
            for j in range(per):
                d2d_copy(i, j).start()

        @pl.when(k == units + 2)
        def _():
            def ours(n, _):
                at = pl.multiple_of(n * tile, tile)
                part = _dot(seen[...], wo[:, pl.ds(pl.multiple_of(mine + at, 128), tile)], 1, 0)
                acc[lax.rem(i, 2), :, :, pl.ds(at, tile)] = part.reshape(per, sub, tile)

            lax.fori_loop(0, half // tile, ours, None)

        @pl.when((k == units + 3) & (i + 1 < nc))
        def _():
            norm(i + 1)

            @pl.when(i + 2 < nc)
            def _():
                for r in range(ch // GROUP):
                    x_copy(i + 2, r).start()

    def valid(s):
        return (s >= 0) & (s < pieces)

    def sum_of(s):
        return acc.at[lax.rem(lax.div(s, per), 2), lax.rem(s, per)]

    def pair(s, _):
        at, ours = lax.rem(s, 2 * per), sum_of(s)
        d2d_copy(lax.div(s, per), lax.rem(s, per)).wait_recv()

        @pl.when(inner)
        def _():
            ours[...] = ours[...] + d2d[at].astype(F32)

        @pl.when(jnp.logical_not(inner))
        def _():
            @pl.when(s >= nb)
            def _():
                up_copy(s - nb).wait_send()

            sendb[lax.rem(s, nb)] = (ours[...] + d2d[at].astype(F32)).astype(BF16)
            up_copy(s).start()

    def relay(s):
        up_copy(s).wait_recv()

        @pl.when(s >= nb)
        def _():
            cross_copy(s - nb).wait_send()

        sendb[lax.rem(s, nb)] = (sum_of(s)[...] + up[lax.rem(s, ring)].astype(F32)).astype(BF16)
        cross_copy(s).start()

    def finish(s):
        b = lax.rem(s, nb)
        cross_copy(s).wait_recv()
        xres_copy(s).wait()

        @pl.when(s >= nb)
        def _():
            out_copy(s - nb).wait_send()
            part_copy(s - nb).wait_send()
            local_copy(s - nb).wait()

        total = sendb[b].astype(F32) + cross[lax.rem(s, cring)].astype(F32)
        resb[b] = (xres[lax.rem(s, nx)].astype(F32) + total).astype(BF16)
        out_copy(s).start()
        part_copy(s).start()
        local_copy(s).start()

    def arrived(s):
        out_copy(s).wait_recv()
        onward_copy(s).start()

    for r in range(ch // GROUP):
        x_copy(0, r).start()
    for n in range(2):
        for_unit(n, lambda copy: copy.start())
    barrier = pltpu.get_barrier_semaphore()
    pl.semaphore_signal(barrier, inc=1, device_id=partner, device_id_type=MESH)

    @pl.when(z < zs - 1)
    def _():
        pl.semaphore_signal(barrier, inc=1, device_id=above, device_id_type=MESH)

    @pl.when(z > 0)
    def _():
        pl.semaphore_signal(barrier, inc=1, device_id=below, device_id_type=MESH)

    def clear(h, _):
        keys[h] = jnp.zeros(keys.shape[1:], BF16)
        vals[h, :HEAD, :] = jnp.zeros((HEAD, vals.shape[2]), BF16)
        vals[h, HEAD:, :] = jnp.ones((vals.shape[1] - HEAD, vals.shape[2]), BF16)

    lax.fori_loop(0, heads, clear, None)
    gain[...] = gain_ref[...].astype(F32)
    norm(0)
    for r in range(ch // GROUP):
        x_copy(1, r).start()
    pl.semaphore_wait(barrier, 1 + jnp.where(z < zs - 1, 1, 0) + jnp.where(z > 0, 1, 0))

    def slot(g, _):
        i, k = lax.div(g, per), lax.rem(g, per)

        @pl.when(jnp.logical_not(inner) & valid(g - lag4))
        def _():
            arrived(g - lag4)

        @pl.when(inner & valid(g - lag3))
        def _():
            finish(g - lag3)

        @pl.when(inner & valid(g - lag3 + 2))
        def _():
            xres_copy(g - lag3 + 2).start()

        @pl.when(inner & valid(g - lag2))
        def _():
            relay(g - lag2)

        first = g - lag1 + jnp.where(k == lag1 - 1, 1, 0)
        end = g - lag1 + jnp.where(k == lag1 - 2, 2, 1)
        lax.fori_loop(jnp.clip(first, 0, pieces), jnp.clip(end, 0, pieces), pair, None)
        pl.when(i < nc)(lambda: compute(i, k))

    lax.fori_loop(0, pieces + lag4, slot, None)

    for j in range(per):
        d2d_copy(nc - 1, j).wait_send()
    for s in range(pieces - nb, pieces):
        up_copy(s).wait_send()

    @pl.when(inner)
    def _():
        for s in range(pieces - nb, pieces):
            out_copy(s).wait_send()
            part_copy(s).wait_send()
            local_copy(s).wait()

    ours, theirs = y_hbm.at[:, pl.ds(mine, half)], y_hbm.at[:, pl.ds(other, half)]

    @pl.when(jnp.logical_not(inner))
    def _():
        remote(ours, ours, part_send, part_recv, partner).wait_send()

    remote(theirs, theirs, part_send, part_recv, partner).wait_recv()


def _placed(y_in, y_out, buf, sem_in, sem_out):
    blocks, size = buf.shape[0], buf.shape[1]
    into = [pltpu.make_async_copy(y_in.at[pl.ds(r * size, size), :], buf.at[r], sem_in.at[r]) for r in range(blocks)]
    out = [pltpu.make_async_copy(buf.at[r], y_out.at[pl.ds(r * size, size), :], sem_out.at[r]) for r in range(blocks)]
    for copy in into:
        copy.start()
    for a, b in zip(into, out):
        a.wait()
        b.start()
    for copy in out:
        copy.wait()


def _tables(nc, ch):
    rate = THETA ** (-np.arange(HEAD // 2) / (HEAD // 2))
    sign = np.repeat([-1.0, 1.0], HEAD // 2)

    def both(place):
        angle = np.tile(place[:, None] * rate, (1, 2))
        return np.stack([np.cos(angle), np.sin(angle) * sign]).astype(np.float32)

    return both(np.arange(nc) * ch), both(np.arange(ch))


def solution(mesh, ch=256, tile=1792, copy_rows=128):
    names = mesh.axis_names
    zs = mesh.shape["tp"] // 2

    def step(x, gain, wq, wk, wv, wo):
        n, d = x.shape
        heads = wq.shape[1] // HEAD
        nc, half = n // ch, d // 2
        per = 3 * (heads // 2) + 7
        sub = ch // per
        base, fine = _tables(nc, ch)
        cfg = dict(ch=ch, sub=sub, per=per, heads=heads, nc=nc, half=half, zs=zs, tile=min(tile, half), names=names)
        nb, ring, cring, nx = 8, 16, 8, 4
        dma = pltpu.SemaphoreType.DMA
        hbm, vmem = pl.BlockSpec(memory_space=pl.ANY), pl.BlockSpec(memory_space=pltpu.VMEM)
        y = pl.pallas_call(
            functools.partial(_kernel, cfg),
            out_shape=jax.ShapeDtypeStruct((n, d), BF16),
            in_specs=[hbm, vmem, vmem, vmem, hbm, hbm, hbm, hbm],
            out_specs=hbm,
            scratch_shapes=[
                pltpu.VMEM((heads, n, HEAD), BF16),
                pltpu.VMEM((heads + 1, HEAD + 8, n), BF16),
                pltpu.VMEM((heads * HEAD, d), BF16),
                pltpu.VMEM((3, d, 2 * HEAD), BF16),
                pltpu.VMEM((2, ch, 2 * HEAD), F32),
                pltpu.VMEM((ch, d), BF16),
                pltpu.VMEM((ch, d), BF16),
                pltpu.VMEM((2, per, sub, half), F32),
                pltpu.VMEM((per, sub, half), BF16),
                pltpu.VMEM((ch, heads * HEAD), BF16),
                pltpu.VMEM((2 * per, sub, half), BF16),
                pltpu.VMEM((ring, sub, half), BF16),
                pltpu.VMEM((cring, sub, half), BF16),
                pltpu.VMEM((nb, sub, half), BF16),
                pltpu.VMEM((nb, sub, half), BF16),
                pltpu.VMEM((nx, sub, half), BF16),
                pltpu.VMEM((ch, HEAD), F32),
                pltpu.VMEM((ch, HEAD), F32),
                pltpu.VMEM((d // 128, 128), F32),
                dma((3, 2)), dma((heads,)), dma((ch // GROUP,)), dma((nx,)),
                dma((per,)), dma((2 * per,)), dma((ring,)), dma((cring,)), dma((ring,)),
                dma((nb,)), dma((nb,)), dma((nb,)), dma((nb,)), dma, dma,
            ],
            compiler_params=pltpu.CompilerParams(collective_id=0, has_side_effects=True, vmem_limit_bytes=67043328),
            name="attention_half",
        )(x, gain.reshape(d // 128, 128), jnp.asarray(base), jnp.asarray(fine), wq, wk, wv, wo)
        blocks = n // copy_rows
        return pl.pallas_call(
            _placed,
            out_shape=jax.ShapeDtypeStruct((n, d), BF16),
            in_specs=[hbm],
            out_specs=hbm,
            scratch_shapes=[pltpu.VMEM((blocks, copy_rows, d), BF16), dma((blocks,)), dma((blocks,))],
            compiler_params=pltpu.CompilerParams(vmem_limit_bytes=67043328),
            name="placed",
        )(y)

    tokens, columns = P("dp", None), P(None, "tp")
    return jax.shard_map(
        step,
        mesh=mesh,
        in_specs=(tokens, P(None), columns, columns, columns, P("tp", None)),
        out_specs=tokens,
        check_vma=False,
    )
```

```python
import functools

import jax
import jax.numpy as jnp
import numpy as np
from jax import lax
from jax.experimental import pallas as pl
from jax.experimental.pallas import tpu as pltpu
from jax.sharding import PartitionSpec as P

HEAD = 128
THETA = 10000
LOG2E = 1.4426950408889634
HIDDEN = -2e30
MESH = pl.DeviceIdType.MESH
BF16, F32 = jnp.bfloat16, jnp.float32
LAGS = (4, 4, 4)
GROUP = 64
WIDE = 4


def _dot(a, b, ca, cb):
    return lax.dot_general(a, b, (((ca,), (cb,)), ((), ())), preferred_element_type=F32)


def _kernel(cfg, x_hbm, gain_ref, base_ref, fine_ref, wq_hbm, wk_hbm, wv_hbm, wo_hbm, y_hbm,
            keys, vals, wo, wbuf, zbuf, xbuf, abuf, acc, stage, seen, d2d, up, cross, sendb, resb, xres, rotc, rots, gain,
            w_sem, wo_sem, x_sem, xres_sem, d2d_send, d2d_recv, up_recv, cross_recv, res_recv,
            send_a, send_b, send_c, send_l, part_send, part_recv):
    ch, sub, per, heads, nc, half, zs, tile, names = (cfg[k] for k in ("ch", "sub", "per", "heads", "nc", "half", "zs", "tile", "names"))
    depth = 2 * half
    units = 3 * (heads // 2) + 2
    pieces = nc * per
    e = HEAD**-0.5 * LOG2E
    lag1 = units + 3
    lag2 = lag1 + LAGS[0]
    lag3 = lag2 + LAGS[1]
    lag4 = lag3 + LAGS[2]
    ring, cring, nb, nx = up.shape[0], cross.shape[0], sendb.shape[0], xres.shape[0]

    dpi, t = lax.axis_index(names[0]), lax.axis_index(names[1])
    core, z = lax.rem(t, 2), lax.div(t, 2)
    inner = (z > 0) & (z < zs - 1)
    partner, above, below = (dpi, t + 1 - 2 * core), (dpi, t + 2), (dpi, t - 2)
    toward = (dpi, jnp.where(z < zs // 2, t + 2, t - 2))
    away = (dpi, jnp.where(z < zs // 2, t - 2, t + 2))
    mine = pl.multiple_of(core * half, 128)
    other = pl.multiple_of((1 - core) * half, 128)

    def rows(s):
        return pl.ds(pl.multiple_of(s * sub, sub), sub)

    def finished(s):
        return y_hbm.at[rows(s), pl.ds(mine, half)]

    def remote(src, dst, send, recv, device):
        return pltpu.make_async_remote_copy(src_ref=src, dst_ref=dst, send_sem=send, recv_sem=recv, device_id=device, device_id_type=MESH)

    def x_copy(i, r):
        at = pl.ds(r * GROUP, GROUP)
        return pltpu.make_async_copy(x_hbm.at[pl.ds(pl.multiple_of(i * ch + r * GROUP, GROUP), GROUP), :], xbuf.at[at, :], x_sem.at[r])

    def for_unit(n, act):
        k, at = lax.rem(n, units), lax.rem(n, 3)
        group, kind = lax.div(k, 3), lax.rem(k, 3)

        def columns(w, h, wide):
            return w.at[:, pl.ds(pl.multiple_of(h * HEAD, HEAD), wide * HEAD)]

        @pl.when((kind == 0) & (2 * group + 1 < heads))
        def _():
            act(pltpu.make_async_copy(columns(wv_hbm, 2 * group, 2), wbuf.at[at], w_sem.at[at, 0]))

        @pl.when((kind == 0) & (2 * group + 1 == heads))
        def _():
            act(pltpu.make_async_copy(columns(wv_hbm, 2 * group, 1), wbuf.at[at, :, :HEAD], w_sem.at[at, 0]))

        @pl.when(kind > 0)
        def _():
            h = 2 * group + kind - 1
            act(pltpu.make_async_copy(columns(wq_hbm, h, 1), wbuf.at[at, :, :HEAD], w_sem.at[at, 0]))
            act(pltpu.make_async_copy(columns(wk_hbm, h, 1), wbuf.at[at, :, HEAD:], w_sem.at[at, 1]))

    def wo_copy(h):
        part = pl.ds(pl.multiple_of(h * HEAD, HEAD), HEAD)
        return pltpu.make_async_copy(wo_hbm.at[part, :], wo.at[part, :], wo_sem.at[h])

    def xres_copy(s):
        b = lax.rem(s, nx)
        return pltpu.make_async_copy(x_hbm.at[rows(s), pl.ds(mine, half)], xres.at[b], xres_sem.at[b])

    def d2d_copy(c, k):
        at = lax.rem(c, 2) * per + k
        return remote(stage.at[k], d2d.at[at], d2d_send.at[k], d2d_recv.at[at], partner)

    def up_copy(s):
        b, r = lax.rem(s, nb), lax.rem(s, ring)
        return remote(sendb.at[b], up.at[r], send_a.at[b], up_recv.at[r], toward)

    def cross_copy(s):
        b, r = lax.rem(s, nb), lax.rem(s, cring)
        return remote(sendb.at[b], cross.at[r], send_a.at[b], cross_recv.at[r], toward)

    def out_copy(s):
        b = lax.rem(s, nb)
        return remote(resb.at[b], finished(s), send_b.at[b], res_recv.at[lax.rem(s, ring)], away)

    def part_copy(s):
        b = lax.rem(s, nb)
        return remote(resb.at[b], finished(s), send_c.at[b], part_recv, partner)

    def local_copy(s):
        b = lax.rem(s, nb)
        return pltpu.make_async_copy(resb.at[b], finished(s), send_l.at[b])

    def onward_copy(s):
        return remote(finished(s), finished(s), part_send, part_recv, partner)

    def norm(i):
        bc, bs = base_ref[0, pl.ds(i, 1), :], base_ref[1, pl.ds(i, 1), :]
        rotc[...] = bc * fine_ref[0] - bs * fine_ref[1]
        rots[...] = bs * fine_ref[0] + bc * fine_ref[1]

        def group(r, _):
            x_copy(i, r).wait()
            at = pl.ds(pl.multiple_of(r * GROUP, GROUP), GROUP)
            cols = [slice(c, c + 128) for c in range(0, depth, 128)]
            sums = [None] * 4
            for n, c in enumerate(cols):
                wide = xbuf[at, c].astype(F32)
                sums[n % 4] = wide * wide if sums[n % 4] is None else sums[n % 4] + wide * wide
            total = functools.reduce(jnp.add, [s for s in sums if s is not None])
            scale = lax.rsqrt(jnp.sum(total, -1, keepdims=True) * (1 / depth) + 1e-6)
            scale = jnp.broadcast_to(scale, (GROUP, 128))
            for n, c in enumerate(cols):
                abuf[at, c] = (xbuf[at, c].astype(F32) * scale * gain[n : n + 1, :]).astype(BF16)

        lax.fori_loop(0, ch // GROUP, group, None)

    def turned(v):
        v = v.astype(BF16).astype(F32)
        return (v * rotc[...] + pltpu.roll(v, HEAD // 2, 1) * rots[...]).astype(BF16)

    def product(n, k, cuts, between):
        if n is None:
            for do in between:
                do()
            return
        at, total = lax.rem(n, 3), None
        for lo, hi, do in zip(cuts, cuts[1:], between):
            if lo < hi:
                part = _dot(abuf[:, lo:hi], wbuf[at, lo:hi, :], 1, 0)
                total = part if total is None else total + part
            do()
        zbuf[lax.rem(k, 2)] = total

    def cut(parts):
        lead = 1 / 7 if parts > 1 else 1
        ends = [0, lead] + [lead + (1 - lead) * (j + 1) / max(parts - 1, 1) for j in range(parts - 1)]
        return [min(round(f * depth / 256) * 256, depth) for f in ends]

    def attention(n, i, k, blocks):
        h = jnp.where(lax.rem(k, 3) == 2, 2 * lax.div(k, 3), 2 * lax.div(k, 3) - 1)
        here = pl.ds(pl.multiple_of(i * ch, ch), ch)
        wide, last = WIDE * ch, blocks - 1
        state = {}

        def scores(j):
            at = slice((last - j) * wide, (last - j + 1) * wide)
            s = _dot(keys[h, at, :], state["q"], 1, 1)
            if j == 0:
                gap = lax.broadcasted_iota(jnp.int32, (wide, ch), 1) - lax.broadcasted_iota(jnp.int32, (wide, ch), 0)
                s = jnp.where(gap >= last * wide - i * ch, s, HIDDEN)
            state["s", j], state["v", j] = s, vals[h, :, at]

        def lead():
            z = zbuf[lax.rem(k + 1, 2)]
            state["q"] = turned(z[:, :HEAD])
            keys[h, here, :] = turned(z[:, HEAD:])
            scores(0)

        def block(j):
            if j + 1 < blocks:
                scores(j + 1)
            s = state.pop(("s", j))
            top = s.max(axis=0, keepdims=True)
            if j:
                top = jnp.maximum(state["top"], top)
            weights = jnp.exp2((s - top) * e).astype(BF16)
            mix = _dot(state.pop(("v", j)), weights, 1, 0)
            if j:
                mix = state["mix"] * jnp.exp2((state["top"] - top) * e) + mix
            state["top"], state["mix"] = top, mix
            if j == last:
                out = mix[:HEAD] * (1 / mix[HEAD : HEAD + 1])
                seen[:, pl.ds(pl.multiple_of(h * HEAD, HEAD), HEAD)] = out.T.astype(BF16)

        product(n, k, cut(blocks + 1), [lead, *(functools.partial(block, j) for j in range(blocks))])

    def values(n, i, k):
        def post():
            z, here = zbuf[lax.rem(k + 1, 2)], pl.ds(pl.multiple_of(i * ch, ch), ch)
            for m in range(2):
                vals[2 * lax.div(k, 3) + m, :HEAD, here] = z[:, m * HEAD : (m + 1) * HEAD].astype(BF16).T

        product(n, k, [0, depth], [post])

    def compute(i, k):
        n = i * units + k
        follows = (k > 1) & (lax.rem(k, 3) != 1)

        @pl.when(k < units)
        def _():
            @pl.when(n + 2 < nc * units)
            def _():
                for_unit(n + 2, lambda copy: copy.start())

            @pl.when((i == 0) & (k < heads))
            def _():
                wo_copy(k).start()

            for_unit(n, lambda copy: copy.wait())

            @pl.when(k == 0)
            def _():
                product(n, k, [0, depth], [lambda: None])

            @pl.when(lax.rem(k, 3) == 1)
            def _():
                values(n, i, k)

            for blocks in range(1, pl.cdiv(nc, WIDE) + 1):
                pl.when(follows & (lax.div(i, WIDE) == blocks - 1))(functools.partial(attention, n, i, k, blocks))

        for blocks in range(1, pl.cdiv(nc, WIDE) + 1):
            pl.when((k == units) & (lax.div(i, WIDE) == blocks - 1))(functools.partial(attention, None, i, k, blocks))

        @pl.when(k == units + 1)
        def _():
            @pl.when(i == 0)
            def _():
                for h in range(heads):
                    wo_copy(h).wait()

            @pl.when(i > 0)
            def _():
                for j in range(per):
                    d2d_copy(i - 1, j).wait_send()

            def theirs(n, _):
                at = pl.multiple_of(n * tile, tile)
                part = _dot(seen[...], wo[:, pl.ds(pl.multiple_of(other + at, 128), tile)], 1, 0)
                stage[:, :, pl.ds(at, tile)] = part.astype(BF16).reshape(per, sub, tile)

            lax.fori_loop(0, half // tile, theirs, None)
            for j in range(per):
                d2d_copy(i, j).start()

        @pl.when(k == units + 2)
        def _():
            def ours(n, _):
                at = pl.multiple_of(n * tile, tile)
                part = _dot(seen[...], wo[:, pl.ds(pl.multiple_of(mine + at, 128), tile)], 1, 0)
                acc[lax.rem(i, 2), :, :, pl.ds(at, tile)] = part.reshape(per, sub, tile)

            lax.fori_loop(0, half // tile, ours, None)

        @pl.when((k == units + 3) & (i + 1 < nc))
        def _():
            norm(i + 1)

            @pl.when(i + 2 < nc)
            def _():
                for r in range(ch // GROUP):
                    x_copy(i + 2, r).start()

    def valid(s):
        return (s >= 0) & (s < pieces)

    def sum_of(s):
        return acc.at[lax.rem(lax.div(s, per), 2), lax.rem(s, per)]

    def pair(s, _):
        at, ours = lax.rem(s, 2 * per), sum_of(s)
        d2d_copy(lax.div(s, per), lax.rem(s, per)).wait_recv()

        @pl.when(inner)
        def _():
            ours[...] = ours[...] + d2d[at].astype(F32)

        @pl.when(jnp.logical_not(inner))
        def _():
            @pl.when(s >= nb)
            def _():
                up_copy(s - nb).wait_send()

            sendb[lax.rem(s, nb)] = (ours[...] + d2d[at].astype(F32)).astype(BF16)
            up_copy(s).start()

    def relay(s):
        up_copy(s).wait_recv()

        @pl.when(s >= nb)
        def _():
            cross_copy(s - nb).wait_send()

        sendb[lax.rem(s, nb)] = (sum_of(s)[...] + up[lax.rem(s, ring)].astype(F32)).astype(BF16)
        cross_copy(s).start()

    def finish(s):
        b = lax.rem(s, nb)
        cross_copy(s).wait_recv()
        xres_copy(s).wait()

        @pl.when(s >= nb)
        def _():
            out_copy(s - nb).wait_send()
            part_copy(s - nb).wait_send()
            local_copy(s - nb).wait()

        total = sendb[b].astype(F32) + cross[lax.rem(s, cring)].astype(F32)
        resb[b] = (xres[lax.rem(s, nx)].astype(F32) + total).astype(BF16)
        out_copy(s).start()
        part_copy(s).start()
        local_copy(s).start()

    def arrived(s):
        out_copy(s).wait_recv()
        onward_copy(s).start()

    for r in range(ch // GROUP):
        x_copy(0, r).start()
    for n in range(2):
        for_unit(n, lambda copy: copy.start())
    barrier = pltpu.get_barrier_semaphore()
    pl.semaphore_signal(barrier, inc=1, device_id=partner, device_id_type=MESH)

    @pl.when(z < zs - 1)
    def _():
        pl.semaphore_signal(barrier, inc=1, device_id=above, device_id_type=MESH)

    @pl.when(z > 0)
    def _():
        pl.semaphore_signal(barrier, inc=1, device_id=below, device_id_type=MESH)

    def clear(h, _):
        keys[h] = jnp.zeros(keys.shape[1:], BF16)
        vals[h, :HEAD, :] = jnp.zeros((HEAD, vals.shape[2]), BF16)
        vals[h, HEAD:, :] = jnp.ones((vals.shape[1] - HEAD, vals.shape[2]), BF16)

    lax.fori_loop(0, heads, clear, None)
    gain[...] = gain_ref[...].astype(F32)
    norm(0)
    for r in range(ch // GROUP):
        x_copy(1, r).start()
    pl.semaphore_wait(barrier, 1 + jnp.where(z < zs - 1, 1, 0) + jnp.where(z > 0, 1, 0))

    def slot(g, _):
        i, k = lax.div(g, per), lax.rem(g, per)

        @pl.when(jnp.logical_not(inner) & valid(g - lag4))
        def _():
            arrived(g - lag4)

        @pl.when(inner & valid(g - lag3))
        def _():
            finish(g - lag3)

        @pl.when(inner & valid(g - lag3 + 3))
        def _():
            xres_copy(g - lag3 + 3).start()

        @pl.when(inner & valid(g - lag2))
        def _():
            relay(g - lag2)

        first = g - lag1 + jnp.where(k == lag1 - 1, 1, 0)
        end = g - lag1 + jnp.where(k == lag1 - 2, 2, 1)
        lax.fori_loop(jnp.clip(first, 0, pieces), jnp.clip(end, 0, pieces), pair, None)
        pl.when(i < nc)(lambda: compute(i, k))

    lax.fori_loop(0, pieces + lag4, slot, None)

    for j in range(per):
        d2d_copy(nc - 1, j).wait_send()
    for s in range(pieces - nb, pieces):
        up_copy(s).wait_send()

    @pl.when(inner)
    def _():
        for s in range(pieces - nb, pieces):
            out_copy(s).wait_send()
            part_copy(s).wait_send()
            local_copy(s).wait()

    ours, theirs = y_hbm.at[:, pl.ds(mine, half)], y_hbm.at[:, pl.ds(other, half)]

    @pl.when(jnp.logical_not(inner))
    def _():
        remote(ours, ours, part_send, part_recv, partner).wait_send()

    remote(theirs, theirs, part_send, part_recv, partner).wait_recv()


def _placed(y_in, y_out, buf, sem_in, sem_out):
    blocks, size, ahead = buf.shape[0], buf.shape[1], 6
    into = [pltpu.make_async_copy(y_in.at[pl.ds(r * size, size), :], buf.at[r], sem_in.at[r]) for r in range(blocks)]
    out = [pltpu.make_async_copy(buf.at[r], y_out.at[pl.ds(r * size, size), :], sem_out.at[r]) for r in range(blocks)]
    for copy in into[:ahead]:
        copy.start()
    for r in range(blocks):
        into[r].wait()
        out[r].start()
        if r + ahead < blocks:
            into[r + ahead].start()
    for copy in out:
        copy.wait()


def _tables(nc, ch):
    rate = THETA ** (-np.arange(HEAD // 2) / (HEAD // 2))
    sign = np.repeat([-1.0, 1.0], HEAD // 2)

    def both(place):
        angle = np.tile(place[:, None] * rate, (1, 2))
        return np.stack([np.cos(angle), np.sin(angle) * sign]).astype(np.float32)

    return both(np.arange(nc) * ch), both(np.arange(ch))


def solution(mesh, ch=128, tile=1792, copy_rows=64):
    names = mesh.axis_names
    zs = mesh.shape["tp"] // 2

    def step(x, gain, wq, wk, wv, wo):
        n, d = x.shape
        heads = wq.shape[1] // HEAD
        nc, half = n // ch, d // 2
        per = 3 * (heads // 2) + 7
        sub = ch // per
        base, fine = _tables(nc, ch)
        cfg = dict(ch=ch, sub=sub, per=per, heads=heads, nc=nc, half=half, zs=zs, tile=min(tile, half), names=names)
        nb, ring, cring, nx = 8, 16, 8, 4
        dma = pltpu.SemaphoreType.DMA
        hbm, vmem = pl.BlockSpec(memory_space=pl.ANY), pl.BlockSpec(memory_space=pltpu.VMEM)
        y = pl.pallas_call(
            functools.partial(_kernel, cfg),
            out_shape=jax.ShapeDtypeStruct((n, d), BF16),
            in_specs=[hbm, vmem, vmem, vmem, hbm, hbm, hbm, hbm],
            out_specs=hbm,
            scratch_shapes=[
                pltpu.VMEM((heads, n, HEAD), BF16),
                pltpu.VMEM((heads + 1, HEAD + 8, n), BF16),
                pltpu.VMEM((heads * HEAD, d), BF16),
                pltpu.VMEM((3, d, 2 * HEAD), BF16),
                pltpu.VMEM((2, ch, 2 * HEAD), F32),
                pltpu.VMEM((ch, d), BF16),
                pltpu.VMEM((ch, d), BF16),
                pltpu.VMEM((2, per, sub, half), F32),
                pltpu.VMEM((per, sub, half), BF16),
                pltpu.VMEM((ch, heads * HEAD), BF16),
                pltpu.VMEM((2 * per, sub, half), BF16),
                pltpu.VMEM((ring, sub, half), BF16),
                pltpu.VMEM((cring, sub, half), BF16),
                pltpu.VMEM((nb, sub, half), BF16),
                pltpu.VMEM((nb, sub, half), BF16),
                pltpu.VMEM((nx, sub, half), BF16),
                pltpu.VMEM((ch, HEAD), F32),
                pltpu.VMEM((ch, HEAD), F32),
                pltpu.VMEM((d // 128, 128), F32),
                dma((3, 2)), dma((heads,)), dma((ch // GROUP,)), dma((nx,)),
                dma((per,)), dma((2 * per,)), dma((ring,)), dma((cring,)), dma((ring,)),
                dma((nb,)), dma((nb,)), dma((nb,)), dma((nb,)), dma, dma,
            ],
            compiler_params=pltpu.CompilerParams(collective_id=0, has_side_effects=True, vmem_limit_bytes=67043328),
            name="attention_half",
        )(x, gain.reshape(d // 128, 128), jnp.asarray(base), jnp.asarray(fine), wq, wk, wv, wo)
        blocks = n // copy_rows
        return pl.pallas_call(
            _placed,
            out_shape=jax.ShapeDtypeStruct((n, d), BF16),
            in_specs=[hbm],
            out_specs=hbm,
            scratch_shapes=[pltpu.VMEM((blocks, copy_rows, d), BF16), dma((blocks,)), dma((blocks,))],
            compiler_params=pltpu.CompilerParams(vmem_limit_bytes=67043328),
            name="placed",
        )(y)

    tokens, columns = P("dp", None), P(None, "tp")
    return jax.shard_map(
        step,
        mesh=mesh,
        in_specs=(tokens, P(None), columns, columns, columns, P("tp", None)),
        out_specs=tokens,
        check_vma=False,
    )
```

```python
import functools

import jax
import jax.numpy as jnp
import numpy as np
from jax import lax
from jax.experimental import pallas as pl
from jax.experimental.pallas import tpu as pltpu
from jax.sharding import PartitionSpec as P

HEAD = 128
THETA = 10000
LOG2E = 1.4426950408889634
HIDDEN = -2e30
MESH = pl.DeviceIdType.MESH
BF16, F32 = jnp.bfloat16, jnp.float32
LAGS = (4, 4, 4)
GROUP = 64
KERNEL_VMEM = 46 * 2**20
WIDE = 4


def _dot(a, b, ca, cb):
    return lax.dot_general(a, b, (((ca,), (cb,)), ((), ())), preferred_element_type=F32)


def _kernel(cfg, x_hbm, gain_ref, base_ref, fine_ref, wq_hbm, wk_hbm, wv_hbm, wo_hbm, early, late,
            keys, vals, wo, wbuf, zbuf, xbuf, abuf, acc, stage, seen, d2d, up, cross, sendb, resb, xres, rotc, rots, gain,
            w_sem, wo_sem, x_sem, xres_sem, d2d_send, d2d_recv, up_recv, cross_recv, res_recv,
            send_a, send_b, send_c, send_l, part_send, part_recv):
    ch, sub, per, heads, nc, half, zs, tile, names = (cfg[k] for k in ("ch", "sub", "per", "heads", "nc", "half", "zs", "tile", "names"))
    depth = 2 * half
    units = 3 * (heads // 2) + 2
    pieces = nc * per
    e = HEAD**-0.5 * LOG2E
    lag1 = units + 3
    lag2 = lag1 + LAGS[0]
    lag3 = lag2 + LAGS[1]
    lag4 = lag3 + LAGS[2]
    ring, cring, nb, nx = up.shape[0], cross.shape[0], sendb.shape[0], xres.shape[0]

    dpi, t = lax.axis_index(names[0]), lax.axis_index(names[1])
    core, z = lax.rem(t, 2), lax.div(t, 2)
    inner = (z > 0) & (z < zs - 1)
    partner, above, below = (dpi, t + 1 - 2 * core), (dpi, t + 2), (dpi, t - 2)
    toward = (dpi, jnp.where(z < zs // 2, t + 2, t - 2))
    away = (dpi, jnp.where(z < zs // 2, t - 2, t + 2))
    mine = pl.multiple_of(core * half, 128)
    other = pl.multiple_of((1 - core) * half, 128)

    def rows(s):
        return pl.ds(pl.multiple_of(s * sub, sub), sub)

    def finished(s, act):
        cols, split = pl.ds(mine, half), early.shape[0] // sub
        pl.when(s < split)(lambda: act(early.at[rows(s), cols], 0))
        pl.when(s >= split)(lambda: act(late.at[rows(s - split), cols], 1))

    def remote(src, dst, send, recv, device):
        return pltpu.make_async_remote_copy(src_ref=src, dst_ref=dst, send_sem=send, recv_sem=recv, device_id=device, device_id_type=MESH)

    def x_copy(i, r):
        at = pl.ds(r * GROUP, GROUP)
        return pltpu.make_async_copy(x_hbm.at[pl.ds(pl.multiple_of(i * ch + r * GROUP, GROUP), GROUP), :], xbuf.at[at, :], x_sem.at[r])

    def for_unit(n, act):
        k, at = lax.rem(n, units), lax.rem(n, 3)
        group, kind = lax.div(k, 3), lax.rem(k, 3)

        def columns(w, h, wide):
            return w.at[:, pl.ds(pl.multiple_of(h * HEAD, HEAD), wide * HEAD)]

        @pl.when((kind == 0) & (2 * group + 1 < heads))
        def _():
            act(pltpu.make_async_copy(columns(wv_hbm, 2 * group, 2), wbuf.at[at], w_sem.at[at, 0]))

        @pl.when((kind == 0) & (2 * group + 1 == heads))
        def _():
            act(pltpu.make_async_copy(columns(wv_hbm, 2 * group, 1), wbuf.at[at, :, :HEAD], w_sem.at[at, 0]))

        @pl.when(kind > 0)
        def _():
            h = 2 * group + kind - 1
            act(pltpu.make_async_copy(columns(wq_hbm, h, 1), wbuf.at[at, :, :HEAD], w_sem.at[at, 0]))
            act(pltpu.make_async_copy(columns(wk_hbm, h, 1), wbuf.at[at, :, HEAD:], w_sem.at[at, 1]))

    def wo_copy(h):
        part = pl.ds(pl.multiple_of(h * HEAD, HEAD), HEAD)
        return pltpu.make_async_copy(wo_hbm.at[part, :], wo.at[part, :], wo_sem.at[h])

    def xres_copy(s):
        b = lax.rem(s, nx)
        return pltpu.make_async_copy(x_hbm.at[rows(s), pl.ds(mine, half)], xres.at[b], xres_sem.at[b])

    def d2d_copy(c, k):
        at = lax.rem(c, 2) * per + k
        return remote(stage.at[k], d2d.at[at], d2d_send.at[k], d2d_recv.at[at], partner)

    def up_copy(s):
        b, r = lax.rem(s, nb), lax.rem(s, ring)
        return remote(sendb.at[b], up.at[r], send_a.at[b], up_recv.at[r], toward)

    def cross_copy(s):
        b, r = lax.rem(s, nb), lax.rem(s, cring)
        return remote(sendb.at[b], cross.at[r], send_a.at[b], cross_recv.at[r], toward)

    def out_copy(s, act):
        b = lax.rem(s, nb)
        finished(s, lambda at, _: act(remote(resb.at[b], at, send_b.at[b], res_recv.at[lax.rem(s, ring)], away)))

    def part_copy(s, act):
        b = lax.rem(s, nb)
        finished(s, lambda at, which: act(remote(resb.at[b], at, send_c.at[b], part_recv.at[which], partner)))

    def local_copy(s, act):
        b = lax.rem(s, nb)
        finished(s, lambda at, _: act(pltpu.make_async_copy(resb.at[b], at, send_l.at[b])))

    def onward_copy(s, act):
        finished(s, lambda at, which: act(remote(at, at, part_send.at[which], part_recv.at[which], partner)))

    def start(copy):
        copy.start()

    def norm(i):
        bc, bs = base_ref[0, pl.ds(i, 1), :], base_ref[1, pl.ds(i, 1), :]
        rotc[...] = bc * fine_ref[0] - bs * fine_ref[1]
        rots[...] = bs * fine_ref[0] + bc * fine_ref[1]

        def group(r, _):
            x_copy(i, r).wait()
            at = pl.ds(pl.multiple_of(r * GROUP, GROUP), GROUP)
            cols = [slice(c, c + 128) for c in range(0, depth, 128)]
            sums = [None] * 4
            for n, c in enumerate(cols):
                wide = xbuf[at, c].astype(F32)
                sums[n % 4] = wide * wide if sums[n % 4] is None else sums[n % 4] + wide * wide
            total = functools.reduce(jnp.add, [s for s in sums if s is not None])
            scale = lax.rsqrt(jnp.sum(total, -1, keepdims=True) * (1 / depth) + 1e-6)
            scale = jnp.broadcast_to(scale, (GROUP, 128))
            for n, c in enumerate(cols):
                abuf[at, c] = (xbuf[at, c].astype(F32) * scale * gain[n : n + 1, :]).astype(BF16)

        lax.fori_loop(0, ch // GROUP, group, None)

    def turned(v):
        v = v.astype(BF16).astype(F32)
        return (v * rotc[...] + pltpu.roll(v, HEAD // 2, 1) * rots[...]).astype(BF16)

    def product(n, k, cuts, between):
        if n is None:
            for do in between:
                do()
            return
        at, total = lax.rem(n, 3), None
        for lo, hi, do in zip(cuts, cuts[1:], between):
            if lo < hi:
                part = _dot(abuf[:, lo:hi], wbuf[at, lo:hi, :], 1, 0)
                total = part if total is None else total + part
            do()
        zbuf[lax.rem(k, 2)] = total

    def cut(parts):
        lead = 1 / 7 if parts > 1 else 1
        ends = [0, lead] + [lead + (1 - lead) * (j + 1) / max(parts - 1, 1) for j in range(parts - 1)]
        return [min(round(f * depth / 256) * 256, depth) for f in ends]

    def attention(n, i, k, blocks):
        h = jnp.where(lax.rem(k, 3) == 2, 2 * lax.div(k, 3), 2 * lax.div(k, 3) - 1)
        here = pl.ds(pl.multiple_of(i * ch, ch), ch)
        wide, last = WIDE * ch, blocks - 1
        state = {}

        def scores(j):
            at = slice((last - j) * wide, (last - j + 1) * wide)
            s = _dot(keys[h, at, :], state["q"], 1, 1)
            if j == 0:
                gap = lax.broadcasted_iota(jnp.int32, (wide, ch), 1) - lax.broadcasted_iota(jnp.int32, (wide, ch), 0)
                s = jnp.where(gap >= last * wide - i * ch, s, HIDDEN)
            state["s", j], state["v", j] = s, vals[h, :, at]

        def lead():
            z = zbuf[lax.rem(k + 1, 2)]
            state["q"] = turned(z[:, :HEAD])
            keys[h, here, :] = turned(z[:, HEAD:])
            scores(0)

        def block(j):
            if j + 1 < blocks:
                scores(j + 1)
            s = state.pop(("s", j))
            top = s.max(axis=0, keepdims=True)
            if j:
                top = jnp.maximum(state["top"], top)
            weights = jnp.exp2((s - top) * e).astype(BF16)
            mix = _dot(state.pop(("v", j)), weights, 1, 0)
            if j:
                mix = state["mix"] * jnp.exp2((state["top"] - top) * e) + mix
            state["top"], state["mix"] = top, mix
            if j == last:
                out = mix[:HEAD] * (1 / mix[HEAD : HEAD + 1])
                seen[:, pl.ds(pl.multiple_of(h * HEAD, HEAD), HEAD)] = out.T.astype(BF16)

        product(n, k, cut(blocks + 1), [lead, *(functools.partial(block, j) for j in range(blocks))])

    def values(n, i, k):
        def post():
            z, here = zbuf[lax.rem(k + 1, 2)], pl.ds(pl.multiple_of(i * ch, ch), ch)
            for m in range(2):
                vals[2 * lax.div(k, 3) + m, :HEAD, here] = z[:, m * HEAD : (m + 1) * HEAD].astype(BF16).T

        product(n, k, [0, depth], [post])

    def compute(i, k):
        n = i * units + k
        follows = (k > 1) & (lax.rem(k, 3) != 1)

        @pl.when(k < units)
        def _():
            @pl.when(n + 2 < nc * units)
            def _():
                for_unit(n + 2, lambda copy: copy.start())

            @pl.when((i == 0) & (k < heads))
            def _():
                wo_copy(k).start()

            for_unit(n, lambda copy: copy.wait())

            @pl.when(k == 0)
            def _():
                product(n, k, [0, depth], [lambda: None])

            @pl.when(lax.rem(k, 3) == 1)
            def _():
                values(n, i, k)

            for blocks in range(1, pl.cdiv(nc, WIDE) + 1):
                pl.when(follows & (lax.div(i, WIDE) == blocks - 1))(functools.partial(attention, n, i, k, blocks))

        for blocks in range(1, pl.cdiv(nc, WIDE) + 1):
            pl.when((k == units) & (lax.div(i, WIDE) == blocks - 1))(functools.partial(attention, None, i, k, blocks))

        @pl.when(k == units + 1)
        def _():
            @pl.when(i == 0)
            def _():
                for h in range(heads):
                    wo_copy(h).wait()

            @pl.when(i > 0)
            def _():
                for j in range(per):
                    d2d_copy(i - 1, j).wait_send()

            def theirs(n, _):
                at = pl.multiple_of(n * tile, tile)
                part = _dot(seen[...], wo[:, pl.ds(pl.multiple_of(other + at, 128), tile)], 1, 0)
                stage[:, :, pl.ds(at, tile)] = part.astype(BF16).reshape(per, sub, tile)

            lax.fori_loop(0, half // tile, theirs, None)
            for j in range(per):
                d2d_copy(i, j).start()

        @pl.when(k == units + 2)
        def _():
            def ours(n, _):
                at = pl.multiple_of(n * tile, tile)
                part = _dot(seen[...], wo[:, pl.ds(pl.multiple_of(mine + at, 128), tile)], 1, 0)
                acc[lax.rem(i, 2), :, :, pl.ds(at, tile)] = part.reshape(per, sub, tile)

            lax.fori_loop(0, half // tile, ours, None)

        @pl.when((k == units + 3) & (i + 1 < nc))
        def _():
            norm(i + 1)

            @pl.when(i + 2 < nc)
            def _():
                for r in range(ch // GROUP):
                    x_copy(i + 2, r).start()

    def valid(s):
        return (s >= 0) & (s < pieces)

    def sum_of(s):
        return acc.at[lax.rem(lax.div(s, per), 2), lax.rem(s, per)]

    def pair(s, _):
        at, ours = lax.rem(s, 2 * per), sum_of(s)
        d2d_copy(lax.div(s, per), lax.rem(s, per)).wait_recv()

        @pl.when(inner)
        def _():
            ours[...] = ours[...] + d2d[at].astype(F32)

        @pl.when(jnp.logical_not(inner))
        def _():
            @pl.when(s >= nb)
            def _():
                up_copy(s - nb).wait_send()

            sendb[lax.rem(s, nb)] = (ours[...] + d2d[at].astype(F32)).astype(BF16)
            up_copy(s).start()

    def relay(s):
        up_copy(s).wait_recv()

        @pl.when(s >= nb)
        def _():
            cross_copy(s - nb).wait_send()

        sendb[lax.rem(s, nb)] = (sum_of(s)[...] + up[lax.rem(s, ring)].astype(F32)).astype(BF16)
        cross_copy(s).start()

    def sent(s):
        out_copy(s, lambda copy: copy.wait_send())
        part_copy(s, lambda copy: copy.wait_send())
        local_copy(s, lambda copy: copy.wait())

    def finish(s):
        b = lax.rem(s, nb)
        cross_copy(s).wait_recv()
        xres_copy(s).wait()

        @pl.when(s >= nb)
        def _():
            sent(s - nb)

        total = sendb[b].astype(F32) + cross[lax.rem(s, cring)].astype(F32)
        resb[b] = (xres[lax.rem(s, nx)].astype(F32) + total).astype(BF16)
        out_copy(s, start)
        part_copy(s, start)
        local_copy(s, start)

    def arrived(s):
        out_copy(s, lambda copy: copy.wait_recv())
        onward_copy(s, start)

    for r in range(ch // GROUP):
        x_copy(0, r).start()
    for n in range(2):
        for_unit(n, lambda copy: copy.start())
    barrier = pltpu.get_barrier_semaphore()
    pl.semaphore_signal(barrier, inc=1, device_id=partner, device_id_type=MESH)

    @pl.when(z < zs - 1)
    def _():
        pl.semaphore_signal(barrier, inc=1, device_id=above, device_id_type=MESH)

    @pl.when(z > 0)
    def _():
        pl.semaphore_signal(barrier, inc=1, device_id=below, device_id_type=MESH)

    def clear(h, _):
        keys[h] = jnp.zeros(keys.shape[1:], BF16)
        vals[h, :HEAD, :] = jnp.zeros((HEAD, vals.shape[2]), BF16)
        vals[h, HEAD:, :] = jnp.ones((vals.shape[1] - HEAD, vals.shape[2]), BF16)

    lax.fori_loop(0, heads, clear, None)
    gain[...] = gain_ref[...].astype(F32)
    norm(0)
    for r in range(ch // GROUP):
        x_copy(1, r).start()
    pl.semaphore_wait(barrier, 1 + jnp.where(z < zs - 1, 1, 0) + jnp.where(z > 0, 1, 0))

    def slot(g, _):
        i, k = lax.div(g, per), lax.rem(g, per)

        @pl.when(jnp.logical_not(inner) & valid(g - lag4))
        def _():
            arrived(g - lag4)

        @pl.when(inner & valid(g - lag3))
        def _():
            finish(g - lag3)

        @pl.when(inner & valid(g - lag3 + 3))
        def _():
            xres_copy(g - lag3 + 3).start()

        @pl.when(inner & valid(g - lag2))
        def _():
            relay(g - lag2)

        first = g - lag1 + jnp.where(k == lag1 - 1, 1, 0)
        end = g - lag1 + jnp.where(k == lag1 - 2, 2, 1)
        lax.fori_loop(jnp.clip(first, 0, pieces), jnp.clip(end, 0, pieces), pair, None)
        pl.when(i < nc)(lambda: compute(i, k))

    lax.fori_loop(0, pieces + lag4, slot, None)

    for j in range(per):
        d2d_copy(nc - 1, j).wait_send()
    for s in range(pieces - nb, pieces):
        up_copy(s).wait_send()

    @pl.when(inner)
    def _():
        for s in range(pieces - nb, pieces):
            sent(s)

    for which, y in enumerate((early, late)):
        ours, theirs = y.at[:, pl.ds(mine, half)], y.at[:, pl.ds(other, half)]
        pl.when(jnp.logical_not(inner))(remote(ours, ours, part_send.at[which], part_recv.at[which], partner).wait_send)
        remote(theirs, theirs, part_send.at[which], part_recv.at[which], partner).wait_recv()


def _placed(early, late, y, buf, sem_in, sem_out, sem_late):
    blocks, size, n = buf.shape[0], buf.shape[1], early.shape[0]
    into = [pltpu.make_async_copy(early.at[pl.ds(r * size, size), :], buf.at[r], sem_in.at[r]) for r in range(blocks)]
    out = [pltpu.make_async_copy(buf.at[r], y.at[pl.ds(r * size, size), :], sem_out.at[r]) for r in range(blocks)]
    rest = pltpu.make_async_copy(late, y.at[pl.ds(n, late.shape[0]), :], sem_late)
    for copy in into:
        copy.start()
    rest.start()
    for a, b in zip(into, out):
        a.wait()
        b.start()
    for copy in (*out, rest):
        copy.wait()


def _tables(nc, ch):
    rate = THETA ** (-np.arange(HEAD // 2) / (HEAD // 2))
    sign = np.repeat([-1.0, 1.0], HEAD // 2)

    def both(place):
        angle = np.tile(place[:, None] * rate, (1, 2))
        return np.stack([np.cos(angle), np.sin(angle) * sign]).astype(np.float32)

    return both(np.arange(nc) * ch), both(np.arange(ch))


def solution(mesh, ch=128, tile=1792, late=1280, copy_rows=64):
    names = mesh.axis_names
    zs = mesh.shape["tp"] // 2

    def step(x, gain, wq, wk, wv, wo):
        n, d = x.shape
        heads = wq.shape[1] // HEAD
        nc, half = n // ch, d // 2
        per = 3 * (heads // 2) + 7
        sub = ch // per
        base, fine = _tables(nc, ch)
        cfg = dict(ch=ch, sub=sub, per=per, heads=heads, nc=nc, half=half, zs=zs, tile=min(tile, half), names=names)
        nb, ring, cring, nx = 8, 16, 8, 4
        dma = pltpu.SemaphoreType.DMA
        hbm, vmem = pl.BlockSpec(memory_space=pl.ANY), pl.BlockSpec(memory_space=pltpu.VMEM)
        y = pl.pallas_call(
            functools.partial(_kernel, cfg),
            out_shape=[jax.ShapeDtypeStruct((n - late, d), BF16), pltpu.VMEM((late, d), BF16)],
            in_specs=[hbm, vmem, vmem, vmem, hbm, hbm, hbm, hbm],
            out_specs=[hbm, vmem],
            scratch_shapes=[
                pltpu.VMEM((heads, n, HEAD), BF16),
                pltpu.VMEM((heads + 1, HEAD + 8, n), BF16),
                pltpu.VMEM((heads * HEAD, d), BF16),
                pltpu.VMEM((3, d, 2 * HEAD), BF16),
                pltpu.VMEM((2, ch, 2 * HEAD), F32),
                pltpu.VMEM((ch, d), BF16),
                pltpu.VMEM((ch, d), BF16),
                pltpu.VMEM((2, per, sub, half), F32),
                pltpu.VMEM((per, sub, half), BF16),
                pltpu.VMEM((ch, heads * HEAD), BF16),
                pltpu.VMEM((2 * per, sub, half), BF16),
                pltpu.VMEM((ring, sub, half), BF16),
                pltpu.VMEM((cring, sub, half), BF16),
                pltpu.VMEM((nb, sub, half), BF16),
                pltpu.VMEM((nb, sub, half), BF16),
                pltpu.VMEM((nx, sub, half), BF16),
                pltpu.VMEM((ch, HEAD), F32),
                pltpu.VMEM((ch, HEAD), F32),
                pltpu.VMEM((d // 128, 128), F32),
                dma((3, 2)), dma((heads,)), dma((ch // GROUP,)), dma((nx,)),
                dma((per,)), dma((2 * per,)), dma((ring,)), dma((cring,)), dma((ring,)),
                dma((nb,)), dma((nb,)), dma((nb,)), dma((nb,)), dma((2,)), dma((2,)),
            ],
            compiler_params=pltpu.CompilerParams(collective_id=0, has_side_effects=True, vmem_limit_bytes=KERNEL_VMEM),
            name="attention_half",
        )(x, gain.reshape(d // 128, 128), jnp.asarray(base), jnp.asarray(fine), wq, wk, wv, wo)
        blocks = (n - late) // copy_rows
        return pl.pallas_call(
            _placed,
            out_shape=jax.ShapeDtypeStruct((n, d), BF16),
            in_specs=[hbm, vmem],
            out_specs=hbm,
            scratch_shapes=[pltpu.VMEM((blocks, copy_rows, d), BF16), dma((blocks,)), dma((blocks,)), dma],
            compiler_params=pltpu.CompilerParams(vmem_limit_bytes=KERNEL_VMEM),
            name="placed",
        )(*(pltpu.with_memory_space_constraint(part, space) for part, space in zip(y, (pltpu.HBM, pltpu.VMEM))))

    tokens, columns = P("dp", None), P(None, "tp")
    return jax.shard_map(
        step,
        mesh=mesh,
        in_specs=(tokens, P(None), columns, columns, columns, P("tp", None)),
        out_specs=tokens,
        check_vma=False,
    )
```

```python
import functools

import jax
import jax.numpy as jnp
import numpy as np
from jax import lax
from jax.experimental import pallas as pl
from jax.experimental.pallas import tpu as pltpu
from jax.sharding import PartitionSpec as P

HEAD = 128
THETA = 10000
LOG2E = 1.4426950408889634
HIDDEN = -2e30
MESH = pl.DeviceIdType.MESH
BF16, F32 = jnp.bfloat16, jnp.float32
LAGS = (4, 4, 4)
GROUP = 64
KERNEL_VMEM = 46 * 2**20
WIDE = 4


def _dot(a, b, ca, cb):
    return lax.dot_general(a, b, (((ca,), (cb,)), ((), ())), preferred_element_type=F32)


def _kernel(cfg, x_hbm, gain_ref, base_ref, fine_ref, wq_hbm, wk_hbm, wv_hbm, wo_hbm, early, late,
            keys, vals, wo, wbuf, zbuf, xbuf, abuf, acc, stage, seen, d2d, up, cross, sendb, resb, xres, rotc, rots, gain,
            w_sem, wo_sem, x_sem, xres_sem, d2d_send, d2d_recv, up_recv, cross_recv, res_recv,
            send_a, send_b, send_c, send_l, part_send, part_recv):
    ch, sub, per, heads, nc, half, zs, tile, names = (cfg[k] for k in ("ch", "sub", "per", "heads", "nc", "half", "zs", "tile", "names"))
    depth = 2 * half
    units = 3 * (heads // 2) + 2
    pieces = nc * per
    e = HEAD**-0.5 * LOG2E
    lag1 = units + 3
    lag2 = lag1 + LAGS[0]
    lag3 = lag2 + LAGS[1]
    lag4 = lag3 + LAGS[2]
    ring, cring, nb, nx = up.shape[0], cross.shape[0], sendb.shape[0], xres.shape[0]
    split = early.shape[0] // sub

    dpi, t = lax.axis_index(names[0]), lax.axis_index(names[1])
    core, z = lax.rem(t, 2), lax.div(t, 2)
    inner = (z > 0) & (z < zs - 1)
    partner, above, below = (dpi, t + 1 - 2 * core), (dpi, t + 2), (dpi, t - 2)
    toward = (dpi, jnp.where(z < zs // 2, t + 2, t - 2))
    away = (dpi, jnp.where(z < zs // 2, t - 2, t + 2))
    mine = pl.multiple_of(core * half, 128)
    other = pl.multiple_of((1 - core) * half, 128)

    def rows(s):
        return pl.ds(pl.multiple_of(s * sub, sub), sub)

    def finished(s, act):
        cols = pl.ds(mine, half)
        pl.when(s < split)(lambda: act(early.at[rows(s), cols], 0))
        pl.when(s >= split)(lambda: act(late.at[rows(s - split), cols], 1))

    def remote(src, dst, send, recv, device):
        return pltpu.make_async_remote_copy(src_ref=src, dst_ref=dst, send_sem=send, recv_sem=recv, device_id=device, device_id_type=MESH)

    def x_copy(i, r):
        at = pl.ds(r * GROUP, GROUP)
        return pltpu.make_async_copy(x_hbm.at[pl.ds(pl.multiple_of(i * ch + r * GROUP, GROUP), GROUP), :], xbuf.at[at, :], x_sem.at[r])

    def for_unit(n, act):
        k, at = lax.rem(n, units), lax.rem(n, 3)
        group, kind = lax.div(k, 3), lax.rem(k, 3)

        def columns(w, h, wide):
            return w.at[:, pl.ds(pl.multiple_of(h * HEAD, HEAD), wide * HEAD)]

        @pl.when((kind == 0) & (2 * group + 1 < heads))
        def _():
            act(pltpu.make_async_copy(columns(wv_hbm, 2 * group, 2), wbuf.at[at], w_sem.at[at, 0]))

        @pl.when((kind == 0) & (2 * group + 1 == heads))
        def _():
            act(pltpu.make_async_copy(columns(wv_hbm, 2 * group, 1), wbuf.at[at, :, :HEAD], w_sem.at[at, 0]))

        @pl.when(kind > 0)
        def _():
            h = 2 * group + kind - 1
            act(pltpu.make_async_copy(columns(wq_hbm, h, 1), wbuf.at[at, :, :HEAD], w_sem.at[at, 0]))
            act(pltpu.make_async_copy(columns(wk_hbm, h, 1), wbuf.at[at, :, HEAD:], w_sem.at[at, 1]))

    def wo_copy(h):
        part = pl.ds(pl.multiple_of(h * HEAD, HEAD), HEAD)
        return pltpu.make_async_copy(wo_hbm.at[part, :], wo.at[part, :], wo_sem.at[h])

    def xres_copy(s):
        b = lax.rem(s, nx)
        return pltpu.make_async_copy(x_hbm.at[rows(s), pl.ds(mine, half)], xres.at[b], xres_sem.at[b])

    def d2d_copy(c, k):
        at = lax.rem(c, 2) * per + k
        return remote(stage.at[k], d2d.at[at], d2d_send.at[k], d2d_recv.at[at], partner)

    def up_copy(s):
        b, r = lax.rem(s, nb), lax.rem(s, ring)
        return remote(sendb.at[b], up.at[r], send_a.at[b], up_recv.at[r], toward)

    def cross_copy(s):
        b, r = lax.rem(s, nb), lax.rem(s, cring)
        return remote(sendb.at[b], cross.at[r], send_a.at[b], cross_recv.at[r], toward)

    def out_copies(s, act):
        b = lax.rem(s, nb)

        def both(at, which):
            src = at if which else resb.at[b]
            act(remote(src, at, send_b.at[b], res_recv.at[lax.rem(s, ring)], away))
            act(remote(src, at, send_c.at[b], part_recv.at[which], partner))

        finished(s, both)

    def local_copy(s):
        b = lax.rem(s, nb)
        return pltpu.make_async_copy(resb.at[b], early.at[rows(s), pl.ds(mine, half)], send_l.at[b])

    def onward_copy(s, act):
        finished(s, lambda at, which: act(remote(at, at, part_send.at[which], part_recv.at[which], partner)))

    def start(copy):
        copy.start()

    def norm(i):
        bc, bs = base_ref[0, pl.ds(i, 1), :], base_ref[1, pl.ds(i, 1), :]
        rotc[...] = bc * fine_ref[0] - bs * fine_ref[1]
        rots[...] = bs * fine_ref[0] + bc * fine_ref[1]

        def group(r, _):
            x_copy(i, r).wait()
            at = pl.ds(pl.multiple_of(r * GROUP, GROUP), GROUP)
            cols = [slice(c, c + 128) for c in range(0, depth, 128)]
            sums = [None] * 4
            for n, c in enumerate(cols):
                wide = xbuf[at, c].astype(F32)
                sums[n % 4] = wide * wide if sums[n % 4] is None else sums[n % 4] + wide * wide
            total = functools.reduce(jnp.add, [s for s in sums if s is not None])
            scale = lax.rsqrt(jnp.sum(total, -1, keepdims=True) * (1 / depth) + 1e-6)
            scale = jnp.broadcast_to(scale, (GROUP, 128))
            for n, c in enumerate(cols):
                abuf[at, c] = (xbuf[at, c].astype(F32) * scale * gain[n : n + 1, :]).astype(BF16)

        lax.fori_loop(0, ch // GROUP, group, None)

    def turned(v):
        v = v.astype(BF16).astype(F32)
        return (v * rotc[...] + pltpu.roll(v, HEAD // 2, 1) * rots[...]).astype(BF16)

    def product(n, k, cuts, between):
        if n is None:
            for do in between:
                do()
            return
        at, total = lax.rem(n, 3), None
        for lo, hi, do in zip(cuts, cuts[1:], between):
            if lo < hi:
                part = _dot(abuf[:, lo:hi], wbuf[at, lo:hi, :], 1, 0)
                total = part if total is None else total + part
            do()
        zbuf[lax.rem(k, 2)] = total

    def cut(parts):
        lead = 1 / 7 if parts > 1 else 1
        ends = [0, lead] + [lead + (1 - lead) * (j + 1) / max(parts - 1, 1) for j in range(parts - 1)]
        return [min(round(f * depth / 256) * 256, depth) for f in ends]

    def attention(n, i, k, blocks):
        h = jnp.where(lax.rem(k, 3) == 2, 2 * lax.div(k, 3), 2 * lax.div(k, 3) - 1)
        here = pl.ds(pl.multiple_of(i * ch, ch), ch)
        wide, last = WIDE * ch, blocks - 1
        state = {}

        def scores(j):
            at = slice((last - j) * wide, (last - j + 1) * wide)
            s = _dot(keys[h, at, :], state["q"], 1, 1)
            if j == 0:
                gap = lax.broadcasted_iota(jnp.int32, (wide, ch), 1) - lax.broadcasted_iota(jnp.int32, (wide, ch), 0)
                s = jnp.where(gap >= last * wide - i * ch, s, HIDDEN)
            state["s", j], state["v", j] = s, vals[h, :, at]

        def lead():
            z = zbuf[lax.rem(k + 1, 2)]
            state["q"] = turned(z[:, :HEAD])
            keys[h, here, :] = turned(z[:, HEAD:])
            scores(0)

        def block(j):
            if j + 1 < blocks:
                scores(j + 1)
            s = state.pop(("s", j))
            top = s.max(axis=0, keepdims=True)
            if j:
                top = jnp.maximum(state["top"], top)
            weights = jnp.exp2((s - top) * e).astype(BF16)
            mix = _dot(state.pop(("v", j)), weights, 1, 0)
            if j:
                mix = state["mix"] * jnp.exp2((state["top"] - top) * e) + mix
            state["top"], state["mix"] = top, mix
            if j == last:
                out = mix[:HEAD] * (1 / mix[HEAD : HEAD + 1])
                seen[:, pl.ds(pl.multiple_of(h * HEAD, HEAD), HEAD)] = out.T.astype(BF16)

        product(n, k, cut(blocks + 1), [lead, *(functools.partial(block, j) for j in range(blocks))])

    def values(n, i, k):
        def post():
            z, here = zbuf[lax.rem(k + 1, 2)], pl.ds(pl.multiple_of(i * ch, ch), ch)
            for m in range(2):
                vals[2 * lax.div(k, 3) + m, :HEAD, here] = z[:, m * HEAD : (m + 1) * HEAD].astype(BF16).T

        product(n, k, [0, depth], [post])

    def compute(i, k):
        n = i * units + k
        follows = (k > 1) & (lax.rem(k, 3) != 1)

        @pl.when(k < units)
        def _():
            @pl.when(n + 2 < nc * units)
            def _():
                for_unit(n + 2, lambda copy: copy.start())

            @pl.when((i == 0) & (k < heads))
            def _():
                wo_copy(k).start()

            for_unit(n, lambda copy: copy.wait())

            @pl.when(k == 0)
            def _():
                product(n, k, [0, depth], [lambda: None])

            @pl.when(lax.rem(k, 3) == 1)
            def _():
                values(n, i, k)

            for blocks in range(1, pl.cdiv(nc, WIDE) + 1):
                pl.when(follows & (lax.div(i, WIDE) == blocks - 1))(functools.partial(attention, n, i, k, blocks))

        for blocks in range(1, pl.cdiv(nc, WIDE) + 1):
            pl.when((k == units) & (lax.div(i, WIDE) == blocks - 1))(functools.partial(attention, None, i, k, blocks))

        @pl.when(k == units + 1)
        def _():
            @pl.when(i == 0)
            def _():
                for h in range(heads):
                    wo_copy(h).wait()

            @pl.when(i > 0)
            def _():
                for j in range(per):
                    d2d_copy(i - 1, j).wait_send()

            def theirs(n, _):
                at = pl.multiple_of(n * tile, tile)
                part = _dot(seen[...], wo[:, pl.ds(pl.multiple_of(other + at, 128), tile)], 1, 0)
                stage[:, :, pl.ds(at, tile)] = part.astype(BF16).reshape(per, sub, tile)

            lax.fori_loop(0, half // tile, theirs, None)
            for j in range(per):
                d2d_copy(i, j).start()

        @pl.when(k == units + 2)
        def _():
            def ours(n, _):
                at = pl.multiple_of(n * tile, tile)
                part = _dot(seen[...], wo[:, pl.ds(pl.multiple_of(mine + at, 128), tile)], 1, 0)
                acc[lax.rem(i, 2), :, :, pl.ds(at, tile)] = part.reshape(per, sub, tile)

            lax.fori_loop(0, half // tile, ours, None)

        @pl.when((k == units + 3) & (i + 1 < nc))
        def _():
            norm(i + 1)

            @pl.when(i + 2 < nc)
            def _():
                for r in range(ch // GROUP):
                    x_copy(i + 2, r).start()

    def valid(s):
        return (s >= 0) & (s < pieces)

    def sum_of(s):
        return acc.at[lax.rem(lax.div(s, per), 2), lax.rem(s, per)]

    def pair(s, _):
        at, ours = lax.rem(s, 2 * per), sum_of(s)
        d2d_copy(lax.div(s, per), lax.rem(s, per)).wait_recv()

        @pl.when(inner)
        def _():
            ours[...] = ours[...] + d2d[at].astype(F32)

        @pl.when(jnp.logical_not(inner))
        def _():
            @pl.when(s >= nb)
            def _():
                up_copy(s - nb).wait_send()

            sendb[lax.rem(s, nb)] = (ours[...] + d2d[at].astype(F32)).astype(BF16)
            up_copy(s).start()

    def relay(s):
        up_copy(s).wait_recv()

        @pl.when(s >= nb)
        def _():
            cross_copy(s - nb).wait_send()

        sendb[lax.rem(s, nb)] = (sum_of(s)[...] + up[lax.rem(s, ring)].astype(F32)).astype(BF16)
        cross_copy(s).start()

    def sent(s):
        out_copies(s, lambda copy: copy.wait_send())
        pl.when(s < split)(lambda: local_copy(s).wait())

    def finish(s):
        b = lax.rem(s, nb)
        cross_copy(s).wait_recv()
        xres_copy(s).wait()

        @pl.when(s >= nb)
        def _():
            sent(s - nb)

        total = sendb[b].astype(F32) + cross[lax.rem(s, cring)].astype(F32)
        y = (xres[lax.rem(s, nx)].astype(F32) + total).astype(BF16)

        @pl.when(s < split)
        def _():
            resb[b] = y
            local_copy(s).start()

        @pl.when(s >= split)
        def _():
            late[rows(s - split), pl.ds(mine, half)] = y

        out_copies(s, start)

    def arrived(s):
        b = lax.rem(s, ring)
        finished(s, lambda at, _: remote(at, at, part_send.at[0], res_recv.at[b], away).wait_recv())
        onward_copy(s, start)

    for r in range(ch // GROUP):
        x_copy(0, r).start()
    for n in range(2):
        for_unit(n, lambda copy: copy.start())
    barrier = pltpu.get_barrier_semaphore()
    pl.semaphore_signal(barrier, inc=1, device_id=partner, device_id_type=MESH)

    @pl.when(z < zs - 1)
    def _():
        pl.semaphore_signal(barrier, inc=1, device_id=above, device_id_type=MESH)

    @pl.when(z > 0)
    def _():
        pl.semaphore_signal(barrier, inc=1, device_id=below, device_id_type=MESH)

    def clear(h, _):
        keys[h] = jnp.zeros(keys.shape[1:], BF16)
        vals[h, :HEAD, :] = jnp.zeros((HEAD, vals.shape[2]), BF16)
        vals[h, HEAD:, :] = jnp.ones((vals.shape[1] - HEAD, vals.shape[2]), BF16)

    lax.fori_loop(0, heads, clear, None)
    gain[...] = gain_ref[...].astype(F32)
    norm(0)
    for r in range(ch // GROUP):
        x_copy(1, r).start()
    pl.semaphore_wait(barrier, 1 + jnp.where(z < zs - 1, 1, 0) + jnp.where(z > 0, 1, 0))

    def slot(g, _):
        i, k = lax.div(g, per), lax.rem(g, per)

        @pl.when(jnp.logical_not(inner) & valid(g - lag4))
        def _():
            arrived(g - lag4)

        @pl.when(inner & valid(g - lag3))
        def _():
            finish(g - lag3)

        @pl.when(inner & valid(g - lag3 + 3))
        def _():
            xres_copy(g - lag3 + 3).start()

        @pl.when(inner & valid(g - lag2))
        def _():
            relay(g - lag2)

        first = g - lag1 + jnp.where(k == lag1 - 1, 1, 0)
        end = g - lag1 + jnp.where(k == lag1 - 2, 2, 1)
        lax.fori_loop(jnp.clip(first, 0, pieces), jnp.clip(end, 0, pieces), pair, None)
        pl.when(i < nc)(lambda: compute(i, k))

    lax.fori_loop(0, pieces + lag4, slot, None)

    for j in range(per):
        d2d_copy(nc - 1, j).wait_send()
    for s in range(pieces - nb, pieces):
        up_copy(s).wait_send()

    @pl.when(inner)
    def _():
        for s in range(pieces - nb, pieces):
            sent(s)

    for which, y in enumerate((early, late)):
        ours, theirs = y.at[:, pl.ds(mine, half)], y.at[:, pl.ds(other, half)]
        pl.when(jnp.logical_not(inner))(remote(ours, ours, part_send.at[which], part_recv.at[which], partner).wait_send)
        remote(theirs, theirs, part_send.at[which], part_recv.at[which], partner).wait_recv()


def _placed(early, late, y, buf, sem_in, sem_out, sem_late):
    blocks, size, n = buf.shape[0], buf.shape[1], early.shape[0]
    into = [pltpu.make_async_copy(early.at[pl.ds(r * size, size), :], buf.at[r], sem_in.at[r]) for r in range(blocks)]
    out = [pltpu.make_async_copy(buf.at[r], y.at[pl.ds(r * size, size), :], sem_out.at[r]) for r in range(blocks)]
    rest = pltpu.make_async_copy(late, y.at[pl.ds(n, late.shape[0]), :], sem_late)
    for copy in into:
        copy.start()
    rest.start()
    for a, b in zip(into, out):
        a.wait()
        b.start()
    for copy in (*out, rest):
        copy.wait()


def _tables(nc, ch):
    rate = THETA ** (-np.arange(HEAD // 2) / (HEAD // 2))
    sign = np.repeat([-1.0, 1.0], HEAD // 2)

    def both(place):
        angle = np.tile(place[:, None] * rate, (1, 2))
        return np.stack([np.cos(angle), np.sin(angle) * sign]).astype(np.float32)

    return both(np.arange(nc) * ch), both(np.arange(ch))


def solution(mesh, ch=128, tile=1792, late=1280, copy_rows=64):
    names = mesh.axis_names
    zs = mesh.shape["tp"] // 2

    def step(x, gain, wq, wk, wv, wo):
        n, d = x.shape
        heads = wq.shape[1] // HEAD
        nc, half = n // ch, d // 2
        per = 3 * (heads // 2) + 7
        sub = ch // per
        base, fine = _tables(nc, ch)
        cfg = dict(ch=ch, sub=sub, per=per, heads=heads, nc=nc, half=half, zs=zs, tile=min(tile, half), names=names)
        nb, ring, cring, nx = 8, 16, 8, 4
        dma = pltpu.SemaphoreType.DMA
        hbm, vmem = pl.BlockSpec(memory_space=pl.ANY), pl.BlockSpec(memory_space=pltpu.VMEM)
        y = pl.pallas_call(
            functools.partial(_kernel, cfg),
            out_shape=[jax.ShapeDtypeStruct((n - late, d), BF16), pltpu.VMEM((late, d), BF16)],
            in_specs=[hbm, vmem, vmem, vmem, hbm, hbm, hbm, hbm],
            out_specs=[hbm, vmem],
            scratch_shapes=[
                pltpu.VMEM((heads, n, HEAD), BF16),
                pltpu.VMEM((heads + 1, HEAD + 8, n), BF16),
                pltpu.VMEM((heads * HEAD, d), BF16),
                pltpu.VMEM((3, d, 2 * HEAD), BF16),
                pltpu.VMEM((2, ch, 2 * HEAD), F32),
                pltpu.VMEM((ch, d), BF16),
                pltpu.VMEM((ch, d), BF16),
                pltpu.VMEM((2, per, sub, half), F32),
                pltpu.VMEM((per, sub, half), BF16),
                pltpu.VMEM((ch, heads * HEAD), BF16),
                pltpu.VMEM((2 * per, sub, half), BF16),
                pltpu.VMEM((ring, sub, half), BF16),
                pltpu.VMEM((cring, sub, half), BF16),
                pltpu.VMEM((nb, sub, half), BF16),
                pltpu.VMEM((nb, sub, half), BF16),
                pltpu.VMEM((nx, sub, half), BF16),
                pltpu.VMEM((ch, HEAD), F32),
                pltpu.VMEM((ch, HEAD), F32),
                pltpu.VMEM((d // 128, 128), F32),
                dma((3, 2)), dma((heads,)), dma((ch // GROUP,)), dma((nx,)),
                dma((per,)), dma((2 * per,)), dma((ring,)), dma((cring,)), dma((ring,)),
                dma((nb,)), dma((nb,)), dma((nb,)), dma((nb,)), dma((2,)), dma((2,)),
            ],
            compiler_params=pltpu.CompilerParams(collective_id=0, has_side_effects=True, vmem_limit_bytes=KERNEL_VMEM),
            name="attention_half",
        )(x, gain.reshape(d // 128, 128), jnp.asarray(base), jnp.asarray(fine), wq, wk, wv, wo)
        blocks = (n - late) // copy_rows
        return pl.pallas_call(
            _placed,
            out_shape=jax.ShapeDtypeStruct((n, d), BF16),
            in_specs=[hbm, vmem],
            out_specs=hbm,
            scratch_shapes=[pltpu.VMEM((blocks, copy_rows, d), BF16), dma((blocks,)), dma((blocks,)), dma],
            compiler_params=pltpu.CompilerParams(vmem_limit_bytes=KERNEL_VMEM),
            name="placed",
        )(*(pltpu.with_memory_space_constraint(part, space) for part, space in zip(y, (pltpu.HBM, pltpu.VMEM))))

    tokens, columns = P("dp", None), P(None, "tp")
    return jax.shard_map(
        step,
        mesh=mesh,
        in_specs=(tokens, P(None), columns, columns, columns, P("tp", None)),
        out_specs=tokens,
        check_vma=False,
    )
```

```python
import functools

import jax
import jax.numpy as jnp
import numpy as np
from jax import lax
from jax.experimental import pallas as pl
from jax.experimental.pallas import tpu as pltpu
from jax.sharding import PartitionSpec as P

HEAD = 128
THETA = 10000
LOG2E = 1.4426950408889634
HIDDEN = -2e30
MESH = pl.DeviceIdType.MESH
BF16, F32 = jnp.bfloat16, jnp.float32
LAGS = (3, 3, 3)
GROUP = 64
KERNEL_VMEM = 46 * 2**20
WIDE = 4


def _dot(a, b, ca, cb):
    return lax.dot_general(a, b, (((ca,), (cb,)), ((), ())), preferred_element_type=F32)


def _kernel(cfg, x_hbm, gain_ref, base_ref, fine_ref, wq_hbm, wk_hbm, wv_hbm, wo_hbm, early, late,
            keys, vals, wo, wbuf, zbuf, xbuf, abuf, acc, stage, seen, d2d, up, cross, sendb, resb, xres, rotc, rots, gain,
            w_sem, wo_sem, x_sem, xres_sem, d2d_send, d2d_recv, up_recv, cross_recv, res_recv,
            send_a, send_b, send_c, send_l, part_send, part_recv):
    ch, sub, per, heads, nc, half, zs, tile, names = (cfg[k] for k in ("ch", "sub", "per", "heads", "nc", "half", "zs", "tile", "names"))
    depth = 2 * half
    units = 3 * (heads // 2) + 2
    batch = per // 2
    pieces = nc * batch
    e = HEAD**-0.5 * LOG2E
    lag1 = (units + 4) // 2
    lag2 = lag1 + LAGS[0]
    lag3 = lag2 + LAGS[1]
    lag4 = lag3 + LAGS[2]
    ring, cring, nb, nx = up.shape[0], cross.shape[0], sendb.shape[0], xres.shape[0]
    split = early.shape[0] // sub

    dpi, t = lax.axis_index(names[0]), lax.axis_index(names[1])
    core, z = lax.rem(t, 2), lax.div(t, 2)
    inner = (z > 0) & (z < zs - 1)
    partner, above, below = (dpi, t + 1 - 2 * core), (dpi, t + 2), (dpi, t - 2)
    toward = (dpi, jnp.where(z < zs // 2, t + 2, t - 2))
    away = (dpi, jnp.where(z < zs // 2, t - 2, t + 2))
    mine = pl.multiple_of(core * half, 128)
    other = pl.multiple_of((1 - core) * half, 128)

    def rows(s):
        return pl.ds(pl.multiple_of(s * sub, sub), sub)

    def finished(s, act):
        cols = pl.ds(mine, half)
        pl.when(s < split)(lambda: act(early.at[rows(s), cols], 0))
        pl.when(s >= split)(lambda: act(late.at[rows(s - split), cols], 1))

    def remote(src, dst, send, recv, device):
        return pltpu.make_async_remote_copy(src_ref=src, dst_ref=dst, send_sem=send, recv_sem=recv, device_id=device, device_id_type=MESH)

    def x_copy(i, r):
        at = pl.ds(r * GROUP, GROUP)
        return pltpu.make_async_copy(x_hbm.at[pl.ds(pl.multiple_of(i * ch + r * GROUP, GROUP), GROUP), :], xbuf.at[at, :], x_sem.at[r])

    def for_unit(n, act):
        k, at = lax.rem(n, units), lax.rem(n, 3)
        group, kind = lax.div(k, 3), lax.rem(k, 3)

        def columns(w, h, wide):
            return w.at[:, pl.ds(pl.multiple_of(h * HEAD, HEAD), wide * HEAD)]

        @pl.when((kind == 0) & (2 * group + 1 < heads))
        def _():
            act(pltpu.make_async_copy(columns(wv_hbm, 2 * group, 2), wbuf.at[at], w_sem.at[at, 0]))

        @pl.when((kind == 0) & (2 * group + 1 == heads))
        def _():
            act(pltpu.make_async_copy(columns(wv_hbm, 2 * group, 1), wbuf.at[at, :, :HEAD], w_sem.at[at, 0]))

        @pl.when(kind > 0)
        def _():
            h = 2 * group + kind - 1
            act(pltpu.make_async_copy(columns(wq_hbm, h, 1), wbuf.at[at, :, :HEAD], w_sem.at[at, 0]))
            act(pltpu.make_async_copy(columns(wk_hbm, h, 1), wbuf.at[at, :, HEAD:], w_sem.at[at, 1]))

    tiles = half // tile

    def wo_copy(m):
        at = jnp.where(m < tiles, other + m * tile, mine + (m - tiles) * tile)
        part = pl.ds(pl.multiple_of(at, 128), tile)
        return pltpu.make_async_copy(wo_hbm.at[:, part], wo.at[:, part], wo_sem.at[m])

    def xres_copy(s):
        b = lax.rem(s, nx)
        return pltpu.make_async_copy(x_hbm.at[rows(s), pl.ds(mine, half)], xres.at[b], xres_sem.at[b])

    def d2d_copy(c, k):
        at = lax.rem(c, 2) * batch + k
        return remote(stage.at[k], d2d.at[at], d2d_send.at[k], d2d_recv.at[at], partner)

    def up_copy(s):
        b, r = lax.rem(s, nb), lax.rem(s, ring)
        return remote(sendb.at[b], up.at[r], send_a.at[b], up_recv.at[r], toward)

    def cross_copy(s):
        b, r = lax.rem(s, nb), lax.rem(s, cring)
        return remote(sendb.at[b], cross.at[r], send_a.at[b], cross_recv.at[r], toward)

    def out_copies(s, act):
        b = lax.rem(s, nb)

        def both(at, which):
            src = at if which else resb.at[b]
            act(remote(src, at, send_b.at[b], res_recv.at[lax.rem(s, ring)], away))
            act(remote(src, at, send_c.at[b], part_recv.at[which], partner))

        finished(s, both)

    def local_copy(s):
        b = lax.rem(s, nb)
        return pltpu.make_async_copy(resb.at[b], early.at[rows(s), pl.ds(mine, half)], send_l.at[b])

    def onward_copy(s, act):
        finished(s, lambda at, which: act(remote(at, at, part_send.at[which], part_recv.at[which], partner)))

    def start(copy):
        copy.start()

    def norm(i):
        bc, bs = base_ref[0, pl.ds(i, 1), :], base_ref[1, pl.ds(i, 1), :]
        rotc[...] = bc * fine_ref[0] - bs * fine_ref[1]
        rots[...] = bs * fine_ref[0] + bc * fine_ref[1]

        def group(r, _):
            x_copy(i, r).wait()
            at = pl.ds(pl.multiple_of(r * GROUP, GROUP), GROUP)
            cols = [slice(c, c + 128) for c in range(0, depth, 128)]
            sums = [None] * 4
            for n, c in enumerate(cols):
                wide = xbuf[at, c].astype(F32)
                sums[n % 4] = wide * wide if sums[n % 4] is None else sums[n % 4] + wide * wide
            total = functools.reduce(jnp.add, [s for s in sums if s is not None])
            scale = lax.rsqrt(jnp.sum(total, -1, keepdims=True) * (1 / depth) + 1e-6)
            scale = jnp.broadcast_to(scale, (GROUP, 128))
            for c in cols:
                abuf[at, c] = (xbuf[at, c].astype(F32) * scale * gain[:, c]).astype(BF16)

        lax.fori_loop(0, ch // GROUP, group, None)

    def turned(v):
        v = v.astype(BF16).astype(F32)
        return (v * rotc[...] + pltpu.roll(v, HEAD // 2, 1) * rots[...]).astype(BF16)

    def product(n, k, cuts, between):
        if n is None:
            for do in between:
                do()
            return
        at, total = lax.rem(n, 3), None
        for lo, hi, do in zip(cuts, cuts[1:], between):
            if lo < hi:
                part = _dot(abuf[:, lo:hi], wbuf[at, lo:hi, :], 1, 0)
                total = part if total is None else total + part
            do()
        zbuf[lax.rem(k, 2)] = total

    def cut(parts):
        lead = 1 / 7 if parts > 1 else 1
        ends = [0, lead] + [lead + (1 - lead) * (j + 1) / max(parts - 1, 1) for j in range(parts - 1)]
        return [min(round(f * depth / 256) * 256, depth) for f in ends]

    def attention(n, i, k, blocks):
        h = jnp.where(lax.rem(k, 3) == 2, 2 * lax.div(k, 3), 2 * lax.div(k, 3) - 1)
        here = pl.ds(pl.multiple_of(i * ch, ch), ch)
        wide, last = WIDE * ch, blocks - 1
        state = {}

        def scores(j):
            at = slice((last - j) * wide, (last - j + 1) * wide)
            s = _dot(keys[h, at, :], state["q"], 1, 1)
            if j == 0:
                gap = lax.broadcasted_iota(jnp.int32, (wide, ch), 1) - lax.broadcasted_iota(jnp.int32, (wide, ch), 0)
                s = jnp.where(gap >= last * wide - i * ch, s, HIDDEN)
            state["s", j], state["v", j] = s, vals[h, :, at]

        def lead():
            z = zbuf[lax.rem(k + 1, 2)]
            state["q"] = turned(z[:, :HEAD])
            keys[h, here, :] = turned(z[:, HEAD:])
            scores(0)

        def block(j):
            if j + 1 < blocks:
                scores(j + 1)
            s = state.pop(("s", j))
            top = s.max(axis=0, keepdims=True)
            if j:
                top = jnp.maximum(state["top"], top)
            weights = jnp.exp2((s - top) * e).astype(BF16)
            mix = _dot(state.pop(("v", j)), weights, 1, 0)
            if j:
                mix = state["mix"] * jnp.exp2((state["top"] - top) * e) + mix
            state["top"], state["mix"] = top, mix
            if j == last:
                out = mix[:HEAD] * (1 / mix[HEAD : HEAD + 1])
                seen[:, pl.ds(pl.multiple_of(h * HEAD, HEAD), HEAD)] = out.T.astype(BF16)

        product(n, k, cut(blocks + 1), [lead, *(functools.partial(block, j) for j in range(blocks))])

    def values(n, i, k):
        def post():
            z, here = zbuf[lax.rem(k + 1, 2)], pl.ds(pl.multiple_of(i * ch, ch), ch)
            for m in range(2):
                vals[2 * lax.div(k, 3) + m, :HEAD, here] = z[:, m * HEAD : (m + 1) * HEAD].astype(BF16).T

        product(n, k, [0, depth], [post])

    def compute(i, k):
        n = i * units + k
        follows = (k > 1) & (lax.rem(k, 3) != 1)

        @pl.when(k < units)
        def _():
            @pl.when((n + 2 < nc * units) & ((n + 2 < units) | (n >= units)))
            def _():
                for_unit(n + 2, start)

            @pl.when(n == units - 2)
            def _():
                for m in range(2 * tiles):
                    wo_copy(m).start()

            for_unit(n, lambda copy: copy.wait())

            @pl.when(k == 0)
            def _():
                product(n, k, [0, depth], [lambda: None])

            @pl.when(lax.rem(k, 3) == 1)
            def _():
                values(n, i, k)

            for blocks in range(1, pl.cdiv(nc, WIDE) + 1):
                pl.when(follows & (lax.div(i, WIDE) == blocks - 1))(functools.partial(attention, n, i, k, blocks))

        for blocks in range(1, pl.cdiv(nc, WIDE) + 1):
            pl.when((k == units) & (lax.div(i, WIDE) == blocks - 1))(functools.partial(attention, None, i, k, blocks))

        @pl.when(k == units + 1)
        def _():
            @pl.when(i == 0)
            def _():
                for n in range(units, units + 2):
                    for_unit(n, start)

            @pl.when(i > 0)
            def _():
                for j in range(batch):
                    d2d_copy(i - 1, j).wait_send()

            def theirs(n, _):
                at = pl.multiple_of(n * tile, tile)
                pl.when(i == 0)(lambda: wo_copy(n).wait())
                part = _dot(seen[...], wo[:, pl.ds(pl.multiple_of(other + at, 128), tile)], 1, 0)
                stage[:, :, pl.ds(at, tile)] = part.astype(BF16).reshape(batch, sub, tile)

            lax.fori_loop(0, half // tile, theirs, None)
            for j in range(batch):
                d2d_copy(i, j).start()

        @pl.when(k == units + 2)
        def _():
            def ours(n, _):
                at = pl.multiple_of(n * tile, tile)
                pl.when(i == 0)(lambda: wo_copy(tiles + n).wait())
                part = _dot(seen[...], wo[:, pl.ds(pl.multiple_of(mine + at, 128), tile)], 1, 0)
                acc[lax.rem(i, 2), :, :, pl.ds(at, tile)] = part.reshape(batch, sub, tile)

            lax.fori_loop(0, half // tile, ours, None)

        @pl.when((k == units + 3) & (i + 1 < nc))
        def _():
            norm(i + 1)

            @pl.when(i + 2 < nc)
            def _():
                for r in range(ch // GROUP):
                    x_copy(i + 2, r).start()

    def valid(s):
        return (s >= 0) & (s < pieces)

    def sum_of(s):
        return acc.at[lax.rem(lax.div(s, batch), 2), lax.rem(s, batch)]

    def pair(s):
        at, ours = lax.rem(s, 2 * batch), sum_of(s)
        d2d_copy(lax.div(s, batch), lax.rem(s, batch)).wait_recv()

        @pl.when(inner)
        def _():
            ours[...] = ours[...] + d2d[at].astype(F32)

        @pl.when(jnp.logical_not(inner))
        def _():
            @pl.when(s >= nb)
            def _():
                up_copy(s - nb).wait_send()

            sendb[lax.rem(s, nb)] = (ours[...] + d2d[at].astype(F32)).astype(BF16)
            up_copy(s).start()

    def relay(s):
        up_copy(s).wait_recv()

        @pl.when(s >= nb)
        def _():
            cross_copy(s - nb).wait_send()

        sendb[lax.rem(s, nb)] = (sum_of(s)[...] + up[lax.rem(s, ring)].astype(F32)).astype(BF16)
        cross_copy(s).start()

    def sent(s):
        out_copies(s, lambda copy: copy.wait_send())
        pl.when(s < split)(lambda: local_copy(s).wait())

    def finish(s):
        b = lax.rem(s, nb)
        cross_copy(s).wait_recv()
        xres_copy(s).wait()

        @pl.when(s >= nb)
        def _():
            sent(s - nb)

        total = sendb[b].astype(F32) + cross[lax.rem(s, cring)].astype(F32)
        y = (xres[lax.rem(s, nx)].astype(F32) + total).astype(BF16)

        @pl.when(s < split)
        def _():
            resb[b] = y
            local_copy(s).start()

        @pl.when(s >= split)
        def _():
            late[rows(s - split), pl.ds(mine, half)] = y

        out_copies(s, start)

    def arrived(s):
        b = lax.rem(s, ring)
        finished(s, lambda at, _: remote(at, at, part_send.at[0], res_recv.at[b], away).wait_recv())
        onward_copy(s, start)

    for r in range(ch // GROUP):
        x_copy(0, r).start()
    for n in range(2):
        for_unit(n, lambda copy: copy.start())
    barrier = pltpu.get_barrier_semaphore()
    pl.semaphore_signal(barrier, inc=1, device_id=partner, device_id_type=MESH)

    @pl.when(z < zs - 1)
    def _():
        pl.semaphore_signal(barrier, inc=1, device_id=above, device_id_type=MESH)

    @pl.when(z > 0)
    def _():
        pl.semaphore_signal(barrier, inc=1, device_id=below, device_id_type=MESH)

    def clear(h, _):
        keys[h] = jnp.zeros(keys.shape[1:], BF16)
        vals[h, :HEAD, :] = jnp.zeros((HEAD, vals.shape[2]), BF16)
        vals[h, HEAD:, :] = jnp.ones((vals.shape[1] - HEAD, vals.shape[2]), BF16)

    lax.fori_loop(0, heads, clear, None)
    for n in range(depth // 128):
        gain[:, n * 128 : (n + 1) * 128] = gain_ref[n : n + 1, :].astype(F32)
    norm(0)
    for r in range(ch // GROUP):
        x_copy(1, r).start()
    pl.semaphore_wait(barrier, 1 + jnp.where(z < zs - 1, 1, 0) + jnp.where(z > 0, 1, 0))

    def serve(g):
        @pl.when(jnp.logical_not(inner) & valid(g - lag4))
        def _():
            arrived(g - lag4)

        @pl.when(inner & valid(g - lag3))
        def _():
            finish(g - lag3)

        @pl.when(inner & valid(g - lag3 + 2))
        def _():
            xres_copy(g - lag3 + 2).start()

        @pl.when(inner & valid(g - lag2))
        def _():
            relay(g - lag2)

        @pl.when(valid(g - lag1))
        def _():
            pair(g - lag1)

    def slot(g, _):
        i, k = lax.div(g, per), lax.rem(g, per)
        pl.when(lax.rem(g, 2) == 0)(lambda: serve(lax.div(g, 2)))
        pl.when(i < nc)(lambda: compute(i, k))

    lax.fori_loop(0, 2 * (pieces + lag4), slot, None)

    for j in range(batch):
        d2d_copy(nc - 1, j).wait_send()
    for s in range(pieces - nb, pieces):
        up_copy(s).wait_send()

    @pl.when(inner)
    def _():
        for s in range(pieces - nb, pieces):
            sent(s)

    for which, y in enumerate((early, late)):
        ours, theirs = y.at[:, pl.ds(mine, half)], y.at[:, pl.ds(other, half)]
        pl.when(jnp.logical_not(inner))(remote(ours, ours, part_send.at[which], part_recv.at[which], partner).wait_send)
        remote(theirs, theirs, part_send.at[which], part_recv.at[which], partner).wait_recv()


def _placed(early, late, y, buf, sem_in, sem_out, sem_late):
    blocks, size, n = buf.shape[0], buf.shape[1], early.shape[0]
    into = [pltpu.make_async_copy(early.at[pl.ds(r * size, size), :], buf.at[r], sem_in.at[r]) for r in range(blocks)]
    out = [pltpu.make_async_copy(buf.at[r], y.at[pl.ds(r * size, size), :], sem_out.at[r]) for r in range(blocks)]
    rest = pltpu.make_async_copy(late, y.at[pl.ds(n, late.shape[0]), :], sem_late)
    for copy in into:
        copy.start()
    rest.start()
    for a, b in zip(into, out):
        a.wait()
        b.start()
    for copy in (*out, rest):
        copy.wait()


def _tables(nc, ch):
    rate = THETA ** (-np.arange(HEAD // 2) / (HEAD // 2))
    sign = np.repeat([-1.0, 1.0], HEAD // 2)

    def both(place):
        angle = np.tile(place[:, None] * rate, (1, 2))
        return np.stack([np.cos(angle), np.sin(angle) * sign]).astype(np.float32)

    return both(np.arange(nc) * ch), both(np.arange(ch))


def solution(mesh, ch=128, tile=1792, late=1280, copy_rows=64):
    names = mesh.axis_names
    zs = mesh.shape["tp"] // 2

    def step(x, gain, wq, wk, wv, wo):
        n, d = x.shape
        heads = wq.shape[1] // HEAD
        nc, half = n // ch, d // 2
        per = 3 * (heads // 2) + 7
        sub = 2 * ch // per
        base, fine = _tables(nc, ch)
        cfg = dict(ch=ch, sub=sub, per=per, heads=heads, nc=nc, half=half, zs=zs, tile=min(tile, half), names=names)
        wide, batch = min(tile, half), per // 2
        nb, ring, cring, nx = 6, 10, 8, 4
        dma = pltpu.SemaphoreType.DMA
        hbm, vmem = pl.BlockSpec(memory_space=pl.ANY), pl.BlockSpec(memory_space=pltpu.VMEM)
        y = pl.pallas_call(
            functools.partial(_kernel, cfg),
            out_shape=[jax.ShapeDtypeStruct((n - late, d), BF16), pltpu.VMEM((late, d), BF16)],
            in_specs=[hbm, vmem, vmem, vmem, hbm, hbm, hbm, hbm],
            out_specs=[hbm, vmem],
            scratch_shapes=[
                pltpu.VMEM((heads, n, HEAD), BF16),
                pltpu.VMEM((heads + 1, HEAD + 8, n), BF16),
                pltpu.VMEM((heads * HEAD, d), BF16),
                pltpu.VMEM((3, d, 2 * HEAD), BF16),
                pltpu.VMEM((2, ch, 2 * HEAD), F32),
                pltpu.VMEM((ch, d), BF16),
                pltpu.VMEM((ch, d), BF16),
                pltpu.VMEM((2, batch, sub, half), F32),
                pltpu.VMEM((batch, sub, half), BF16),
                pltpu.VMEM((ch, heads * HEAD), BF16),
                pltpu.VMEM((2 * batch, sub, half), BF16),
                pltpu.VMEM((ring, sub, half), BF16),
                pltpu.VMEM((cring, sub, half), BF16),
                pltpu.VMEM((nb, sub, half), BF16),
                pltpu.VMEM((nb, sub, half), BF16),
                pltpu.VMEM((nx, sub, half), BF16),
                pltpu.VMEM((ch, HEAD), F32),
                pltpu.VMEM((ch, HEAD), F32),
                pltpu.VMEM((1, d), F32),
                dma((3, 2)), dma((2 * half // wide,)), dma((ch // GROUP,)), dma((nx,)),
                dma((batch,)), dma((2 * batch,)), dma((ring,)), dma((cring,)), dma((ring,)),
                dma((nb,)), dma((nb,)), dma((nb,)), dma((nb,)), dma((2,)), dma((2,)),
            ],
            compiler_params=pltpu.CompilerParams(collective_id=0, has_side_effects=True, vmem_limit_bytes=KERNEL_VMEM),
            name="attention_half",
        )(x, gain.reshape(d // 128, 128), jnp.asarray(base), jnp.asarray(fine), wq, wk, wv, wo)
        blocks = (n - late) // copy_rows
        return pl.pallas_call(
            _placed,
            out_shape=jax.ShapeDtypeStruct((n, d), BF16),
            in_specs=[hbm, vmem],
            out_specs=hbm,
            scratch_shapes=[pltpu.VMEM((blocks, copy_rows, d), BF16), dma((blocks,)), dma((blocks,)), dma],
            compiler_params=pltpu.CompilerParams(vmem_limit_bytes=KERNEL_VMEM),
            name="placed",
        )(*(pltpu.with_memory_space_constraint(part, space) for part, space in zip(y, (pltpu.HBM, pltpu.VMEM))))

    tokens, columns = P("dp", None), P(None, "tp")
    return jax.shard_map(
        step,
        mesh=mesh,
        in_specs=(tokens, P(None), columns, columns, columns, P("tp", None)),
        out_specs=tokens,
        check_vma=False,
    )
```

```python
import functools

import jax
import jax.numpy as jnp
import numpy as np
from jax import lax
from jax.experimental import pallas as pl
from jax.experimental.pallas import tpu as pltpu
from jax.sharding import PartitionSpec as P

HEAD = 128
THETA = 10000
LOG2E = 1.4426950408889634
HIDDEN = -2e30
MESH = pl.DeviceIdType.MESH
BF16, F32 = jnp.bfloat16, jnp.float32
LAGS, GROWN, EARLY = 2, 1, 12
GROUP = 64
KERNEL_VMEM = 37_500_000
WIDE = 4


def _dot(a, b, ca, cb):
    return lax.dot_general(a, b, (((ca,), (cb,)), ((), ())), preferred_element_type=F32)


def _kernel(cfg, x_hbm, gain_ref, base_ref, fine_ref, wq_hbm, wk_hbm, wv_hbm, wo_hbm, early, y_ref,
            keys, vals, wbuf, zbuf, xbuf, abuf, acc, stage, seen, d2d, up, cross, sendb, resb, xres, rotc, rots, gain,
            w_sem, wo_sem, x_sem, xres_sem, d2d_send, d2d_recv, up_recv, cross_recv, res_recv,
            send_a, send_b, send_c, send_l, part_send, part_recv, home_sem):
    ch, sub, per, heads, nc, half, zs, tile, names = (cfg[k] for k in ("ch", "sub", "per", "heads", "nc", "half", "zs", "tile", "names"))
    depth = 2 * half
    units = 3 * (heads // 2) + 2
    batch = per // 2
    pieces = nc * batch
    e = HEAD**-0.5 * LOG2E
    lag1 = (units + 4) // 2
    turn = lag1 + EARLY
    last_lag = lag1 + 3 * (LAGS + GROWN)
    ring, cring, nb, nx = up.shape[0], cross.shape[0], sendb.shape[0], xres.shape[0]
    wo, split = y_ref.at[: early.shape[0], :], early.shape[0] // sub

    dpi, t = lax.axis_index(names[0]), lax.axis_index(names[1])
    core, z = lax.rem(t, 2), lax.div(t, 2)
    inner = (z > 0) & (z < zs - 1)
    partner, above, below = (dpi, t + 1 - 2 * core), (dpi, t + 2), (dpi, t - 2)
    toward = (dpi, jnp.where(z < zs // 2, t + 2, t - 2))
    away = (dpi, jnp.where(z < zs // 2, t - 2, t + 2))
    mine = pl.multiple_of(core * half, 128)
    other = pl.multiple_of((1 - core) * half, 128)

    def rows(s):
        return pl.ds(pl.multiple_of(s * sub, sub), sub)

    def finished(s, act):
        cols = pl.ds(mine, half)
        pl.when(s < split)(lambda: act(early.at[rows(s), cols], 0))
        pl.when(s >= split)(lambda: act(y_ref.at[rows(s), cols], 1))

    def remote(src, dst, send, recv, device):
        return pltpu.make_async_remote_copy(src_ref=src, dst_ref=dst, send_sem=send, recv_sem=recv, device_id=device, device_id_type=MESH)

    def x_copy(i, r):
        at = pl.ds(r * GROUP, GROUP)
        return pltpu.make_async_copy(x_hbm.at[pl.ds(pl.multiple_of(i * ch + r * GROUP, GROUP), GROUP), :], xbuf.at[at, :], x_sem.at[r])

    def for_unit(n, act):
        k, at = lax.rem(n, units), lax.rem(n, 3)
        group, kind = lax.div(k, 3), lax.rem(k, 3)

        def columns(w, h, wide):
            return w.at[:, pl.ds(pl.multiple_of(h * HEAD, HEAD), wide * HEAD)]

        @pl.when((kind == 0) & (2 * group + 1 < heads))
        def _():
            act(pltpu.make_async_copy(columns(wv_hbm, 2 * group, 2), wbuf.at[at], w_sem.at[at, 0]))

        @pl.when((kind == 0) & (2 * group + 1 == heads))
        def _():
            act(pltpu.make_async_copy(columns(wv_hbm, 2 * group, 1), wbuf.at[at, :, :HEAD], w_sem.at[at, 0]))

        @pl.when(kind > 0)
        def _():
            h = 2 * group + kind - 1
            act(pltpu.make_async_copy(columns(wq_hbm, h, 1), wbuf.at[at, :, :HEAD], w_sem.at[at, 0]))
            act(pltpu.make_async_copy(columns(wk_hbm, h, 1), wbuf.at[at, :, HEAD:], w_sem.at[at, 1]))

    tiles = half // tile

    def wo_copy(m):
        at = jnp.where(m < tiles, other + m * tile, mine + (m - tiles) * tile)
        part = pl.ds(pl.multiple_of(at, 128), tile)
        return pltpu.make_async_copy(wo_hbm.at[:, part], wo.at[:, part], wo_sem.at[m])

    def xres_copy(s):
        b = lax.rem(s, nx)
        return pltpu.make_async_copy(x_hbm.at[rows(s), pl.ds(mine, half)], xres.at[b], xres_sem.at[b])

    def d2d_copy(c, k):
        at = lax.rem(c, 2) * batch + k
        return remote(stage.at[k], d2d.at[at], d2d_send.at[k], d2d_recv.at[at], partner)

    def up_copy(s):
        b, r = lax.rem(s, nb), lax.rem(s, ring)
        return remote(sendb.at[b], up.at[r], send_a.at[b], up_recv.at[r], toward)

    def cross_copy(s):
        b, r = lax.rem(s, nb), lax.rem(s, cring)
        return remote(sendb.at[b], cross.at[r], send_a.at[b], cross_recv.at[r], toward)

    def out_copies(s, act):
        b = lax.rem(s, nb)

        def both(at, which):
            src = at if which else resb.at[b]
            act(remote(src, at, send_b.at[b], res_recv.at[lax.rem(s, ring)], away))
            act(remote(src, at, send_c.at[b], part_recv.at[which], partner))

        finished(s, both)

    def local_copy(s):
        b = lax.rem(s, nb)
        return pltpu.make_async_copy(resb.at[b], early.at[rows(s), pl.ds(mine, half)], send_l.at[b])

    def onward_copy(s, act):
        finished(s, lambda at, which: act(remote(at, at, part_send.at[which], part_recv.at[which], partner)))

    def start(copy):
        copy.start()

    def norm(i):
        bc, bs = base_ref[0, pl.ds(i, 1), :], base_ref[1, pl.ds(i, 1), :]
        rotc[...] = bc * fine_ref[0] - bs * fine_ref[1]
        rots[...] = bs * fine_ref[0] + bc * fine_ref[1]

        def group(r, _):
            x_copy(i, r).wait()
            at = pl.ds(pl.multiple_of(r * GROUP, GROUP), GROUP)
            cols = [slice(c, c + 128) for c in range(0, depth, 128)]
            sums = [None] * 4
            for n, c in enumerate(cols):
                wide = xbuf[at, c].astype(F32)
                sums[n % 4] = wide * wide if sums[n % 4] is None else sums[n % 4] + wide * wide
            total = functools.reduce(jnp.add, [s for s in sums if s is not None])
            scale = lax.rsqrt(jnp.sum(total, -1, keepdims=True) * (1 / depth) + 1e-6)
            scale = jnp.broadcast_to(scale, (GROUP, 128))
            for c in cols:
                abuf[at, c] = (xbuf[at, c].astype(F32) * scale * gain[:, c]).astype(BF16)

        lax.fori_loop(0, ch // GROUP, group, None)

    def turned(v):
        v = v.astype(BF16).astype(F32)
        return (v * rotc[...] + pltpu.roll(v, HEAD // 2, 1) * rots[...]).astype(BF16)

    def product(n, k, cuts, between):
        if n is None:
            for do in between:
                do()
            return
        at, total = lax.rem(n, 3), None
        for lo, hi, do in zip(cuts, cuts[1:], between):
            if lo < hi:
                part = _dot(abuf[:, lo:hi], wbuf[at, lo:hi, :], 1, 0)
                total = part if total is None else total + part
            do()
        zbuf[lax.rem(k, 2)] = total

    def cut(parts):
        lead = 1 / 7 if parts > 1 else 1
        ends = [0, lead] + [lead + (1 - lead) * (j + 1) / max(parts - 1, 1) for j in range(parts - 1)]
        return [min(round(f * depth / 256) * 256, depth) for f in ends]

    def attention(n, i, k, blocks):
        h = jnp.where(lax.rem(k, 3) == 2, 2 * lax.div(k, 3), 2 * lax.div(k, 3) - 1)
        here = pl.ds(pl.multiple_of(i * ch, ch), ch)
        wide, last = WIDE * ch, blocks - 1
        state = {}

        def scores(j):
            at = slice((last - j) * wide, (last - j + 1) * wide)
            s = _dot(keys[h, at, :], state["q"], 1, 1)
            if j == 0:
                gap = lax.broadcasted_iota(jnp.int32, (wide, ch), 1) - lax.broadcasted_iota(jnp.int32, (wide, ch), 0)
                s = jnp.where(gap >= last * wide - i * ch, s, HIDDEN)
            state["s", j], state["v", j] = s, vals[h, :, at]

        def lead():
            z = zbuf[lax.rem(k + 1, 2)]
            state["q"] = turned(z[:, :HEAD])
            keys[h, here, :] = turned(z[:, HEAD:])
            scores(0)

        def block(j):
            if j + 1 < blocks:
                scores(j + 1)
            s = state.pop(("s", j))
            top = s.max(axis=0, keepdims=True)
            if j:
                top = jnp.maximum(state["top"], top)
            weights = jnp.exp2((s - top) * e).astype(BF16)
            mix = _dot(state.pop(("v", j)), weights, 1, 0)
            if j:
                mix = state["mix"] * jnp.exp2((state["top"] - top) * e) + mix
            state["top"], state["mix"] = top, mix
            if j == last:
                out = mix[:HEAD] * (1 / mix[HEAD : HEAD + 1])
                seen[:, pl.ds(pl.multiple_of(h * HEAD, HEAD), HEAD)] = out.T.astype(BF16)

        product(n, k, cut(blocks + 1), [lead, *(functools.partial(block, j) for j in range(blocks))])

    def values(n, i, k):
        def post():
            z, here = zbuf[lax.rem(k + 1, 2)], pl.ds(pl.multiple_of(i * ch, ch), ch)
            for m in range(2):
                vals[2 * lax.div(k, 3) + m, :HEAD, here] = z[:, m * HEAD : (m + 1) * HEAD].astype(BF16).T

        product(n, k, [0, depth], [post])

    def compute(i, k):
        n = i * units + k
        follows = (k > 1) & (lax.rem(k, 3) != 1)

        @pl.when(k < units)
        def _():
            @pl.when((n + 2 < nc * units) & ((n + 2 < units) | (n >= units)))
            def _():
                for_unit(n + 2, start)

            @pl.when(n == units - 2)
            def _():
                for m in range(2 * tiles):
                    wo_copy(m).start()

            for_unit(n, lambda copy: copy.wait())

            @pl.when(k == 0)
            def _():
                product(n, k, [0, depth], [lambda: None])

            @pl.when(lax.rem(k, 3) == 1)
            def _():
                values(n, i, k)

            for blocks in range(1, pl.cdiv(nc, WIDE) + 1):
                pl.when(follows & (lax.div(i, WIDE) == blocks - 1))(functools.partial(attention, n, i, k, blocks))

        for blocks in range(1, pl.cdiv(nc, WIDE) + 1):
            pl.when((k == units) & (lax.div(i, WIDE) == blocks - 1))(functools.partial(attention, None, i, k, blocks))

        @pl.when(k == units + 1)
        def _():
            @pl.when(i == 0)
            def _():
                for n in range(units, units + 2):
                    for_unit(n, start)

            @pl.when(i > 0)
            def _():
                for j in range(batch):
                    d2d_copy(i - 1, j).wait_send()

            def theirs(n, _):
                at = pl.multiple_of(n * tile, tile)
                pl.when(i == 0)(lambda: wo_copy(n).wait())
                part = _dot(seen[...], wo[:, pl.ds(pl.multiple_of(other + at, 128), tile)], 1, 0)
                stage[:, :, pl.ds(at, tile)] = part.astype(BF16).reshape(batch, sub, tile)

            lax.fori_loop(0, half // tile, theirs, None)
            for j in range(batch):
                d2d_copy(i, j).start()

        @pl.when(k == units + 2)
        def _():
            def ours(n, _):
                at = pl.multiple_of(n * tile, tile)
                pl.when(i == 0)(lambda: wo_copy(tiles + n).wait())
                part = _dot(seen[...], wo[:, pl.ds(pl.multiple_of(mine + at, 128), tile)], 1, 0)
                acc[lax.rem(i, 2), :, :, pl.ds(at, tile)] = part.reshape(batch, sub, tile)

            lax.fori_loop(0, half // tile, ours, None)

        @pl.when((k == units + 3) & (i + 1 < nc))
        def _():
            norm(i + 1)

            @pl.when(i + 2 < nc)
            def _():
                for r in range(ch // GROUP):
                    x_copy(i + 2, r).start()

    def valid(s):
        return (s >= 0) & (s < pieces)

    def sum_of(s):
        return acc.at[lax.rem(lax.div(s, batch), 2), lax.rem(s, batch)]

    def pair(s):
        at, ours = lax.rem(s, 2 * batch), sum_of(s)
        d2d_copy(lax.div(s, batch), lax.rem(s, batch)).wait_recv()

        @pl.when(inner)
        def _():
            ours[...] = ours[...] + d2d[at].astype(F32)

        @pl.when(jnp.logical_not(inner))
        def _():
            @pl.when(s >= nb)
            def _():
                up_copy(s - nb).wait_send()

            sendb[lax.rem(s, nb)] = (ours[...] + d2d[at].astype(F32)).astype(BF16)
            up_copy(s).start()

    def relay(s):
        up_copy(s).wait_recv()

        @pl.when(s >= nb)
        def _():
            cross_copy(s - nb).wait_send()

        sendb[lax.rem(s, nb)] = (sum_of(s)[...] + up[lax.rem(s, ring)].astype(F32)).astype(BF16)
        cross_copy(s).start()

    def sent(s):
        out_copies(s, lambda copy: copy.wait_send())
        pl.when(s < split)(lambda: local_copy(s).wait())

    def finish(s):
        b = lax.rem(s, nb)
        cross_copy(s).wait_recv()
        xres_copy(s).wait()

        @pl.when(s >= nb)
        def _():
            sent(s - nb)

        total = sendb[b].astype(F32) + cross[lax.rem(s, cring)].astype(F32)
        y = (xres[lax.rem(s, nx)].astype(F32) + total).astype(BF16)

        @pl.when(s < split)
        def _():
            resb[b] = y
            local_copy(s).start()

        @pl.when(s >= split)
        def _():
            y_ref[rows(s), pl.ds(mine, half)] = y

        out_copies(s, start)

    def arrived(s):
        b = lax.rem(s, ring)
        finished(s, lambda at, _: remote(at, at, part_send.at[0], res_recv.at[b], away).wait_recv())
        onward_copy(s, start)

    for r in range(ch // GROUP):
        x_copy(0, r).start()
    for n in range(2):
        for_unit(n, lambda copy: copy.start())
    barrier = pltpu.get_barrier_semaphore()
    pl.semaphore_signal(barrier, inc=1, device_id=partner, device_id_type=MESH)

    @pl.when(z < zs - 1)
    def _():
        pl.semaphore_signal(barrier, inc=1, device_id=above, device_id_type=MESH)

    @pl.when(z > 0)
    def _():
        pl.semaphore_signal(barrier, inc=1, device_id=below, device_id_type=MESH)

    def clear(h, _):
        keys[h] = jnp.zeros(keys.shape[1:], BF16)
        vals[h, :HEAD, :] = jnp.zeros((HEAD, vals.shape[2]), BF16)
        vals[h, HEAD:, :] = jnp.ones((vals.shape[1] - HEAD, vals.shape[2]), BF16)

    lax.fori_loop(0, heads, clear, None)
    for n in range(depth // 128):
        gain[:, n * 128 : (n + 1) * 128] = gain_ref[n : n + 1, :].astype(F32)
    norm(0)
    for r in range(ch // GROUP):
        x_copy(1, r).start()
    pl.semaphore_wait(barrier, 1 + jnp.where(z < zs - 1, 1, 0) + jnp.where(z > 0, 1, 0))

    def served(g, stage, do):
        grown = stage * GROWN
        s = g - lag1 - stage * LAGS - jnp.clip(g - turn, 0, grown)
        pl.when(valid(s) & ((g <= turn) | (g > turn + grown)))(functools.partial(do, s))

    def serve(g):
        pl.when(jnp.logical_not(inner))(lambda: served(g, 3, arrived))

        @pl.when(inner)
        def _():
            served(g, 2, finish)
            served(g + 2, 2, lambda s: xres_copy(s).start())
            served(g, 1, relay)

        served(g, 0, pair)

    homes = [
        pltpu.make_async_copy(early.at[pl.ds(r * GROUP, GROUP), :], y_ref.at[pl.ds(r * GROUP, GROUP), :], home_sem.at[r])
        for r in range(early.shape[0] // GROUP)
    ]

    def theirs_arrived(which, y):
        at = y.at[:, pl.ds(other, half)]
        remote(at, at, part_send.at[which], part_recv.at[which], partner).wait_recv()

    def slot(g, _):
        i, k = lax.div(g, per), lax.rem(g, per)
        pl.when(lax.rem(g, 2) == 0)(lambda: serve(lax.div(g, 2)))
        pl.when(i < nc)(lambda: compute(i, k))

        @pl.when(g == max(nc * per, 2 * (split + last_lag)))
        def _():
            theirs_arrived(0, early)
            for copy in homes:
                copy.start()

    lax.fori_loop(0, 2 * (pieces + last_lag), slot, None)

    for j in range(batch):
        d2d_copy(nc - 1, j).wait_send()
    for s in range(pieces - nb, pieces):
        up_copy(s).wait_send()

    @pl.when(inner)
    def _():
        for s in range(pieces - nb, pieces):
            sent(s)

    rest = y_ref.at[early.shape[0] :, :]
    theirs_arrived(1, rest)
    for which, y in enumerate((early, rest)):
        ours = y.at[:, pl.ds(mine, half)]
        pl.when(jnp.logical_not(inner))(remote(ours, ours, part_send.at[which], part_recv.at[which], partner).wait_send)
    for copy in homes:
        copy.wait()


def _placed(y_in, y_out, sem):
    size = y_in.shape[0] // sem.shape[0]
    copies = [pltpu.make_async_copy(y_in.at[pl.ds(r, size), :], y_out.at[pl.ds(r, size), :], sem.at[r // size]) for r in range(0, y_in.shape[0], size)]
    for copy in copies:
        copy.start()
    for copy in copies:
        copy.wait()


def _tables(nc, ch):
    rate = THETA ** (-np.arange(HEAD // 2) / (HEAD // 2))
    sign = np.repeat([-1.0, 1.0], HEAD // 2)

    def both(place):
        angle = np.tile(place[:, None] * rate, (1, 2))
        return np.stack([np.cos(angle), np.sin(angle) * sign]).astype(np.float32)

    return both(np.arange(nc) * ch), both(np.arange(ch))


def solution(mesh, ch=128, tile=1792, copy_rows=128):
    names = mesh.axis_names
    zs = mesh.shape["tp"] // 2

    def step(x, gain, wq, wk, wv, wo):
        n, d = x.shape
        heads = wq.shape[1] // HEAD
        nc, half = n // ch, d // 2
        per = 3 * (heads // 2) + 7
        sub = 2 * ch // per
        base, fine = _tables(nc, ch)
        cfg = dict(ch=ch, sub=sub, per=per, heads=heads, nc=nc, half=half, zs=zs, tile=min(tile, half), names=names)
        wide, batch = min(tile, half), per // 2
        nb, ring, cring, nx = 6, 10, 8, 4
        dma = pltpu.SemaphoreType.DMA
        hbm, vmem = pl.BlockSpec(memory_space=pl.ANY), pl.BlockSpec(memory_space=pltpu.VMEM)
        _, y = pl.pallas_call(
            functools.partial(_kernel, cfg),
            out_shape=[jax.ShapeDtypeStruct((heads * HEAD, d), BF16), pltpu.VMEM((n, d), BF16)],
            in_specs=[hbm, vmem, vmem, vmem, hbm, hbm, hbm, hbm],
            out_specs=[hbm, vmem],
            scratch_shapes=[
                pltpu.VMEM((heads, n, HEAD), BF16),
                pltpu.VMEM((heads + 1, HEAD + 8, n), BF16),
                pltpu.VMEM((3, d, 2 * HEAD), BF16),
                pltpu.VMEM((2, ch, 2 * HEAD), F32),
                pltpu.VMEM((ch, d), BF16),
                pltpu.VMEM((ch, d), BF16),
                pltpu.VMEM((2, batch, sub, half), F32),
                pltpu.VMEM((batch, sub, half), BF16),
                pltpu.VMEM((ch, heads * HEAD), BF16),
                pltpu.VMEM((2 * batch, sub, half), BF16),
                pltpu.VMEM((ring, sub, half), BF16),
                pltpu.VMEM((cring, sub, half), BF16),
                pltpu.VMEM((nb, sub, half), BF16),
                pltpu.VMEM((nb, sub, half), BF16),
                pltpu.VMEM((nx, sub, half), BF16),
                pltpu.VMEM((ch, HEAD), F32),
                pltpu.VMEM((ch, HEAD), F32),
                pltpu.VMEM((1, d), F32),
                dma((3, 2)), dma((2 * half // wide,)), dma((ch // GROUP,)), dma((nx,)),
                dma((batch,)), dma((2 * batch,)), dma((ring,)), dma((cring,)), dma((ring,)),
                dma((nb,)), dma((nb,)), dma((nb,)), dma((nb,)), dma((2,)), dma((2,)),
                dma((heads * HEAD // GROUP,)),
            ],
            compiler_params=pltpu.CompilerParams(collective_id=0, has_side_effects=True, vmem_limit_bytes=KERNEL_VMEM),
            name="attention_half",
        )(x, gain.reshape(d // 128, 128), jnp.asarray(base), jnp.asarray(fine), wq, wk, wv, wo)
        return pl.pallas_call(
            _placed,
            out_shape=jax.ShapeDtypeStruct((n, d), BF16),
            in_specs=[vmem],
            out_specs=hbm,
            scratch_shapes=[dma((n // copy_rows,))],
            compiler_params=pltpu.CompilerParams(vmem_limit_bytes=2**20),
            name="placed",
        )(pltpu.with_memory_space_constraint(y, pltpu.VMEM))

    tokens, columns = P("dp", None), P(None, "tp")
    return jax.shard_map(
        step,
        mesh=mesh,
        in_specs=(tokens, P(None), columns, columns, columns, P("tp", None)),
        out_specs=tokens,
        check_vma=False,
    )
```

```python
import functools

import jax
import jax.numpy as jnp
import numpy as np
from jax import lax
from jax.experimental import pallas as pl
from jax.experimental.pallas import tpu as pltpu
from jax.sharding import PartitionSpec as P

HEAD = 128
THETA = 10000
LOG2E = 1.4426950408889634
HIDDEN = -2e30
MESH = pl.DeviceIdType.MESH
BF16, F32 = jnp.bfloat16, jnp.float32
LAGS = (0, 3, 6, 12)
GROUP = 64
KERNEL_VMEM = 37_500_000
WIDE = 4


def _dot(a, b, ca, cb):
    return lax.dot_general(a, b, (((ca,), (cb,)), ((), ())), preferred_element_type=F32)


def _kernel(cfg, x_hbm, gain_ref, base_ref, fine_ref, wq_hbm, wk_hbm, wv_hbm, wo_hbm, early, y_ref,
            keys, vals, wbuf, zbuf, xbuf, abuf, acc, stage, seen, d2d, up, cross, sendb, resb, xres, rotc, rots, gain,
            w_sem, wo_sem, x_sem, xres_sem, d2d_send, d2d_recv, up_recv, cross_recv, res_recv,
            send_a, send_b, send_c, send_l, part_send, part_recv, home_sem):
    ch, sub, per, heads, nc, half, zs, tile, names = (cfg[k] for k in ("ch", "sub", "per", "heads", "nc", "half", "zs", "tile", "names"))
    depth = 2 * half
    units = 3 * (heads // 2) + 2
    batch = per // 2
    pieces = nc * batch
    e = HEAD**-0.5 * LOG2E
    lag1 = (units + 4) // 2
    last_lag = lag1 + LAGS[3]
    ring, cring, nb, nx = up.shape[0], cross.shape[0], sendb.shape[0], xres.shape[0]
    wo, split = y_ref.at[: early.shape[0], :], early.shape[0] // sub

    dpi, t = lax.axis_index(names[0]), lax.axis_index(names[1])
    core, z = lax.rem(t, 2), lax.div(t, 2)
    inner = (z > 0) & (z < zs - 1)
    partner, above, below = (dpi, t + 1 - 2 * core), (dpi, t + 2), (dpi, t - 2)
    toward = (dpi, jnp.where(z < zs // 2, t + 2, t - 2))
    away = (dpi, jnp.where(z < zs // 2, t - 2, t + 2))
    mine = pl.multiple_of(core * half, 128)
    other = pl.multiple_of((1 - core) * half, 128)

    def rows(s):
        return pl.ds(pl.multiple_of(s * sub, sub), sub)

    def finished(s, act):
        cols = pl.ds(mine, half)
        pl.when(s < split)(lambda: act(early.at[rows(s), cols], 0))
        pl.when(s >= split)(lambda: act(y_ref.at[rows(s), cols], 1))

    def remote(src, dst, send, recv, device):
        return pltpu.make_async_remote_copy(src_ref=src, dst_ref=dst, send_sem=send, recv_sem=recv, device_id=device, device_id_type=MESH)

    def x_copy(i, r):
        at = pl.ds(r * GROUP, GROUP)
        return pltpu.make_async_copy(x_hbm.at[pl.ds(pl.multiple_of(i * ch + r * GROUP, GROUP), GROUP), :], xbuf.at[at, :], x_sem.at[r])

    def for_unit(n, act):
        k, at = lax.rem(n, units), lax.rem(n, 3)
        group, kind = lax.div(k, 3), lax.rem(k, 3)

        def columns(w, h, wide):
            return w.at[:, pl.ds(pl.multiple_of(h * HEAD, HEAD), wide * HEAD)]

        @pl.when((kind == 0) & (2 * group + 1 < heads))
        def _():
            act(pltpu.make_async_copy(columns(wv_hbm, 2 * group, 2), wbuf.at[at], w_sem.at[at, 0]))

        @pl.when((kind == 0) & (2 * group + 1 == heads))
        def _():
            act(pltpu.make_async_copy(columns(wv_hbm, 2 * group, 1), wbuf.at[at, :, :HEAD], w_sem.at[at, 0]))

        @pl.when(kind > 0)
        def _():
            h = 2 * group + kind - 1
            act(pltpu.make_async_copy(columns(wq_hbm, h, 1), wbuf.at[at, :, :HEAD], w_sem.at[at, 0]))
            act(pltpu.make_async_copy(columns(wk_hbm, h, 1), wbuf.at[at, :, HEAD:], w_sem.at[at, 1]))

    tiles = half // tile

    def wo_copy(m):
        at = jnp.where(m < tiles, other + m * tile, mine + (m - tiles) * tile)
        part = pl.ds(pl.multiple_of(at, 128), tile)
        return pltpu.make_async_copy(wo_hbm.at[:, part], wo.at[:, part], wo_sem.at[m])

    def xres_copy(s):
        b = lax.rem(s, nx)
        return pltpu.make_async_copy(x_hbm.at[rows(s), pl.ds(mine, half)], xres.at[b], xres_sem.at[b])

    def d2d_copy(c, k):
        at = lax.rem(c, 2) * batch + k
        return remote(stage.at[k], d2d.at[at], d2d_send.at[k], d2d_recv.at[at], partner)

    def up_copy(s):
        b, r = lax.rem(s, nb), lax.rem(s, ring)
        return remote(sendb.at[b], up.at[r], send_a.at[b], up_recv.at[r], toward)

    def cross_copy(s):
        b, r = lax.rem(s, nb), lax.rem(s, cring)
        return remote(sendb.at[b], cross.at[r], send_a.at[b], cross_recv.at[r], toward)

    def out_copies(s, act):
        b = lax.rem(s, nb)

        def both(at, which):
            src = at if which else resb.at[b]
            act(remote(src, at, send_b.at[b], res_recv.at[lax.rem(s, ring)], away))
            act(remote(src, at, send_c.at[b], part_recv.at[which], partner))

        finished(s, both)

    def local_copy(s):
        b = lax.rem(s, nb)
        return pltpu.make_async_copy(resb.at[b], early.at[rows(s), pl.ds(mine, half)], send_l.at[b])

    def onward_copy(s, act):
        finished(s, lambda at, which: act(remote(at, at, part_send.at[which], part_recv.at[which], partner)))

    def start(copy):
        copy.start()

    def norm(i):
        bc, bs = base_ref[0, pl.ds(i, 1), :], base_ref[1, pl.ds(i, 1), :]
        rotc[...] = bc * fine_ref[0] - bs * fine_ref[1]
        rots[...] = bs * fine_ref[0] + bc * fine_ref[1]

        def group(r, _):
            x_copy(i, r).wait()
            at = pl.ds(pl.multiple_of(r * GROUP, GROUP), GROUP)
            cols = [slice(c, c + 128) for c in range(0, depth, 128)]
            sums = [None] * 4
            for n, c in enumerate(cols):
                wide = xbuf[at, c].astype(F32)
                sums[n % 4] = wide * wide if sums[n % 4] is None else sums[n % 4] + wide * wide
            total = functools.reduce(jnp.add, [s for s in sums if s is not None])
            scale = lax.rsqrt(jnp.sum(total, -1, keepdims=True) * (1 / depth) + 1e-6)
            scale = jnp.broadcast_to(scale, (GROUP, 128))
            for c in cols:
                abuf[at, c] = (xbuf[at, c].astype(F32) * scale * gain[:, c]).astype(BF16)

        lax.fori_loop(0, ch // GROUP, group, None)

    def turned(v):
        v = v.astype(BF16).astype(F32)
        return (v * rotc[...] + pltpu.roll(v, HEAD // 2, 1) * rots[...]).astype(BF16)

    def product(n, k, cuts, between):
        if n is None:
            for do in between:
                do()
            return
        at, total = lax.rem(n, 3), None
        for lo, hi, do in zip(cuts, cuts[1:], between):
            if lo < hi:
                part = _dot(abuf[:, lo:hi], wbuf[at, lo:hi, :], 1, 0)
                total = part if total is None else total + part
            do()
        zbuf[lax.rem(k, 2)] = total

    def cut(parts):
        lead = 1 / 7 if parts > 1 else 1
        ends = [0, lead] + [lead + (1 - lead) * (j + 1) / max(parts - 1, 1) for j in range(parts - 1)]
        return [min(round(f * depth / 256) * 256, depth) for f in ends]

    def attention(n, i, k, blocks):
        h = jnp.where(lax.rem(k, 3) == 2, 2 * lax.div(k, 3), 2 * lax.div(k, 3) - 1)
        here = pl.ds(pl.multiple_of(i * ch, ch), ch)
        wide, last = WIDE * ch, blocks - 1
        state = {}

        def scores(j):
            at = slice((last - j) * wide, (last - j + 1) * wide)
            s = _dot(keys[h, at, :], state["q"], 1, 1)
            if j == 0:
                gap = lax.broadcasted_iota(jnp.int32, (wide, ch), 1) - lax.broadcasted_iota(jnp.int32, (wide, ch), 0)
                s = jnp.where(gap >= last * wide - i * ch, s, HIDDEN)
            state["s", j], state["v", j] = s, vals[h, :, at]

        def lead():
            z = zbuf[lax.rem(k + 1, 2)]
            state["q"] = turned(z[:, :HEAD])
            keys[h, here, :] = turned(z[:, HEAD:])
            scores(0)

        def block(j):
            if j + 1 < blocks:
                scores(j + 1)
            s = state.pop(("s", j))
            top = s.max(axis=0, keepdims=True)
            if j:
                top = jnp.maximum(state["top"], top)
            weights = jnp.exp2((s - top) * e).astype(BF16)
            mix = _dot(state.pop(("v", j)), weights, 1, 0)
            if j:
                mix = state["mix"] * jnp.exp2((state["top"] - top) * e) + mix
            state["top"], state["mix"] = top, mix
            if j == last:
                out = mix[:HEAD] * (1 / mix[HEAD : HEAD + 1])
                seen[:, pl.ds(pl.multiple_of(h * HEAD, HEAD), HEAD)] = out.T.astype(BF16)

        product(n, k, cut(blocks + 1), [lead, *(functools.partial(block, j) for j in range(blocks))])

    def values(n, i, k):
        def post():
            z, here = zbuf[lax.rem(k + 1, 2)], pl.ds(pl.multiple_of(i * ch, ch), ch)
            for m in range(2):
                vals[2 * lax.div(k, 3) + m, :HEAD, here] = z[:, m * HEAD : (m + 1) * HEAD].astype(BF16).T

        product(n, k, [0, depth], [post])

    def compute(i, k):
        n = i * units + k
        follows = (k > 1) & (lax.rem(k, 3) != 1)

        @pl.when(k < units)
        def _():
            @pl.when((n + 2 < nc * units) & ((n + 2 < units) | (n >= units)))
            def _():
                for_unit(n + 2, start)

            @pl.when(n == units - 2)
            def _():
                for m in range(2 * tiles):
                    wo_copy(m).start()

            for_unit(n, lambda copy: copy.wait())

            @pl.when(k == 0)
            def _():
                product(n, k, [0, depth], [lambda: None])

            @pl.when(lax.rem(k, 3) == 1)
            def _():
                values(n, i, k)

            for blocks in range(1, pl.cdiv(nc, WIDE) + 1):
                pl.when(follows & (lax.div(i, WIDE) == blocks - 1))(functools.partial(attention, n, i, k, blocks))

        for blocks in range(1, pl.cdiv(nc, WIDE) + 1):
            pl.when((k == units) & (lax.div(i, WIDE) == blocks - 1))(functools.partial(attention, None, i, k, blocks))

        @pl.when(k == units + 1)
        def _():
            @pl.when(i == 0)
            def _():
                for n in range(units, units + 2):
                    for_unit(n, start)

            @pl.when(i > 0)
            def _():
                for j in range(batch):
                    d2d_copy(i - 1, j).wait_send()

            def theirs(n, _):
                at = pl.multiple_of(n * tile, tile)
                pl.when(i == 0)(lambda: wo_copy(n).wait())
                part = _dot(seen[...], wo[:, pl.ds(pl.multiple_of(other + at, 128), tile)], 1, 0)
                stage[:, :, pl.ds(at, tile)] = part.astype(BF16).reshape(batch, sub, tile)

            lax.fori_loop(0, half // tile, theirs, None)
            for j in range(batch):
                d2d_copy(i, j).start()

        @pl.when(k == units + 2)
        def _():
            def ours(n, _):
                at = pl.multiple_of(n * tile, tile)
                pl.when(i == 0)(lambda: wo_copy(tiles + n).wait())
                part = _dot(seen[...], wo[:, pl.ds(pl.multiple_of(mine + at, 128), tile)], 1, 0)
                acc[lax.rem(i, 2), :, :, pl.ds(at, tile)] = part.reshape(batch, sub, tile)

            lax.fori_loop(0, half // tile, ours, None)

        @pl.when((k == units + 3) & (i + 1 < nc))
        def _():
            norm(i + 1)

            @pl.when(i + 2 < nc)
            def _():
                for r in range(ch // GROUP):
                    x_copy(i + 2, r).start()

    def valid(s):
        return (s >= 0) & (s < pieces)

    def sum_of(s):
        return acc.at[lax.rem(lax.div(s, batch), 2), lax.rem(s, batch)]

    def pair(s):
        at, ours = lax.rem(s, 2 * batch), sum_of(s)
        d2d_copy(lax.div(s, batch), lax.rem(s, batch)).wait_recv()

        @pl.when(inner)
        def _():
            ours[...] = ours[...] + d2d[at].astype(F32)

        @pl.when(jnp.logical_not(inner))
        def _():
            @pl.when(s >= nb)
            def _():
                up_copy(s - nb).wait_send()

            sendb[lax.rem(s, nb)] = (ours[...] + d2d[at].astype(F32)).astype(BF16)
            up_copy(s).start()

    def relay(s):
        up_copy(s).wait_recv()

        @pl.when(s >= nb)
        def _():
            cross_copy(s - nb).wait_send()

        sendb[lax.rem(s, nb)] = (sum_of(s)[...] + up[lax.rem(s, ring)].astype(F32)).astype(BF16)
        cross_copy(s).start()

    def sent(s):
        out_copies(s, lambda copy: copy.wait_send())
        pl.when(s < split)(lambda: local_copy(s).wait())

    def finish(s):
        b = lax.rem(s, nb)
        cross_copy(s).wait_recv()
        xres_copy(s).wait()

        @pl.when(s >= nb)
        def _():
            sent(s - nb)

        total = sendb[b].astype(F32) + cross[lax.rem(s, cring)].astype(F32)
        y = (xres[lax.rem(s, nx)].astype(F32) + total).astype(BF16)

        @pl.when(s < split)
        def _():
            resb[b] = y
            local_copy(s).start()

        @pl.when(s >= split)
        def _():
            y_ref[rows(s), pl.ds(mine, half)] = y

        out_copies(s, start)

    def arrived(s):
        b = lax.rem(s, ring)
        finished(s, lambda at, _: remote(at, at, part_send.at[0], res_recv.at[b], away).wait_recv())
        onward_copy(s, start)

    for r in range(ch // GROUP):
        x_copy(0, r).start()
    for n in range(2):
        for_unit(n, lambda copy: copy.start())
    barrier = pltpu.get_barrier_semaphore()
    pl.semaphore_signal(barrier, inc=1, device_id=partner, device_id_type=MESH)

    @pl.when(z < zs - 1)
    def _():
        pl.semaphore_signal(barrier, inc=1, device_id=above, device_id_type=MESH)

    @pl.when(z > 0)
    def _():
        pl.semaphore_signal(barrier, inc=1, device_id=below, device_id_type=MESH)

    def clear(h, _):
        keys[h] = jnp.zeros(keys.shape[1:], BF16)
        vals[h, :HEAD, :] = jnp.zeros((HEAD, vals.shape[2]), BF16)
        vals[h, HEAD:, :] = jnp.ones((vals.shape[1] - HEAD, vals.shape[2]), BF16)

    lax.fori_loop(0, heads, clear, None)
    for n in range(depth // 128):
        gain[:, n * 128 : (n + 1) * 128] = gain_ref[n : n + 1, :].astype(F32)
    norm(0)
    for r in range(ch // GROUP):
        x_copy(1, r).start()
    pl.semaphore_wait(barrier, 1 + jnp.where(z < zs - 1, 1, 0) + jnp.where(z > 0, 1, 0))

    def served(g, stage, do):
        s = g - lag1 - LAGS[stage]
        pl.when(valid(s))(functools.partial(do, s))

    def serve(g):
        pl.when(jnp.logical_not(inner))(lambda: served(g, 3, arrived))

        @pl.when(inner)
        def _():
            served(g, 2, finish)
            served(g + 2, 2, lambda s: xres_copy(s).start())
            served(g, 1, relay)

        served(g, 0, pair)

    homes = [
        pltpu.make_async_copy(early.at[pl.ds(r * GROUP, GROUP), :], y_ref.at[pl.ds(r * GROUP, GROUP), :], home_sem.at[r])
        for r in range(early.shape[0] // GROUP)
    ]

    def theirs_arrived(which, y):
        at = y.at[:, pl.ds(other, half)]
        remote(at, at, part_send.at[which], part_recv.at[which], partner).wait_recv()

    def slot(g, _):
        i, k = lax.div(g, per), lax.rem(g, per)
        pl.when(lax.rem(g, 2) == 0)(lambda: serve(lax.div(g, 2)))
        pl.when(i < nc)(lambda: compute(i, k))

        @pl.when(g == max(nc * per, 2 * (split + last_lag)))
        def _():
            theirs_arrived(0, early)
            for copy in homes:
                copy.start()

    lax.fori_loop(0, 2 * (pieces + last_lag), slot, None)

    for j in range(batch):
        d2d_copy(nc - 1, j).wait_send()
    for s in range(pieces - nb, pieces):
        up_copy(s).wait_send()

    @pl.when(inner)
    def _():
        for s in range(pieces - nb, pieces):
            sent(s)

    rest = y_ref.at[early.shape[0] :, :]
    theirs_arrived(1, rest)
    for which, y in enumerate((early, rest)):
        ours = y.at[:, pl.ds(mine, half)]
        pl.when(jnp.logical_not(inner))(remote(ours, ours, part_send.at[which], part_recv.at[which], partner).wait_send)
    for copy in homes:
        copy.wait()


def _placed(y_in, y_out, sem):
    size = y_in.shape[0] // sem.shape[0]
    copies = [pltpu.make_async_copy(y_in.at[pl.ds(r, size), :], y_out.at[pl.ds(r, size), :], sem.at[r // size]) for r in range(0, y_in.shape[0], size)]
    for copy in copies:
        copy.start()
    for copy in copies:
        copy.wait()


def _tables(nc, ch):
    rate = THETA ** (-np.arange(HEAD // 2) / (HEAD // 2))
    sign = np.repeat([-1.0, 1.0], HEAD // 2)

    def both(place):
        angle = np.tile(place[:, None] * rate, (1, 2))
        return np.stack([np.cos(angle), np.sin(angle) * sign]).astype(np.float32)

    return both(np.arange(nc) * ch), both(np.arange(ch))


def solution(mesh, ch=128, tile=1792, copy_rows=128):
    names = mesh.axis_names
    zs = mesh.shape["tp"] // 2

    def step(x, gain, wq, wk, wv, wo):
        n, d = x.shape
        heads = wq.shape[1] // HEAD
        nc, half = n // ch, d // 2
        per = 3 * (heads // 2) + 7
        sub = 2 * ch // per
        base, fine = _tables(nc, ch)
        cfg = dict(ch=ch, sub=sub, per=per, heads=heads, nc=nc, half=half, zs=zs, tile=min(tile, half), names=names)
        wide, batch = min(tile, half), per // 2
        nb, ring, cring, nx = 6, 13, 8, 4
        dma = pltpu.SemaphoreType.DMA
        hbm, vmem = pl.BlockSpec(memory_space=pl.ANY), pl.BlockSpec(memory_space=pltpu.VMEM)
        _, y = pl.pallas_call(
            functools.partial(_kernel, cfg),
            out_shape=[jax.ShapeDtypeStruct((heads * HEAD, d), BF16), pltpu.VMEM((n, d), BF16)],
            in_specs=[hbm, vmem, vmem, vmem, hbm, hbm, hbm, hbm],
            out_specs=[hbm, vmem],
            scratch_shapes=[
                pltpu.VMEM((heads, n, HEAD), BF16),
                pltpu.VMEM((heads + 1, HEAD + 8, n), BF16),
                pltpu.VMEM((3, d, 2 * HEAD), BF16),
                pltpu.VMEM((2, ch, 2 * HEAD), F32),
                pltpu.VMEM((ch, d), BF16),
                pltpu.VMEM((ch, d), BF16),
                pltpu.VMEM((2, batch, sub, half), F32),
                pltpu.VMEM((batch, sub, half), BF16),
                pltpu.VMEM((ch, heads * HEAD), BF16),
                pltpu.VMEM((2 * batch, sub, half), BF16),
                pltpu.VMEM((ring, sub, half), BF16),
                pltpu.VMEM((cring, sub, half), BF16),
                pltpu.VMEM((nb, sub, half), BF16),
                pltpu.VMEM((nb, sub, half), BF16),
                pltpu.VMEM((nx, sub, half), BF16),
                pltpu.VMEM((ch, HEAD), F32),
                pltpu.VMEM((ch, HEAD), F32),
                pltpu.VMEM((1, d), F32),
                dma((3, 2)), dma((2 * half // wide,)), dma((ch // GROUP,)), dma((nx,)),
                dma((batch,)), dma((2 * batch,)), dma((ring,)), dma((cring,)), dma((ring,)),
                dma((nb,)), dma((nb,)), dma((nb,)), dma((nb,)), dma((2,)), dma((2,)),
                dma((heads * HEAD // GROUP,)),
            ],
            compiler_params=pltpu.CompilerParams(collective_id=0, has_side_effects=True, vmem_limit_bytes=KERNEL_VMEM),
            name="attention_half",
        )(x, gain.reshape(d // 128, 128), jnp.asarray(base), jnp.asarray(fine), wq, wk, wv, wo)
        return pl.pallas_call(
            _placed,
            out_shape=jax.ShapeDtypeStruct((n, d), BF16),
            in_specs=[vmem],
            out_specs=hbm,
            scratch_shapes=[dma((n // copy_rows,))],
            compiler_params=pltpu.CompilerParams(vmem_limit_bytes=2**20),
            name="placed",
        )(pltpu.with_memory_space_constraint(y, pltpu.VMEM))

    tokens, columns = P("dp", None), P(None, "tp")
    return jax.shard_map(
        step,
        mesh=mesh,
        in_specs=(tokens, P(None), columns, columns, columns, P("tp", None)),
        out_specs=tokens,
        check_vma=False,
    )
```

```python
import functools

import jax
import jax.numpy as jnp
import numpy as np
from jax import lax
from jax.experimental import pallas as pl
from jax.experimental.pallas import tpu as pltpu
from jax.sharding import PartitionSpec as P

HEAD = 128
THETA = 10000
LOG2E = 1.4426950408889634
HIDDEN = -2e30
MESH = pl.DeviceIdType.MESH
BF16, F32 = jnp.bfloat16, jnp.float32
LAGS, GROWN, EARLY = (0, 2, 4, 12), (0, 1, 2, 0), 12
GROUP = 64
KERNEL_VMEM = 37_500_000
WIDE = 4


def _dot(a, b, ca, cb):
    return lax.dot_general(a, b, (((ca,), (cb,)), ((), ())), preferred_element_type=F32)


def _kernel(cfg, x_hbm, gain_ref, base_ref, fine_ref, wq_hbm, wk_hbm, wv_hbm, wo_hbm, early, y_ref,
            keys, vals, wbuf, zbuf, xbuf, abuf, acc, stage, seen, d2d, up, cross, sendb, resb, xres, rotc, rots, gain,
            w_sem, wo_sem, x_sem, xres_sem, d2d_send, d2d_recv, up_recv, cross_recv, res_recv,
            send_a, send_b, send_c, send_l, part_send, part_recv, home_sem):
    ch, sub, per, heads, nc, half, zs, tile, names = (cfg[k] for k in ("ch", "sub", "per", "heads", "nc", "half", "zs", "tile", "names"))
    depth = 2 * half
    units = 3 * (heads // 2) + 2
    batch = per // 2
    pieces = nc * batch
    e = HEAD**-0.5 * LOG2E
    lag1 = (units + 4) // 2
    last_lag = lag1 + LAGS[3]
    turn = lag1 + EARLY
    ring, cring, nb, nx = up.shape[0], cross.shape[0], sendb.shape[0], xres.shape[0]
    wo, split = y_ref.at[: early.shape[0], :], early.shape[0] // sub

    dpi, t = lax.axis_index(names[0]), lax.axis_index(names[1])
    core, z = lax.rem(t, 2), lax.div(t, 2)
    inner = (z > 0) & (z < zs - 1)
    partner, above, below = (dpi, t + 1 - 2 * core), (dpi, t + 2), (dpi, t - 2)
    toward = (dpi, jnp.where(z < zs // 2, t + 2, t - 2))
    away = (dpi, jnp.where(z < zs // 2, t - 2, t + 2))
    mine = pl.multiple_of(core * half, 128)
    other = pl.multiple_of((1 - core) * half, 128)

    def rows(s):
        return pl.ds(pl.multiple_of(s * sub, sub), sub)

    def finished(s, act):
        cols = pl.ds(mine, half)
        pl.when(s < split)(lambda: act(early.at[rows(s), cols], 0))
        pl.when(s >= split)(lambda: act(y_ref.at[rows(s), cols], 1))

    def remote(src, dst, send, recv, device):
        return pltpu.make_async_remote_copy(src_ref=src, dst_ref=dst, send_sem=send, recv_sem=recv, device_id=device, device_id_type=MESH)

    def x_copy(i, r):
        at = pl.ds(r * GROUP, GROUP)
        return pltpu.make_async_copy(x_hbm.at[pl.ds(pl.multiple_of(i * ch + r * GROUP, GROUP), GROUP), :], xbuf.at[at, :], x_sem.at[r])

    def for_unit(n, act):
        k, at = lax.rem(n, units), lax.rem(n, 3)
        group, kind = lax.div(k, 3), lax.rem(k, 3)

        def columns(w, h, wide):
            return w.at[:, pl.ds(pl.multiple_of(h * HEAD, HEAD), wide * HEAD)]

        @pl.when((kind == 0) & (2 * group + 1 < heads))
        def _():
            act(pltpu.make_async_copy(columns(wv_hbm, 2 * group, 2), wbuf.at[at], w_sem.at[at, 0]))

        @pl.when((kind == 0) & (2 * group + 1 == heads))
        def _():
            act(pltpu.make_async_copy(columns(wv_hbm, 2 * group, 1), wbuf.at[at, :, :HEAD], w_sem.at[at, 0]))

        @pl.when(kind > 0)
        def _():
            h = 2 * group + kind - 1
            act(pltpu.make_async_copy(columns(wq_hbm, h, 1), wbuf.at[at, :, :HEAD], w_sem.at[at, 0]))
            act(pltpu.make_async_copy(columns(wk_hbm, h, 1), wbuf.at[at, :, HEAD:], w_sem.at[at, 1]))

    tiles = half // tile

    def wo_copy(m):
        at = jnp.where(m < tiles, other + m * tile, mine + (m - tiles) * tile)
        part = pl.ds(pl.multiple_of(at, 128), tile)
        return pltpu.make_async_copy(wo_hbm.at[:, part], wo.at[:, part], wo_sem.at[m])

    def xres_copy(s):
        b = lax.rem(s, nx)
        return pltpu.make_async_copy(x_hbm.at[rows(s), pl.ds(mine, half)], xres.at[b], xres_sem.at[b])

    def d2d_copy(c, k):
        at = lax.rem(c, 2) * batch + k
        return remote(stage.at[k], d2d.at[at], d2d_send.at[k], d2d_recv.at[at], partner)

    def up_copy(s):
        b, r = lax.rem(s, nb), lax.rem(s, ring)
        return remote(sendb.at[b], up.at[r], send_a.at[b], up_recv.at[r], toward)

    def cross_copy(s):
        b, r = lax.rem(s, nb), lax.rem(s, cring)
        return remote(sendb.at[b], cross.at[r], send_a.at[b], cross_recv.at[r], toward)

    def out_copies(s, act):
        b = lax.rem(s, nb)

        def both(at, which):
            src = at if which else resb.at[b]
            act(remote(src, at, send_b.at[b], res_recv.at[lax.rem(s, ring)], away))
            act(remote(src, at, send_c.at[b], part_recv.at[which], partner))

        finished(s, both)

    def local_copy(s):
        b = lax.rem(s, nb)
        return pltpu.make_async_copy(resb.at[b], early.at[rows(s), pl.ds(mine, half)], send_l.at[b])

    def onward_copy(s, act):
        finished(s, lambda at, which: act(remote(at, at, part_send.at[which], part_recv.at[which], partner)))

    def start(copy):
        copy.start()

    def norm(i):
        bc, bs = base_ref[0, pl.ds(i, 1), :], base_ref[1, pl.ds(i, 1), :]
        rotc[...] = bc * fine_ref[0] - bs * fine_ref[1]
        rots[...] = bs * fine_ref[0] + bc * fine_ref[1]

        def group(r, _):
            x_copy(i, r).wait()
            at = pl.ds(pl.multiple_of(r * GROUP, GROUP), GROUP)
            cols = [slice(c, c + 128) for c in range(0, depth, 128)]
            sums = [None] * 4
            for n, c in enumerate(cols):
                wide = xbuf[at, c].astype(F32)
                sums[n % 4] = wide * wide if sums[n % 4] is None else sums[n % 4] + wide * wide
            total = functools.reduce(jnp.add, [s for s in sums if s is not None])
            scale = lax.rsqrt(jnp.sum(total, -1, keepdims=True) * (1 / depth) + 1e-6)
            scale = jnp.broadcast_to(scale, (GROUP, 128))
            for c in cols:
                abuf[at, c] = (xbuf[at, c].astype(F32) * scale * gain[:, c]).astype(BF16)

        lax.fori_loop(0, ch // GROUP, group, None)

    def turned(v):
        v = v.astype(BF16).astype(F32)
        return (v * rotc[...] + pltpu.roll(v, HEAD // 2, 1) * rots[...]).astype(BF16)

    def product(n, k, cuts, between):
        if n is None:
            for do in between:
                do()
            return
        at, total = lax.rem(n, 3), None
        for lo, hi, do in zip(cuts, cuts[1:], between):
            if lo < hi:
                part = _dot(abuf[:, lo:hi], wbuf[at, lo:hi, :], 1, 0)
                total = part if total is None else total + part
            do()
        zbuf[lax.rem(k, 2)] = total

    def cut(parts):
        lead = 1 / 7 if parts > 1 else 1
        ends = [0, lead] + [lead + (1 - lead) * (j + 1) / max(parts - 1, 1) for j in range(parts - 1)]
        return [min(round(f * depth / 256) * 256, depth) for f in ends]

    def attention(n, i, k, blocks):
        h = jnp.where(lax.rem(k, 3) == 2, 2 * lax.div(k, 3), 2 * lax.div(k, 3) - 1)
        here = pl.ds(pl.multiple_of(i * ch, ch), ch)
        wide, last = WIDE * ch, blocks - 1
        state = {}

        def scores(j):
            at = slice((last - j) * wide, (last - j + 1) * wide)
            s = _dot(keys[h, at, :], state["q"], 1, 1)
            if j == 0:
                gap = lax.broadcasted_iota(jnp.int32, (wide, ch), 1) - lax.broadcasted_iota(jnp.int32, (wide, ch), 0)
                s = jnp.where(gap >= last * wide - i * ch, s, HIDDEN)
            state["s", j], state["v", j] = s, vals[h, :, at]

        def lead():
            z = zbuf[lax.rem(k + 1, 2)]
            state["q"] = turned(z[:, :HEAD])
            keys[h, here, :] = turned(z[:, HEAD:])
            scores(0)

        def block(j):
            if j + 1 < blocks:
                scores(j + 1)
            s = state.pop(("s", j))
            top = s.max(axis=0, keepdims=True)
            if j:
                top = jnp.maximum(state["top"], top)
            weights = jnp.exp2((s - top) * e).astype(BF16)
            mix = _dot(state.pop(("v", j)), weights, 1, 0)
            if j:
                mix = state["mix"] * jnp.exp2((state["top"] - top) * e) + mix
            state["top"], state["mix"] = top, mix
            if j == last:
                out = mix[:HEAD] * (1 / mix[HEAD : HEAD + 1])
                seen[:, pl.ds(pl.multiple_of(h * HEAD, HEAD), HEAD)] = out.T.astype(BF16)

        product(n, k, cut(blocks + 1), [lead, *(functools.partial(block, j) for j in range(blocks))])

    def values(n, i, k):
        def post():
            z, here = zbuf[lax.rem(k + 1, 2)], pl.ds(pl.multiple_of(i * ch, ch), ch)
            for m in range(2):
                vals[2 * lax.div(k, 3) + m, :HEAD, here] = z[:, m * HEAD : (m + 1) * HEAD].astype(BF16).T

        product(n, k, [0, depth], [post])

    def compute(i, k):
        n = i * units + k
        follows = (k > 1) & (lax.rem(k, 3) != 1)

        @pl.when(k < units)
        def _():
            @pl.when((n + 2 < nc * units) & ((n + 2 < units) | (n >= units)))
            def _():
                for_unit(n + 2, start)

            @pl.when(n == units - 2)
            def _():
                for m in range(2 * tiles):
                    wo_copy(m).start()

            for_unit(n, lambda copy: copy.wait())

            @pl.when(k == 0)
            def _():
                product(n, k, [0, depth], [lambda: None])

            @pl.when(lax.rem(k, 3) == 1)
            def _():
                values(n, i, k)

            for blocks in range(1, pl.cdiv(nc, WIDE) + 1):
                pl.when(follows & (lax.div(i, WIDE) == blocks - 1))(functools.partial(attention, n, i, k, blocks))

        for blocks in range(1, pl.cdiv(nc, WIDE) + 1):
            pl.when((k == units) & (lax.div(i, WIDE) == blocks - 1))(functools.partial(attention, None, i, k, blocks))

        @pl.when(k == units + 1)
        def _():
            @pl.when(i == 0)
            def _():
                for n in range(units, units + 2):
                    for_unit(n, start)

            @pl.when(i > 0)
            def _():
                for j in range(batch):
                    d2d_copy(i - 1, j).wait_send()

            def theirs(n, _):
                at = pl.multiple_of(n * tile, tile)
                pl.when(i == 0)(lambda: wo_copy(n).wait())
                part = _dot(seen[...], wo[:, pl.ds(pl.multiple_of(other + at, 128), tile)], 1, 0)
                stage[:, :, pl.ds(at, tile)] = part.astype(BF16).reshape(batch, sub, tile)

            lax.fori_loop(0, half // tile, theirs, None)
            for j in range(batch):
                d2d_copy(i, j).start()

        @pl.when(k == units + 2)
        def _():
            def ours(n, _):
                at = pl.multiple_of(n * tile, tile)
                pl.when(i == 0)(lambda: wo_copy(tiles + n).wait())
                part = _dot(seen[...], wo[:, pl.ds(pl.multiple_of(mine + at, 128), tile)], 1, 0)
                acc[lax.rem(i, 2), :, :, pl.ds(at, tile)] = part.reshape(batch, sub, tile)

            lax.fori_loop(0, half // tile, ours, None)

        @pl.when((k == units + 3) & (i + 1 < nc))
        def _():
            norm(i + 1)

            @pl.when(i + 2 < nc)
            def _():
                for r in range(ch // GROUP):
                    x_copy(i + 2, r).start()

    def valid(s):
        return (s >= 0) & (s < pieces)

    def sum_of(s):
        return acc.at[lax.rem(lax.div(s, batch), 2), lax.rem(s, batch)]

    def pair(s):
        at, ours = lax.rem(s, 2 * batch), sum_of(s)
        d2d_copy(lax.div(s, batch), lax.rem(s, batch)).wait_recv()

        @pl.when(inner)
        def _():
            ours[...] = ours[...] + d2d[at].astype(F32)

        @pl.when(jnp.logical_not(inner))
        def _():
            @pl.when(s >= nb)
            def _():
                up_copy(s - nb).wait_send()

            sendb[lax.rem(s, nb)] = (ours[...] + d2d[at].astype(F32)).astype(BF16)
            up_copy(s).start()

    def relay(s):
        up_copy(s).wait_recv()

        @pl.when(s >= nb)
        def _():
            cross_copy(s - nb).wait_send()

        sendb[lax.rem(s, nb)] = (sum_of(s)[...] + up[lax.rem(s, ring)].astype(F32)).astype(BF16)
        cross_copy(s).start()

    def sent(s):
        out_copies(s, lambda copy: copy.wait_send())
        pl.when(s < split)(lambda: local_copy(s).wait())

    def finish(s):
        b = lax.rem(s, nb)
        cross_copy(s).wait_recv()
        xres_copy(s).wait()

        @pl.when(s >= nb)
        def _():
            sent(s - nb)

        total = sendb[b].astype(F32) + cross[lax.rem(s, cring)].astype(F32)
        y = (xres[lax.rem(s, nx)].astype(F32) + total).astype(BF16)

        @pl.when(s < split)
        def _():
            resb[b] = y
            local_copy(s).start()

        @pl.when(s >= split)
        def _():
            y_ref[rows(s), pl.ds(mine, half)] = y

        out_copies(s, start)

    def arrived(s):
        b = lax.rem(s, ring)
        finished(s, lambda at, _: remote(at, at, part_send.at[0], res_recv.at[b], away).wait_recv())
        onward_copy(s, start)

    for r in range(ch // GROUP):
        x_copy(0, r).start()
    for n in range(2):
        for_unit(n, lambda copy: copy.start())
    barrier = pltpu.get_barrier_semaphore()
    pl.semaphore_signal(barrier, inc=1, device_id=partner, device_id_type=MESH)

    @pl.when(z < zs - 1)
    def _():
        pl.semaphore_signal(barrier, inc=1, device_id=above, device_id_type=MESH)

    @pl.when(z > 0)
    def _():
        pl.semaphore_signal(barrier, inc=1, device_id=below, device_id_type=MESH)

    def clear(h, _):
        keys[h] = jnp.zeros(keys.shape[1:], BF16)
        vals[h, :HEAD, :] = jnp.zeros((HEAD, vals.shape[2]), BF16)
        vals[h, HEAD:, :] = jnp.ones((vals.shape[1] - HEAD, vals.shape[2]), BF16)

    lax.fori_loop(0, heads, clear, None)
    for n in range(depth // 128):
        gain[:, n * 128 : (n + 1) * 128] = gain_ref[n : n + 1, :].astype(F32)
    norm(0)
    for r in range(ch // GROUP):
        x_copy(1, r).start()
    pl.semaphore_wait(barrier, 1 + jnp.where(z < zs - 1, 1, 0) + jnp.where(z > 0, 1, 0))

    def served(g, stage, do):
        s = g - lag1 - LAGS[stage] - jnp.clip(g - turn, 0, GROWN[stage])
        pl.when(valid(s) & ((g <= turn) | (g > turn + GROWN[stage])))(functools.partial(do, s))

    def serve(g):
        pl.when(jnp.logical_not(inner))(lambda: served(g, 3, arrived))

        @pl.when(inner)
        def _():
            served(g, 2, finish)
            served(g + 2, 2, lambda s: xres_copy(s).start())
            served(g, 1, relay)

        served(g, 0, pair)

    homes = [
        pltpu.make_async_copy(early.at[pl.ds(r * GROUP, GROUP), :], y_ref.at[pl.ds(r * GROUP, GROUP), :], home_sem.at[r])
        for r in range(early.shape[0] // GROUP)
    ]

    def theirs_arrived(which, y):
        at = y.at[:, pl.ds(other, half)]
        remote(at, at, part_send.at[which], part_recv.at[which], partner).wait_recv()

    def slot(g, _):
        i, k = lax.div(g, per), lax.rem(g, per)
        pl.when(lax.rem(g, 2) == 0)(lambda: serve(lax.div(g, 2)))
        pl.when(i < nc)(lambda: compute(i, k))

        @pl.when(g == max(nc * per, 2 * (split + last_lag)))
        def _():
            theirs_arrived(0, early)
            for copy in homes:
                copy.start()

    lax.fori_loop(0, 2 * (pieces + last_lag), slot, None)

    for j in range(batch):
        d2d_copy(nc - 1, j).wait_send()
    for s in range(pieces - nb, pieces):
        up_copy(s).wait_send()

    @pl.when(inner)
    def _():
        for s in range(pieces - nb, pieces):
            sent(s)

    rest = y_ref.at[early.shape[0] :, :]
    theirs_arrived(1, rest)
    for which, y in enumerate((early, rest)):
        ours = y.at[:, pl.ds(mine, half)]
        pl.when(jnp.logical_not(inner))(remote(ours, ours, part_send.at[which], part_recv.at[which], partner).wait_send)
    for copy in homes:
        copy.wait()


def _placed(y_in, y_out, sem):
    size = y_in.shape[0] // sem.shape[0]
    copies = [pltpu.make_async_copy(y_in.at[pl.ds(r, size), :], y_out.at[pl.ds(r, size), :], sem.at[r // size]) for r in range(0, y_in.shape[0], size)]
    for copy in copies:
        copy.start()
    for copy in copies:
        copy.wait()


def _tables(nc, ch):
    rate = THETA ** (-np.arange(HEAD // 2) / (HEAD // 2))
    sign = np.repeat([-1.0, 1.0], HEAD // 2)

    def both(place):
        angle = np.tile(place[:, None] * rate, (1, 2))
        return np.stack([np.cos(angle), np.sin(angle) * sign]).astype(np.float32)

    return both(np.arange(nc) * ch), both(np.arange(ch))


def solution(mesh, ch=128, tile=1792, copy_rows=128):
    names = mesh.axis_names
    zs = mesh.shape["tp"] // 2

    def step(x, gain, wq, wk, wv, wo):
        n, d = x.shape
        heads = wq.shape[1] // HEAD
        nc, half = n // ch, d // 2
        per = 3 * (heads // 2) + 7
        sub = 2 * ch // per
        base, fine = _tables(nc, ch)
        cfg = dict(ch=ch, sub=sub, per=per, heads=heads, nc=nc, half=half, zs=zs, tile=min(tile, half), names=names)
        wide, batch = min(tile, half), per // 2
        nb, ring, cring, nx = 6, 13, 8, 4
        dma = pltpu.SemaphoreType.DMA
        hbm, vmem = pl.BlockSpec(memory_space=pl.ANY), pl.BlockSpec(memory_space=pltpu.VMEM)
        _, y = pl.pallas_call(
            functools.partial(_kernel, cfg),
            out_shape=[jax.ShapeDtypeStruct((heads * HEAD, d), BF16), pltpu.VMEM((n, d), BF16)],
            in_specs=[hbm, vmem, vmem, vmem, hbm, hbm, hbm, hbm],
            out_specs=[hbm, vmem],
            scratch_shapes=[
                pltpu.VMEM((heads, n, HEAD), BF16),
                pltpu.VMEM((heads + 1, HEAD + 8, n), BF16),
                pltpu.VMEM((3, d, 2 * HEAD), BF16),
                pltpu.VMEM((2, ch, 2 * HEAD), F32),
                pltpu.VMEM((ch, d), BF16),
                pltpu.VMEM((ch, d), BF16),
                pltpu.VMEM((2, batch, sub, half), F32),
                pltpu.VMEM((batch, sub, half), BF16),
                pltpu.VMEM((ch, heads * HEAD), BF16),
                pltpu.VMEM((2 * batch, sub, half), BF16),
                pltpu.VMEM((ring, sub, half), BF16),
                pltpu.VMEM((cring, sub, half), BF16),
                pltpu.VMEM((nb, sub, half), BF16),
                pltpu.VMEM((nb, sub, half), BF16),
                pltpu.VMEM((nx, sub, half), BF16),
                pltpu.VMEM((ch, HEAD), F32),
                pltpu.VMEM((ch, HEAD), F32),
                pltpu.VMEM((1, d), F32),
                dma((3, 2)), dma((2 * half // wide,)), dma((ch // GROUP,)), dma((nx,)),
                dma((batch,)), dma((2 * batch,)), dma((ring,)), dma((cring,)), dma((ring,)),
                dma((nb,)), dma((nb,)), dma((nb,)), dma((nb,)), dma((2,)), dma((2,)),
                dma((heads * HEAD // GROUP,)),
            ],
            compiler_params=pltpu.CompilerParams(collective_id=0, has_side_effects=True, vmem_limit_bytes=KERNEL_VMEM),
            name="attention_half",
        )(x, gain.reshape(d // 128, 128), jnp.asarray(base), jnp.asarray(fine), wq, wk, wv, wo)
        return pl.pallas_call(
            _placed,
            out_shape=jax.ShapeDtypeStruct((n, d), BF16),
            in_specs=[vmem],
            out_specs=hbm,
            scratch_shapes=[dma((n // copy_rows,))],
            compiler_params=pltpu.CompilerParams(vmem_limit_bytes=2**20),
            name="placed",
        )(pltpu.with_memory_space_constraint(y, pltpu.VMEM))

    tokens, columns = P("dp", None), P(None, "tp")
    return jax.shard_map(
        step,
        mesh=mesh,
        in_specs=(tokens, P(None), columns, columns, columns, P("tp", None)),
        out_specs=tokens,
        check_vma=False,
    )
```

```python
import functools

import jax
import jax.numpy as jnp
import numpy as np
from jax import lax
from jax.experimental import pallas as pl
from jax.experimental.pallas import tpu as pltpu
from jax.sharding import PartitionSpec as P

HEAD = 128
THETA = 10000
LOG2E = 1.4426950408889634
HIDDEN = -2e30
MESH = pl.DeviceIdType.MESH
BF16, F32 = jnp.bfloat16, jnp.float32
LAGS = (0, 2, 5, 12)
GROUP = 64
KERNEL_VMEM = 37_500_000
WIDE = 4


def _dot(a, b, ca, cb):
    return lax.dot_general(a, b, (((ca,), (cb,)), ((), ())), preferred_element_type=F32)


def _kernel(cfg, x_hbm, gain_ref, base_ref, fine_ref, wq_hbm, wk_hbm, wv_hbm, wo_hbm, early, y_ref,
            keys, vals, wbuf, zbuf, xbuf, abuf, acc, stage, seen, d2d, up, cross, sendb, resb, xres, rotc, rots, gain,
            w_sem, wo_sem, x_sem, xres_sem, d2d_send, d2d_recv, up_recv, cross_recv, res_recv,
            send_a, send_b, send_c, send_l, part_send, part_recv, home_sem):
    ch, sub, per, heads, nc, half, zs, tile, names = (cfg[k] for k in ("ch", "sub", "per", "heads", "nc", "half", "zs", "tile", "names"))
    depth = 2 * half
    units = 3 * (heads // 2) + 2
    batch = per // 2
    pieces = nc * batch
    e = HEAD**-0.5 * LOG2E
    lag1 = (units + 4) // 2
    last_lag = lag1 + LAGS[3]
    ring, cring, nb, nx = up.shape[0], cross.shape[0], sendb.shape[0], xres.shape[0]
    wo, split = y_ref.at[: early.shape[0], :], early.shape[0] // sub

    dpi, t = lax.axis_index(names[0]), lax.axis_index(names[1])
    core, z = lax.rem(t, 2), lax.div(t, 2)
    inner = (z > 0) & (z < zs - 1)
    partner, above, below = (dpi, t + 1 - 2 * core), (dpi, t + 2), (dpi, t - 2)
    toward = (dpi, jnp.where(z < zs // 2, t + 2, t - 2))
    away = (dpi, jnp.where(z < zs // 2, t - 2, t + 2))
    mine = pl.multiple_of(core * half, 128)
    other = pl.multiple_of((1 - core) * half, 128)

    def rows(s):
        return pl.ds(pl.multiple_of(s * sub, sub), sub)

    def finished(s, act):
        cols = pl.ds(mine, half)
        pl.when(s < split)(lambda: act(early.at[rows(s), cols], 0))
        pl.when(s >= split)(lambda: act(y_ref.at[rows(s), cols], 1))

    def remote(src, dst, send, recv, device):
        return pltpu.make_async_remote_copy(src_ref=src, dst_ref=dst, send_sem=send, recv_sem=recv, device_id=device, device_id_type=MESH)

    def x_copy(i, r):
        at = pl.ds(r * GROUP, GROUP)
        return pltpu.make_async_copy(x_hbm.at[pl.ds(pl.multiple_of(i * ch + r * GROUP, GROUP), GROUP), :], xbuf.at[at, :], x_sem.at[r])

    def for_unit(n, act):
        k, at = lax.rem(n, units), lax.rem(n, 3)
        group, kind = lax.div(k, 3), lax.rem(k, 3)

        def columns(w, h, wide):
            return w.at[:, pl.ds(pl.multiple_of(h * HEAD, HEAD), wide * HEAD)]

        @pl.when((kind == 0) & (2 * group + 1 < heads))
        def _():
            act(pltpu.make_async_copy(columns(wv_hbm, 2 * group, 2), wbuf.at[at], w_sem.at[at, 0]))

        @pl.when((kind == 0) & (2 * group + 1 == heads))
        def _():
            act(pltpu.make_async_copy(columns(wv_hbm, 2 * group, 1), wbuf.at[at, :, :HEAD], w_sem.at[at, 0]))

        @pl.when(kind > 0)
        def _():
            h = 2 * group + kind - 1
            act(pltpu.make_async_copy(columns(wq_hbm, h, 1), wbuf.at[at, :, :HEAD], w_sem.at[at, 0]))
            act(pltpu.make_async_copy(columns(wk_hbm, h, 1), wbuf.at[at, :, HEAD:], w_sem.at[at, 1]))

    tiles = half // tile

    def wo_copy(m):
        at = jnp.where(m < tiles, other + m * tile, mine + (m - tiles) * tile)
        part = pl.ds(pl.multiple_of(at, 128), tile)
        return pltpu.make_async_copy(wo_hbm.at[:, part], wo.at[:, part], wo_sem.at[m])

    def xres_copy(s):
        b = lax.rem(s, nx)
        return pltpu.make_async_copy(x_hbm.at[rows(s), pl.ds(mine, half)], xres.at[b], xres_sem.at[b])

    def d2d_copy(c, k):
        at = lax.rem(c, 2) * batch + k
        return remote(stage.at[k], d2d.at[at], d2d_send.at[k], d2d_recv.at[at], partner)

    def up_copy(s):
        b, r = lax.rem(s, nb), lax.rem(s, ring)
        return remote(sendb.at[b], up.at[r], send_a.at[b], up_recv.at[r], toward)

    def cross_copy(s):
        b, r = lax.rem(s, nb), lax.rem(s, cring)
        return remote(sendb.at[b], cross.at[r], send_a.at[b], cross_recv.at[r], toward)

    def out_copies(s, act):
        b = lax.rem(s, nb)

        def both(at, which):
            src = at if which else resb.at[b]
            act(remote(src, at, send_b.at[b], res_recv.at[lax.rem(s, ring)], away))
            act(remote(src, at, send_c.at[b], part_recv.at[which], partner))

        finished(s, both)

    def local_copy(s):
        b = lax.rem(s, nb)
        return pltpu.make_async_copy(resb.at[b], early.at[rows(s), pl.ds(mine, half)], send_l.at[b])

    def onward_copy(s, act):
        finished(s, lambda at, which: act(remote(at, at, part_send.at[which], part_recv.at[which], partner)))

    def start(copy):
        copy.start()

    def norm(i):
        bc, bs = base_ref[0, pl.ds(i, 1), :], base_ref[1, pl.ds(i, 1), :]
        rotc[...] = bc * fine_ref[0] - bs * fine_ref[1]
        rots[...] = bs * fine_ref[0] + bc * fine_ref[1]

        def group(r, _):
            x_copy(i, r).wait()
            at = pl.ds(pl.multiple_of(r * GROUP, GROUP), GROUP)
            cols = [slice(c, c + 128) for c in range(0, depth, 128)]
            sums = [None] * 4
            for n, c in enumerate(cols):
                wide = xbuf[at, c].astype(F32)
                sums[n % 4] = wide * wide if sums[n % 4] is None else sums[n % 4] + wide * wide
            total = functools.reduce(jnp.add, [s for s in sums if s is not None])
            scale = lax.rsqrt(jnp.sum(total, -1, keepdims=True) * (1 / depth) + 1e-6)
            scale = jnp.broadcast_to(scale, (GROUP, 128))
            for c in cols:
                abuf[at, c] = (xbuf[at, c].astype(F32) * scale * gain[:, c]).astype(BF16)

        lax.fori_loop(0, ch // GROUP, group, None)

    def turned(v):
        v = v.astype(BF16).astype(F32)
        return (v * rotc[...] + pltpu.roll(v, HEAD // 2, 1) * rots[...]).astype(BF16)

    def product(n, k, cuts, between):
        if n is None:
            for do in between:
                do()
            return
        at, total = lax.rem(n, 3), None
        for lo, hi, do in zip(cuts, cuts[1:], between):
            if lo < hi:
                part = _dot(abuf[:, lo:hi], wbuf[at, lo:hi, :], 1, 0)
                total = part if total is None else total + part
            do()
        zbuf[lax.rem(k, 2)] = total

    def cut(parts):
        lead = 1 / 7 if parts > 1 else 1
        ends = [0, lead] + [lead + (1 - lead) * (j + 1) / max(parts - 1, 1) for j in range(parts - 1)]
        return [min(round(f * depth / 256) * 256, depth) for f in ends]

    def attention(n, i, k, blocks):
        h = jnp.where(lax.rem(k, 3) == 2, 2 * lax.div(k, 3), 2 * lax.div(k, 3) - 1)
        here = pl.ds(pl.multiple_of(i * ch, ch), ch)
        wide, last = WIDE * ch, blocks - 1
        state = {}

        def scores(j):
            at = slice((last - j) * wide, (last - j + 1) * wide)
            s = _dot(keys[h, at, :], state["q"], 1, 1)
            if j == 0:
                gap = lax.broadcasted_iota(jnp.int32, (wide, ch), 1) - lax.broadcasted_iota(jnp.int32, (wide, ch), 0)
                s = jnp.where(gap >= last * wide - i * ch, s, HIDDEN)
            state["s", j], state["v", j] = s, vals[h, :, at]

        def lead():
            z = zbuf[lax.rem(k + 1, 2)]
            state["q"] = turned(z[:, :HEAD])
            keys[h, here, :] = turned(z[:, HEAD:])
            scores(0)

        def block(j):
            if j + 1 < blocks:
                scores(j + 1)
            s = state.pop(("s", j))
            top = s.max(axis=0, keepdims=True)
            if j:
                top = jnp.maximum(state["top"], top)
            weights = jnp.exp2((s - top) * e).astype(BF16)
            mix = _dot(state.pop(("v", j)), weights, 1, 0)
            if j:
                mix = state["mix"] * jnp.exp2((state["top"] - top) * e) + mix
            state["top"], state["mix"] = top, mix
            if j == last:
                out = mix[:HEAD] * (1 / mix[HEAD : HEAD + 1])
                seen[:, pl.ds(pl.multiple_of(h * HEAD, HEAD), HEAD)] = out.T.astype(BF16)

        product(n, k, cut(blocks + 1), [lead, *(functools.partial(block, j) for j in range(blocks))])

    def values(n, i, k):
        def post():
            z, here = zbuf[lax.rem(k + 1, 2)], pl.ds(pl.multiple_of(i * ch, ch), ch)
            for m in range(2):
                vals[2 * lax.div(k, 3) + m, :HEAD, here] = z[:, m * HEAD : (m + 1) * HEAD].astype(BF16).T

        product(n, k, [0, depth], [post])

    def compute(i, k):
        n = i * units + k
        follows = (k > 1) & (lax.rem(k, 3) != 1)

        @pl.when(k < units)
        def _():
            @pl.when((n + 2 < nc * units) & ((n + 2 < units) | (n >= units)))
            def _():
                for_unit(n + 2, start)

            @pl.when(n == units - 2)
            def _():
                for m in range(2 * tiles):
                    wo_copy(m).start()

            for_unit(n, lambda copy: copy.wait())

            @pl.when(k == 0)
            def _():
                product(n, k, [0, depth], [lambda: None])

            @pl.when(lax.rem(k, 3) == 1)
            def _():
                values(n, i, k)

            for blocks in range(1, pl.cdiv(nc, WIDE) + 1):
                pl.when(follows & (lax.div(i, WIDE) == blocks - 1))(functools.partial(attention, n, i, k, blocks))

        for blocks in range(1, pl.cdiv(nc, WIDE) + 1):
            pl.when((k == units) & (lax.div(i, WIDE) == blocks - 1))(functools.partial(attention, None, i, k, blocks))

        @pl.when(k == units + 1)
        def _():
            @pl.when(i > 0)
            def _():
                for j in range(batch):
                    d2d_copy(i - 1, j).wait_send()

            def theirs(n, _):
                at = pl.multiple_of(n * tile, tile)
                pl.when(i == 0)(lambda: wo_copy(n).wait())
                part = _dot(seen[...], wo[:, pl.ds(pl.multiple_of(other + at, 128), tile)], 1, 0)
                stage[:, :, pl.ds(at, tile)] = part.astype(BF16).reshape(batch, sub, tile)

            lax.fori_loop(0, half // tile, theirs, None)
            for j in range(batch):
                d2d_copy(i, j).start()

        @pl.when(k == units + 2)
        def _():
            def ours(n, _):
                at = pl.multiple_of(n * tile, tile)
                pl.when(i == 0)(lambda: wo_copy(tiles + n).wait())
                part = _dot(seen[...], wo[:, pl.ds(pl.multiple_of(mine + at, 128), tile)], 1, 0)
                acc[lax.rem(i, 2), :, :, pl.ds(at, tile)] = part.reshape(batch, sub, tile)

            lax.fori_loop(0, half // tile, ours, None)

            @pl.when(i == 0)
            def _():
                for r in range(ch // GROUP):
                    x_copy(1, r).start()
                for n in range(units, units + 2):
                    for_unit(n, start)

        @pl.when((k == units + 3) & (i + 1 < nc))
        def _():
            norm(i + 1)

            @pl.when(i + 2 < nc)
            def _():
                for r in range(ch // GROUP):
                    x_copy(i + 2, r).start()

    def valid(s):
        return (s >= 0) & (s < pieces)

    def sum_of(s):
        return acc.at[lax.rem(lax.div(s, batch), 2), lax.rem(s, batch)]

    def pair(s):
        at, ours = lax.rem(s, 2 * batch), sum_of(s)
        d2d_copy(lax.div(s, batch), lax.rem(s, batch)).wait_recv()

        @pl.when(inner)
        def _():
            ours[...] = ours[...] + d2d[at].astype(F32)

        @pl.when(jnp.logical_not(inner))
        def _():
            @pl.when(s >= nb)
            def _():
                up_copy(s - nb).wait_send()

            sendb[lax.rem(s, nb)] = (ours[...] + d2d[at].astype(F32)).astype(BF16)
            up_copy(s).start()

    def relay(s):
        up_copy(s).wait_recv()

        @pl.when(s >= nb)
        def _():
            cross_copy(s - nb).wait_send()

        sendb[lax.rem(s, nb)] = (sum_of(s)[...] + up[lax.rem(s, ring)].astype(F32)).astype(BF16)
        cross_copy(s).start()

    def sent(s):
        out_copies(s, lambda copy: copy.wait_send())
        pl.when(s < split)(lambda: local_copy(s).wait())

    def finish(s):
        b = lax.rem(s, nb)
        cross_copy(s).wait_recv()
        xres_copy(s).wait()

        @pl.when(s >= nb)
        def _():
            sent(s - nb)

        total = sendb[b].astype(F32) + cross[lax.rem(s, cring)].astype(F32)
        y = (xres[lax.rem(s, nx)].astype(F32) + total).astype(BF16)

        @pl.when(s < split)
        def _():
            resb[b] = y
            local_copy(s).start()

        @pl.when(s >= split)
        def _():
            y_ref[rows(s), pl.ds(mine, half)] = y

        out_copies(s, start)

    def arrived(s):
        b = lax.rem(s, ring)
        finished(s, lambda at, _: remote(at, at, part_send.at[0], res_recv.at[b], away).wait_recv())
        onward_copy(s, start)

    for r in range(ch // GROUP):
        x_copy(0, r).start()
    for n in range(2):
        for_unit(n, lambda copy: copy.start())
    barrier = pltpu.get_barrier_semaphore()
    pl.semaphore_signal(barrier, inc=1, device_id=partner, device_id_type=MESH)

    @pl.when(z < zs - 1)
    def _():
        pl.semaphore_signal(barrier, inc=1, device_id=above, device_id_type=MESH)

    @pl.when(z > 0)
    def _():
        pl.semaphore_signal(barrier, inc=1, device_id=below, device_id_type=MESH)

    def clear(h, _):
        keys[h] = jnp.zeros(keys.shape[1:], BF16)
        vals[h, :HEAD, :] = jnp.zeros((HEAD, vals.shape[2]), BF16)
        vals[h, HEAD:, :] = jnp.ones((vals.shape[1] - HEAD, vals.shape[2]), BF16)

    lax.fori_loop(0, heads, clear, None)
    for n in range(depth // 128):
        gain[:, n * 128 : (n + 1) * 128] = gain_ref[n : n + 1, :].astype(F32)
    norm(0)
    pl.semaphore_wait(barrier, 1 + jnp.where(z < zs - 1, 1, 0) + jnp.where(z > 0, 1, 0))

    def served(g, stage, do):
        s = g - lag1 - LAGS[stage]
        pl.when(valid(s))(functools.partial(do, s))

    def serve(g):
        pl.when(jnp.logical_not(inner))(lambda: served(g, 3, arrived))

        @pl.when(inner)
        def _():
            served(g, 2, finish)
            served(g + 2, 2, lambda s: xres_copy(s).start())

        served(g, 0, pair)

    homes = [
        pltpu.make_async_copy(early.at[pl.ds(r * GROUP, GROUP), :], y_ref.at[pl.ds(r * GROUP, GROUP), :], home_sem.at[r])
        for r in range(early.shape[0] // GROUP)
    ]

    def theirs_arrived(which, y):
        at = y.at[:, pl.ds(other, half)]
        remote(at, at, part_send.at[which], part_recv.at[which], partner).wait_recv()

    def slot(g, _):
        i, k = lax.div(g, per), lax.rem(g, per)
        pl.when(lax.rem(g, 2) == 0)(lambda: serve(lax.div(g, 2)))
        pl.when((lax.rem(g, 2) == 1) & inner)(lambda: served(lax.div(g, 2), 1, relay))
        pl.when(i < nc)(lambda: compute(i, k))

        @pl.when(g == max(nc * per, 2 * (split + last_lag)))
        def _():
            theirs_arrived(0, early)
            for copy in homes:
                copy.start()

    lax.fori_loop(0, 2 * (pieces + last_lag), slot, None)

    for j in range(batch):
        d2d_copy(nc - 1, j).wait_send()
    for s in range(pieces - nb, pieces):
        up_copy(s).wait_send()

    @pl.when(inner)
    def _():
        for s in range(pieces - nb, pieces):
            sent(s)

    rest = y_ref.at[early.shape[0] :, :]
    theirs_arrived(1, rest)
    for which, y in enumerate((early, rest)):
        ours = y.at[:, pl.ds(mine, half)]
        pl.when(jnp.logical_not(inner))(remote(ours, ours, part_send.at[which], part_recv.at[which], partner).wait_send)
    for copy in homes:
        copy.wait()


def _placed(y_in, y_out, sem):
    size = y_in.shape[0] // sem.shape[0]
    copies = [pltpu.make_async_copy(y_in.at[pl.ds(r, size), :], y_out.at[pl.ds(r, size), :], sem.at[r // size]) for r in range(0, y_in.shape[0], size)]
    for copy in copies:
        copy.start()
    for copy in copies:
        copy.wait()


def _tables(nc, ch):
    rate = THETA ** (-np.arange(HEAD // 2) / (HEAD // 2))
    sign = np.repeat([-1.0, 1.0], HEAD // 2)

    def both(place):
        angle = np.tile(place[:, None] * rate, (1, 2))
        return np.stack([np.cos(angle), np.sin(angle) * sign]).astype(np.float32)

    return both(np.arange(nc) * ch), both(np.arange(ch))


def solution(mesh, ch=128, tile=1792, copy_rows=128):
    names = mesh.axis_names
    zs = mesh.shape["tp"] // 2

    def step(x, gain, wq, wk, wv, wo):
        n, d = x.shape
        heads = wq.shape[1] // HEAD
        nc, half = n // ch, d // 2
        per = 3 * (heads // 2) + 7
        sub = 2 * ch // per
        base, fine = _tables(nc, ch)
        cfg = dict(ch=ch, sub=sub, per=per, heads=heads, nc=nc, half=half, zs=zs, tile=min(tile, half), names=names)
        wide, batch = min(tile, half), per // 2
        nb, ring, cring, nx = 6, 13, 8, 4
        dma = pltpu.SemaphoreType.DMA
        hbm, vmem = pl.BlockSpec(memory_space=pl.ANY), pl.BlockSpec(memory_space=pltpu.VMEM)
        _, y = pl.pallas_call(
            functools.partial(_kernel, cfg),
            out_shape=[jax.ShapeDtypeStruct((heads * HEAD, d), BF16), pltpu.VMEM((n, d), BF16)],
            in_specs=[hbm, vmem, vmem, vmem, hbm, hbm, hbm, hbm],
            out_specs=[hbm, vmem],
            scratch_shapes=[
                pltpu.VMEM((heads, n, HEAD), BF16),
                pltpu.VMEM((heads + 1, HEAD + 8, n), BF16),
                pltpu.VMEM((3, d, 2 * HEAD), BF16),
                pltpu.VMEM((2, ch, 2 * HEAD), F32),
                pltpu.VMEM((ch, d), BF16),
                pltpu.VMEM((ch, d), BF16),
                pltpu.VMEM((2, batch, sub, half), F32),
                pltpu.VMEM((batch, sub, half), BF16),
                pltpu.VMEM((ch, heads * HEAD), BF16),
                pltpu.VMEM((2 * batch, sub, half), BF16),
                pltpu.VMEM((ring, sub, half), BF16),
                pltpu.VMEM((cring, sub, half), BF16),
                pltpu.VMEM((nb, sub, half), BF16),
                pltpu.VMEM((nb, sub, half), BF16),
                pltpu.VMEM((nx, sub, half), BF16),
                pltpu.VMEM((ch, HEAD), F32),
                pltpu.VMEM((ch, HEAD), F32),
                pltpu.VMEM((1, d), F32),
                dma((3, 2)), dma((2 * half // wide,)), dma((ch // GROUP,)), dma((nx,)),
                dma((batch,)), dma((2 * batch,)), dma((ring,)), dma((cring,)), dma((ring,)),
                dma((nb,)), dma((nb,)), dma((nb,)), dma((nb,)), dma((2,)), dma((2,)),
                dma((heads * HEAD // GROUP,)),
            ],
            compiler_params=pltpu.CompilerParams(collective_id=0, has_side_effects=True, vmem_limit_bytes=KERNEL_VMEM),
            name="attention_half",
        )(x, gain.reshape(d // 128, 128), jnp.asarray(base), jnp.asarray(fine), wq, wk, wv, wo)
        return pl.pallas_call(
            _placed,
            out_shape=jax.ShapeDtypeStruct((n, d), BF16),
            in_specs=[vmem],
            out_specs=hbm,
            scratch_shapes=[dma((n // copy_rows,))],
            compiler_params=pltpu.CompilerParams(vmem_limit_bytes=2**20),
            name="placed",
        )(pltpu.with_memory_space_constraint(y, pltpu.VMEM))

    tokens, columns = P("dp", None), P(None, "tp")
    return jax.shard_map(
        step,
        mesh=mesh,
        in_specs=(tokens, P(None), columns, columns, columns, P("tp", None)),
        out_specs=tokens,
        check_vma=False,
    )
```

```python
import functools

import jax
import jax.numpy as jnp
import numpy as np
from jax import lax
from jax.experimental import pallas as pl
from jax.experimental.pallas import tpu as pltpu
from jax.sharding import PartitionSpec as P

HEAD = 128
THETA = 10000
LOG2E = 1.4426950408889634
HIDDEN = -2e30
MESH = pl.DeviceIdType.MESH
BF16, F32 = jnp.bfloat16, jnp.float32
LAGS = (0, 2, 5, 9)
GROUP = 64
KERNEL_VMEM = 37_600_000
WIDE = 4
AHEAD = 3


def _dot(a, b, ca, cb):
    return lax.dot_general(a, b, (((ca,), (cb,)), ((), ())), preferred_element_type=F32)


def _kernel(cfg, x_hbm, gain_ref, base_ref, fine_ref, wq_hbm, wk_hbm, wv_hbm, wo_hbm, early, y_ref,
            keys, vals, wbuf, zbuf, abuf, acc, stage, seen, d2d, up, cross, sendb, resb, xres, rotc, rots, gain,
            w_sem, wo_sem, x_sem, xres_sem, d2d_send, d2d_recv, up_recv, cross_recv, res_recv,
            send_a, send_b, send_c, send_l, part_send, part_recv, home_sem):
    ch, sub, per, heads, nc, half, zs, tile, names = (cfg[k] for k in ("ch", "sub", "per", "heads", "nc", "half", "zs", "tile", "names"))
    depth = 2 * half
    units = 3 * (heads // 2) + 2
    batch = per // 2
    pieces = nc * batch
    e = HEAD**-0.5 * LOG2E
    lag1 = (units + 4) // 2
    last_lag = lag1 + LAGS[3]
    ring, cring, nb, nx = up.shape[0], cross.shape[0], sendb.shape[0], xres.shape[0]
    wo, split = y_ref.at[: early.shape[0], :], early.shape[0] // sub
    xbuf = y_ref.at[(nc - 1) * ch :, :]

    dpi, t = lax.axis_index(names[0]), lax.axis_index(names[1])
    core, z = lax.rem(t, 2), lax.div(t, 2)
    inner = (z > 0) & (z < zs - 1)
    partner, above, below = (dpi, t + 1 - 2 * core), (dpi, t + 2), (dpi, t - 2)
    toward = (dpi, jnp.where(z < zs // 2, t + 2, t - 2))
    away = (dpi, jnp.where(z < zs // 2, t - 2, t + 2))
    mine = pl.multiple_of(core * half, 128)
    other = pl.multiple_of((1 - core) * half, 128)

    def rows(s):
        return pl.ds(pl.multiple_of(s * sub, sub), sub)

    def finished(s, act):
        cols = pl.ds(mine, half)
        pl.when(s < split)(lambda: act(early.at[rows(s), cols], 0))
        pl.when(s >= split)(lambda: act(y_ref.at[rows(s), cols], 1))

    def remote(src, dst, send, recv, device):
        return pltpu.make_async_remote_copy(src_ref=src, dst_ref=dst, send_sem=send, recv_sem=recv, device_id=device, device_id_type=MESH)

    def x_copy(i, r):
        at = pl.ds(r * GROUP, GROUP)
        return pltpu.make_async_copy(x_hbm.at[pl.ds(pl.multiple_of(i * ch + r * GROUP, GROUP), GROUP), :], xbuf.at[at, :], x_sem.at[r])

    def for_unit(n, act):
        k, at = lax.rem(n, units), lax.rem(n, AHEAD + 1)
        group, kind = lax.div(k, 3), lax.rem(k, 3)

        def columns(w, h, wide):
            return w.at[:, pl.ds(pl.multiple_of(h * HEAD, HEAD), wide * HEAD)]

        @pl.when((kind == 0) & (2 * group + 1 < heads))
        def _():
            act(pltpu.make_async_copy(columns(wv_hbm, 2 * group, 2), wbuf.at[at], w_sem.at[at, 0]))

        @pl.when((kind == 0) & (2 * group + 1 == heads))
        def _():
            act(pltpu.make_async_copy(columns(wv_hbm, 2 * group, 1), wbuf.at[at, :, :HEAD], w_sem.at[at, 0]))

        @pl.when(kind > 0)
        def _():
            h = 2 * group + kind - 1
            act(pltpu.make_async_copy(columns(wq_hbm, h, 1), wbuf.at[at, :, :HEAD], w_sem.at[at, 0]))
            act(pltpu.make_async_copy(columns(wk_hbm, h, 1), wbuf.at[at, :, HEAD:], w_sem.at[at, 1]))

    tiles = half // tile

    def wo_copy(m):
        at = jnp.where(m < tiles, other + m * tile, mine + (m - tiles) * tile)
        part = pl.ds(pl.multiple_of(at, 128), tile)
        return pltpu.make_async_copy(wo_hbm.at[:, part], wo.at[:, part], wo_sem.at[m])

    def xres_copy(s):
        b = lax.rem(s, nx)
        return pltpu.make_async_copy(x_hbm.at[rows(s), pl.ds(mine, half)], xres.at[b], xres_sem.at[b])

    def d2d_copy(c, k):
        at = lax.rem(c, 2) * batch + k
        return remote(stage.at[k], d2d.at[at], d2d_send.at[k], d2d_recv.at[at], partner)

    def up_copy(s):
        b, r = lax.rem(s, nb), lax.rem(s, ring)
        return remote(sendb.at[b], up.at[r], send_a.at[b], up_recv.at[r], toward)

    def cross_copy(s):
        b, r = lax.rem(s, nb), lax.rem(s, cring)
        return remote(sendb.at[b], cross.at[r], send_a.at[b], cross_recv.at[r], toward)

    def out_copies(s, act):
        b = lax.rem(s, nb)

        def both(at, which):
            src = at if which else resb.at[b]
            act(remote(src, at, send_b.at[b], res_recv.at[lax.rem(s, ring)], away))
            act(remote(src, at, send_c.at[b], part_recv.at[which], partner))

        finished(s, both)

    def local_copy(s):
        b = lax.rem(s, nb)
        return pltpu.make_async_copy(resb.at[b], early.at[rows(s), pl.ds(mine, half)], send_l.at[b])

    def onward_copy(s, act):
        finished(s, lambda at, which: act(remote(at, at, part_send.at[which], part_recv.at[which], partner)))

    def start(copy):
        copy.start()

    def norm(i):
        bc, bs = base_ref[0, pl.ds(i, 1), :], base_ref[1, pl.ds(i, 1), :]
        rotc[...] = bc * fine_ref[0] - bs * fine_ref[1]
        rots[...] = bs * fine_ref[0] + bc * fine_ref[1]

        def group(r, _):
            x_copy(i, r).wait()
            at = pl.ds(pl.multiple_of(r * GROUP, GROUP), GROUP)
            cols = [slice(c, c + 128) for c in range(0, depth, 128)]
            sums = [None] * 4
            for n, c in enumerate(cols):
                wide = xbuf[at, c].astype(F32)
                sums[n % 4] = wide * wide if sums[n % 4] is None else sums[n % 4] + wide * wide
            total = functools.reduce(jnp.add, [s for s in sums if s is not None])
            scale = lax.rsqrt(jnp.sum(total, -1, keepdims=True) * (1 / depth) + 1e-6)
            scale = jnp.broadcast_to(scale, (GROUP, 128))
            for c in cols:
                abuf[at, c] = (xbuf[at, c].astype(F32) * scale * gain[:, c]).astype(BF16)

        lax.fori_loop(0, ch // GROUP, group, None)

    def turned(v):
        v = v.astype(BF16).astype(F32)
        return (v * rotc[...] + pltpu.roll(v, HEAD // 2, 1) * rots[...]).astype(BF16)

    def product(n, k, cuts, between):
        if n is None:
            for do in between:
                do()
            return
        at, total = lax.rem(n, AHEAD + 1), None
        for lo, hi, do in zip(cuts, cuts[1:], between):
            if lo < hi:
                part = _dot(abuf[:, lo:hi], wbuf[at, lo:hi, :], 1, 0)
                total = part if total is None else total + part
            do()
        zbuf[lax.rem(k, 2)] = total

    def cut(parts):
        lead = 1 / 7 if parts > 1 else 1
        ends = [0, lead] + [lead + (1 - lead) * (j + 1) / max(parts - 1, 1) for j in range(parts - 1)]
        return [min(round(f * depth / 256) * 256, depth) for f in ends]

    def attention(n, i, k, blocks):
        h = jnp.where(lax.rem(k, 3) == 2, 2 * lax.div(k, 3), 2 * lax.div(k, 3) - 1)
        here = pl.ds(pl.multiple_of(i * ch, ch), ch)
        wide, last = WIDE * ch, blocks - 1
        state = {}

        def scores(j):
            at = slice((last - j) * wide, (last - j + 1) * wide)
            s = _dot(keys[h, at, :], state["q"], 1, 1)
            if j == 0:
                gap = lax.broadcasted_iota(jnp.int32, (wide, ch), 1) - lax.broadcasted_iota(jnp.int32, (wide, ch), 0)
                s = jnp.where(gap >= last * wide - i * ch, s, HIDDEN)
            state["s", j], state["v", j] = s, vals[h, :, at]

        def lead():
            z = zbuf[lax.rem(k + 1, 2)]
            state["q"] = turned(z[:, :HEAD])
            keys[h, here, :] = turned(z[:, HEAD:])
            scores(0)

        def block(j):
            if j + 1 < blocks:
                scores(j + 1)
            s = state.pop(("s", j))
            top = s.max(axis=0, keepdims=True)
            if j:
                top = jnp.maximum(state["top"], top)
            weights = jnp.exp2((s - top) * e).astype(BF16)
            mix = _dot(state.pop(("v", j)), weights, 1, 0)
            if j:
                mix = state["mix"] * jnp.exp2((state["top"] - top) * e) + mix
            state["top"], state["mix"] = top, mix
            if j == last:
                out = mix[:HEAD] * (1 / mix[HEAD : HEAD + 1])
                seen[:, pl.ds(pl.multiple_of(h * HEAD, HEAD), HEAD)] = out.T.astype(BF16)

        product(n, k, cut(blocks + 1), [lead, *(functools.partial(block, j) for j in range(blocks))])

    def values(n, i, k):
        def post():
            z, here = zbuf[lax.rem(k + 1, 2)], pl.ds(pl.multiple_of(i * ch, ch), ch)
            for m in (1, 0):
                h = jnp.minimum(2 * lax.div(k, 3) + m, heads - 1)
                vals[h, :HEAD, here] = z[:, m * HEAD : (m + 1) * HEAD].astype(BF16).T

        product(n, k, [0, depth], [post])

    def compute(i, k):
        n = i * units + k
        follows = (k > 1) & (lax.rem(k, 3) != 1)

        @pl.when(k < units)
        def _():
            @pl.when((n + AHEAD < nc * units) & ((n + AHEAD < units) | (n >= units)))
            def _():
                for_unit(n + AHEAD, start)

            @pl.when(n == units - AHEAD)
            def _():
                for m in range(2 * tiles):
                    wo_copy(m).start()

            for_unit(n, lambda copy: copy.wait())

            @pl.when(k == 0)
            def _():
                product(n, k, [0, depth], [lambda: None])

            @pl.when(lax.rem(k, 3) == 1)
            def _():
                values(n, i, k)

            for blocks in range(1, pl.cdiv(nc, WIDE) + 1):
                pl.when(follows & (lax.div(i, WIDE) == blocks - 1))(functools.partial(attention, n, i, k, blocks))

        for blocks in range(1, pl.cdiv(nc, WIDE) + 1):
            pl.when((k == units) & (lax.div(i, WIDE) == blocks - 1))(functools.partial(attention, None, i, k, blocks))

        @pl.when(k == units + 1)
        def _():
            @pl.when(i > 0)
            def _():
                for j in range(batch):
                    d2d_copy(i - 1, j).wait_send()

            def theirs(n, _):
                at = pl.multiple_of(n * tile, tile)
                pl.when(i == 0)(lambda: wo_copy(n).wait())
                part = _dot(seen[...], wo[:, pl.ds(pl.multiple_of(other + at, 128), tile)], 1, 0)
                stage[:, :, pl.ds(at, tile)] = part.astype(BF16).reshape(batch, sub, tile)

            lax.fori_loop(0, half // tile, theirs, None)
            for j in range(batch):
                d2d_copy(i, j).start()

        @pl.when(k == units + 2)
        def _():
            def ours(n, _):
                at = pl.multiple_of(n * tile, tile)
                pl.when(i == 0)(lambda: wo_copy(tiles + n).wait())
                part = _dot(seen[...], wo[:, pl.ds(pl.multiple_of(mine + at, 128), tile)], 1, 0)
                acc[lax.rem(i, 2), :, :, pl.ds(at, tile)] = part.reshape(batch, sub, tile)

            lax.fori_loop(0, half // tile, ours, None)

            @pl.when(i == 0)
            def _():
                for r in range(ch // GROUP):
                    x_copy(1, r).start()
                for n in range(units, units + AHEAD):
                    for_unit(n, start)

        @pl.when((k == units + 3) & (i + 1 < nc))
        def _():
            norm(i + 1)

            @pl.when(i + 2 < nc)
            def _():
                for r in range(ch // GROUP):
                    x_copy(i + 2, r).start()

    def valid(s):
        return (s >= 0) & (s < pieces)

    def sum_of(s):
        return acc.at[lax.rem(lax.div(s, batch), 2), lax.rem(s, batch)]

    def pair(s):
        at, ours = lax.rem(s, 2 * batch), sum_of(s)
        d2d_copy(lax.div(s, batch), lax.rem(s, batch)).wait_recv()

        @pl.when(inner)
        def _():
            ours[...] = ours[...] + d2d[at].astype(F32)

        @pl.when(jnp.logical_not(inner))
        def _():
            @pl.when(s >= nb)
            def _():
                up_copy(s - nb).wait_send()

            sendb[lax.rem(s, nb)] = (ours[...] + d2d[at].astype(F32)).astype(BF16)
            up_copy(s).start()

    def relay(s):
        up_copy(s).wait_recv()

        @pl.when(s >= nb)
        def _():
            cross_copy(s - nb).wait_send()

        sendb[lax.rem(s, nb)] = (sum_of(s)[...] + up[lax.rem(s, ring)].astype(F32)).astype(BF16)
        cross_copy(s).start()

    def sent(s):
        out_copies(s, lambda copy: copy.wait_send())
        pl.when(s < split)(lambda: local_copy(s).wait())

    def finish(s):
        b = lax.rem(s, nb)
        cross_copy(s).wait_recv()
        xres_copy(s).wait()

        @pl.when(s >= nb)
        def _():
            sent(s - nb)

        total = sendb[b].astype(F32) + cross[lax.rem(s, cring)].astype(F32)
        y = (xres[lax.rem(s, nx)].astype(F32) + total).astype(BF16)

        @pl.when(s < split)
        def _():
            resb[b] = y
            local_copy(s).start()

        @pl.when(s >= split)
        def _():
            y_ref[rows(s), pl.ds(mine, half)] = y

        out_copies(s, start)

    def arrived(s):
        b = lax.rem(s, ring)
        finished(s, lambda at, _: remote(at, at, part_send.at[0], res_recv.at[b], away).wait_recv())
        onward_copy(s, start)

    for r in range(ch // GROUP):
        x_copy(0, r).start()
    for n in range(AHEAD):
        for_unit(n, start)
    barrier = pltpu.get_barrier_semaphore()
    pl.semaphore_signal(barrier, inc=1, device_id=partner, device_id_type=MESH)

    @pl.when(z < zs - 1)
    def _():
        pl.semaphore_signal(barrier, inc=1, device_id=above, device_id_type=MESH)

    @pl.when(z > 0)
    def _():
        pl.semaphore_signal(barrier, inc=1, device_id=below, device_id_type=MESH)

    def clear(h, _):
        keys[h] = jnp.zeros(keys.shape[1:], BF16)
        vals[h, :HEAD, :] = jnp.zeros((HEAD, vals.shape[2]), BF16)
        vals[h, HEAD:, :] = jnp.ones((vals.shape[1] - HEAD, vals.shape[2]), BF16)

    lax.fori_loop(0, heads, clear, None)
    for n in range(depth // 128):
        gain[:, n * 128 : (n + 1) * 128] = gain_ref[n : n + 1, :].astype(F32)
    norm(0)
    pl.semaphore_wait(barrier, 1 + jnp.where(z < zs - 1, 1, 0) + jnp.where(z > 0, 1, 0))

    def served(g, stage, do):
        s = g - lag1 - LAGS[stage]
        pl.when(valid(s))(functools.partial(do, s))

    def serve(g):
        pl.when(jnp.logical_not(inner))(lambda: served(g, 3, arrived))

        @pl.when(inner)
        def _():
            served(g, 2, finish)
            served(g + 2, 2, lambda s: xres_copy(s).start())

        served(g, 0, pair)

    homes = [
        pltpu.make_async_copy(early.at[pl.ds(r * GROUP, GROUP), :], y_ref.at[pl.ds(r * GROUP, GROUP), :], home_sem.at[r])
        for r in range(early.shape[0] // GROUP)
    ]

    def theirs_arrived(which, y):
        at = y.at[:, pl.ds(other, half)]
        remote(at, at, part_send.at[which], part_recv.at[which], partner).wait_recv()

    def slot(g, _):
        i, k = lax.div(g, per), lax.rem(g, per)
        pl.when(lax.rem(g, 2) == 0)(lambda: serve(lax.div(g, 2)))
        pl.when((lax.rem(g, 2) == 1) & inner)(lambda: served(lax.div(g, 2), 1, relay))
        pl.when(i < nc)(lambda: compute(i, k))

        @pl.when(g == max(nc * per, 2 * (split + last_lag)))
        def _():
            theirs_arrived(0, early)
            for copy in homes:
                copy.start()

    lax.fori_loop(0, 2 * (pieces + last_lag), slot, None)

    for j in range(batch):
        d2d_copy(nc - 1, j).wait_send()
    for s in range(pieces - nb, pieces):
        up_copy(s).wait_send()

    @pl.when(inner)
    def _():
        for s in range(pieces - nb, pieces):
            sent(s)

    rest = y_ref.at[early.shape[0] :, :]
    theirs_arrived(1, rest)
    for which, y in enumerate((early, rest)):
        ours = y.at[:, pl.ds(mine, half)]
        pl.when(jnp.logical_not(inner))(remote(ours, ours, part_send.at[which], part_recv.at[which], partner).wait_send)
    for copy in homes:
        copy.wait()


def _placed(y_in, y_out, sem):
    size = y_in.shape[0] // sem.shape[0]
    copies = [pltpu.make_async_copy(y_in.at[pl.ds(r, size), :], y_out.at[pl.ds(r, size), :], sem.at[r // size]) for r in range(0, y_in.shape[0], size)]
    for copy in copies:
        copy.start()
    for copy in copies:
        copy.wait()


def _tables(nc, ch):
    rate = THETA ** (-np.arange(HEAD // 2) / (HEAD // 2))
    sign = np.repeat([-1.0, 1.0], HEAD // 2)

    def both(place):
        angle = np.tile(place[:, None] * rate, (1, 2))
        return np.stack([np.cos(angle), np.sin(angle) * sign]).astype(np.float32)

    return both(np.arange(nc) * ch), both(np.arange(ch))


def solution(mesh, ch=128, tile=1792, copy_rows=128):
    names = mesh.axis_names
    zs = mesh.shape["tp"] // 2

    def step(x, gain, wq, wk, wv, wo):
        n, d = x.shape
        heads = wq.shape[1] // HEAD
        nc, half = n // ch, d // 2
        per = 3 * (heads // 2) + 7
        sub = 2 * ch // per
        base, fine = _tables(nc, ch)
        cfg = dict(ch=ch, sub=sub, per=per, heads=heads, nc=nc, half=half, zs=zs, tile=min(tile, half), names=names)
        wide, batch = min(tile, half), per // 2
        nb, ring, cring, nx = 4, 10, 6, 3
        dma = pltpu.SemaphoreType.DMA
        hbm, vmem = pl.BlockSpec(memory_space=pl.ANY), pl.BlockSpec(memory_space=pltpu.VMEM)
        _, y = pl.pallas_call(
            functools.partial(_kernel, cfg),
            out_shape=[jax.ShapeDtypeStruct((heads * HEAD, d), BF16), pltpu.VMEM((n, d), BF16)],
            in_specs=[hbm, vmem, vmem, vmem, hbm, hbm, hbm, hbm],
            out_specs=[hbm, vmem],
            scratch_shapes=[
                pltpu.VMEM((heads, n, HEAD), BF16),
                pltpu.VMEM((heads, HEAD + 8, n), BF16),
                pltpu.VMEM((AHEAD + 1, d, 2 * HEAD), BF16),
                pltpu.VMEM((2, ch, 2 * HEAD), F32),
                pltpu.VMEM((ch, d), BF16),
                pltpu.VMEM((2, batch, sub, half), F32),
                pltpu.VMEM((batch, sub, half), BF16),
                pltpu.VMEM((ch, heads * HEAD), BF16),
                pltpu.VMEM((2 * batch, sub, half), BF16),
                pltpu.VMEM((ring, sub, half), BF16),
                pltpu.VMEM((cring, sub, half), BF16),
                pltpu.VMEM((nb, sub, half), BF16),
                pltpu.VMEM((nb, sub, half), BF16),
                pltpu.VMEM((nx, sub, half), BF16),
                pltpu.VMEM((ch, HEAD), F32),
                pltpu.VMEM((ch, HEAD), F32),
                pltpu.VMEM((1, d), F32),
                dma((AHEAD + 1, 2)), dma((2 * half // wide,)), dma((ch // GROUP,)), dma((nx,)),
                dma((batch,)), dma((2 * batch,)), dma((ring,)), dma((cring,)), dma((ring,)),
                dma((nb,)), dma((nb,)), dma((nb,)), dma((nb,)), dma((2,)), dma((2,)),
                dma((heads * HEAD // GROUP,)),
            ],
            compiler_params=pltpu.CompilerParams(collective_id=0, has_side_effects=True, vmem_limit_bytes=KERNEL_VMEM),
            name="attention_half",
        )(x, gain.reshape(d // 128, 128), jnp.asarray(base), jnp.asarray(fine), wq, wk, wv, wo)
        return pl.pallas_call(
            _placed,
            out_shape=jax.ShapeDtypeStruct((n, d), BF16),
            in_specs=[vmem],
            out_specs=hbm,
            scratch_shapes=[dma((n // copy_rows,))],
            compiler_params=pltpu.CompilerParams(vmem_limit_bytes=2**20),
            name="placed",
        )(pltpu.with_memory_space_constraint(y, pltpu.VMEM))

    tokens, columns = P("dp", None), P(None, "tp")
    return jax.shard_map(
        step,
        mesh=mesh,
        in_specs=(tokens, P(None), columns, columns, columns, P("tp", None)),
        out_specs=tokens,
        check_vma=False,
    )
```

```python
import functools

import jax
import jax.numpy as jnp
import numpy as np
from jax import lax
from jax.experimental import pallas as pl
from jax.experimental.pallas import tpu as pltpu
from jax.sharding import PartitionSpec as P

HEAD = 128
THETA = 10000
LOG2E = 1.4426950408889634
HIDDEN = -2e30
MESH = pl.DeviceIdType.MESH
BF16, F32 = jnp.bfloat16, jnp.float32
LAGS = (0, 2, 5, 9)
GROUP = 64
KERNEL_VMEM = 37_600_000
WIDE = 4
AHEAD = 3


def _dot(a, b, ca, cb):
    return lax.dot_general(a, b, (((ca,), (cb,)), ((), ())), preferred_element_type=F32)


def _kernel(cfg, x_hbm, gain_ref, base_ref, fine_ref, wq_hbm, wk_hbm, wv_hbm, wo_hbm, early, y_ref,
            keys, vals, wbuf, zbuf, abuf, acc, stage, seen, d2d, up, cross, sendb, resb, xres, rotc, rots, gain,
            w_sem, wo_sem, x_sem, xres_sem, d2d_send, d2d_recv, up_recv, cross_recv, res_recv,
            send_a, send_b, send_c, send_l, part_send, part_recv, home_sem):
    ch, sub, per, heads, nc, half, zs, tile, names = (cfg[k] for k in ("ch", "sub", "per", "heads", "nc", "half", "zs", "tile", "names"))
    depth = 2 * half
    units = 3 * (heads // 2) + 2
    batch = per // 2
    pieces = nc * batch
    e = HEAD**-0.5 * LOG2E
    lag1 = (units + 4) // 2
    last_lag = lag1 + LAGS[3]
    ring, cring, nb, nx = up.shape[0], cross.shape[0], sendb.shape[0], xres.shape[0]
    wo, split = y_ref.at[: early.shape[0], :], early.shape[0] // sub
    xbuf = y_ref.at[(nc - 1) * ch :, :]

    dpi, t = lax.axis_index(names[0]), lax.axis_index(names[1])
    core, z = lax.rem(t, 2), lax.div(t, 2)
    inner = (z > 0) & (z < zs - 1)
    partner, above, below = (dpi, t + 1 - 2 * core), (dpi, t + 2), (dpi, t - 2)
    toward = (dpi, jnp.where(z < zs // 2, t + 2, t - 2))
    away = (dpi, jnp.where(z < zs // 2, t - 2, t + 2))
    mine = pl.multiple_of(core * half, 128)
    other = pl.multiple_of((1 - core) * half, 128)

    def rows(s):
        return pl.ds(pl.multiple_of(s * sub, sub), sub)

    def finished(s, act):
        cols = pl.ds(mine, half)
        pl.when(s < split)(lambda: act(early.at[rows(s), cols], 0))
        pl.when(s >= split)(lambda: act(y_ref.at[rows(s), cols], 1))

    def remote(src, dst, send, recv, device):
        return pltpu.make_async_remote_copy(src_ref=src, dst_ref=dst, send_sem=send, recv_sem=recv, device_id=device, device_id_type=MESH)

    def x_copy(i, r):
        at = pl.ds(r * GROUP, GROUP)
        return pltpu.make_async_copy(x_hbm.at[pl.ds(pl.multiple_of(i * ch + r * GROUP, GROUP), GROUP), :], xbuf.at[at, :], x_sem.at[r])

    def for_unit(n, act):
        k, at = lax.rem(n, units), lax.rem(n, AHEAD + 1)
        group, kind = lax.div(k, 3), lax.rem(k, 3)

        def columns(w, h, wide):
            return w.at[:, pl.ds(pl.multiple_of(h * HEAD, HEAD), wide * HEAD)]

        @pl.when((kind == 0) & (2 * group + 1 < heads))
        def _():
            act(pltpu.make_async_copy(columns(wv_hbm, 2 * group, 2), wbuf.at[at], w_sem.at[at, 0]))

        @pl.when((kind == 0) & (2 * group + 1 == heads))
        def _():
            act(pltpu.make_async_copy(columns(wv_hbm, 2 * group, 1), wbuf.at[at, :, :HEAD], w_sem.at[at, 0]))

        @pl.when(kind > 0)
        def _():
            h = 2 * group + kind - 1
            act(pltpu.make_async_copy(columns(wq_hbm, h, 1), wbuf.at[at, :, :HEAD], w_sem.at[at, 0]))
            act(pltpu.make_async_copy(columns(wk_hbm, h, 1), wbuf.at[at, :, HEAD:], w_sem.at[at, 1]))

    tiles = half // tile

    def wo_copy(m):
        at = jnp.where(m < tiles, other + m * tile, mine + (m - tiles) * tile)
        part = pl.ds(pl.multiple_of(at, 128), tile)
        return pltpu.make_async_copy(wo_hbm.at[:, part], wo.at[:, part], wo_sem.at[m])

    def xres_copy(s):
        b = lax.rem(s, nx)
        return pltpu.make_async_copy(x_hbm.at[rows(s), pl.ds(mine, half)], xres.at[b], xres_sem.at[b])

    def d2d_copy(c, k):
        at = lax.rem(c, 2) * batch + k
        return remote(stage.at[k], d2d.at[at], d2d_send.at[k], d2d_recv.at[at], partner)

    def up_copy(s):
        b, r = lax.rem(s, nb), lax.rem(s, ring)
        return remote(sendb.at[b], up.at[r], send_a.at[b], up_recv.at[r], toward)

    def cross_copy(s):
        b, r = lax.rem(s, nb), lax.rem(s, cring)
        return remote(sendb.at[b], cross.at[r], send_a.at[b], cross_recv.at[r], toward)

    def out_copies(s, act):
        b = lax.rem(s, nb)

        def both(at, which):
            src = at if which else resb.at[b]
            act(remote(src, at, send_b.at[b], res_recv.at[lax.rem(s, ring)], away))
            act(remote(src, at, send_c.at[b], part_recv.at[which], partner))

        finished(s, both)

    def local_copy(s):
        b = lax.rem(s, nb)
        return pltpu.make_async_copy(resb.at[b], early.at[rows(s), pl.ds(mine, half)], send_l.at[b])

    def onward_copy(s, act):
        finished(s, lambda at, which: act(remote(at, at, part_send.at[which], part_recv.at[which], partner)))

    def start(copy):
        copy.start()

    def turn_by(i):
        bc, bs = base_ref[0, pl.ds(i, 1), :], base_ref[1, pl.ds(i, 1), :]
        rotc[...] = bc * fine_ref[0] - bs * fine_ref[1]
        rots[...] = bs * fine_ref[0] + bc * fine_ref[1]

    def norm(r):
        at = pl.ds(pl.multiple_of(r * GROUP, GROUP), GROUP)
        cols = [slice(c, c + 128) for c in range(0, depth, 128)]
        sums = [None] * 4
        for n, c in enumerate(cols):
            wide = xbuf[at, c].astype(F32)
            sums[n % 4] = wide * wide if sums[n % 4] is None else sums[n % 4] + wide * wide
        total = functools.reduce(jnp.add, [s for s in sums if s is not None])
        scale = lax.rsqrt(jnp.sum(total, -1, keepdims=True) * (1 / depth) + 1e-6)
        scale = jnp.broadcast_to(scale, (GROUP, 128))
        for c in cols:
            abuf[at, c] = (xbuf[at, c].astype(F32) * scale * gain[:, c]).astype(BF16)

    def turned(v):
        v = v.astype(BF16).astype(F32)
        return (v * rotc[...] + pltpu.roll(v, HEAD // 2, 1) * rots[...]).astype(BF16)

    def product(n, k, cuts, between):
        if n is None:
            for do in between:
                do()
            return
        at, total = lax.rem(n, AHEAD + 1), None
        for lo, hi, do in zip(cuts, cuts[1:], between):
            if lo < hi:
                part = _dot(abuf[:, lo:hi], wbuf[at, lo:hi, :], 1, 0)
                total = part if total is None else total + part
            do()
        zbuf[lax.rem(k, 2)] = total

    def cut(parts):
        lead = 1 / 7 if parts > 1 else 1
        ends = [0, lead] + [lead + (1 - lead) * (j + 1) / max(parts - 1, 1) for j in range(parts - 1)]
        return [min(round(f * depth / 256) * 256, depth) for f in ends]

    def attention(n, i, k, blocks):
        h = jnp.where(lax.rem(k, 3) == 2, 2 * lax.div(k, 3), 2 * lax.div(k, 3) - 1)
        here = pl.ds(pl.multiple_of(i * ch, ch), ch)
        wide, last = WIDE * ch, blocks - 1
        state = {}

        def scores(j):
            at = slice((last - j) * wide, (last - j + 1) * wide)
            s = _dot(keys[h, at, :], state["q"], 1, 1)
            if j == 0:
                gap = lax.broadcasted_iota(jnp.int32, (wide, ch), 1) - lax.broadcasted_iota(jnp.int32, (wide, ch), 0)
                s = jnp.where(gap >= last * wide - i * ch, s, HIDDEN)
            state["s", j], state["v", j] = s, vals[h, :, at]

        def lead():
            z = zbuf[lax.rem(k + 1, 2)]
            state["q"] = turned(z[:, :HEAD])
            keys[h, here, :] = turned(z[:, HEAD:])
            scores(0)

        def block(j):
            if j + 1 < blocks:
                scores(j + 1)
            s = state.pop(("s", j))
            top = s.max(axis=0, keepdims=True)
            if j:
                top = jnp.maximum(state["top"], top)
            weights = jnp.exp2((s - top) * e).astype(BF16)
            mix = _dot(state.pop(("v", j)), weights, 1, 0)
            if j:
                mix = state["mix"] * jnp.exp2((state["top"] - top) * e) + mix
            state["top"], state["mix"] = top, mix
            if j == last:
                out = mix[:HEAD] * (1 / mix[HEAD : HEAD + 1])
                seen[:, pl.ds(pl.multiple_of(h * HEAD, HEAD), HEAD)] = out.T.astype(BF16)

        product(n, k, cut(blocks + 1), [lead, *(functools.partial(block, j) for j in range(blocks))])

    def values(n, i, k):
        def post():
            z, here = zbuf[lax.rem(k + 1, 2)], pl.ds(pl.multiple_of(i * ch, ch), ch)
            for m in (1, 0):
                h = jnp.minimum(2 * lax.div(k, 3) + m, heads - 1)
                vals[h, :HEAD, here] = z[:, m * HEAD : (m + 1) * HEAD].astype(BF16).T

        product(n, k, [0, depth], [post])

    def compute(i, k):
        n = i * units + k
        follows = (k > 1) & (lax.rem(k, 3) != 1)

        @pl.when(k < units)
        def _():
            @pl.when((n + AHEAD < nc * units) & ((n + AHEAD < units) | (n >= units)))
            def _():
                for_unit(n + AHEAD, start)

            @pl.when(n == units - AHEAD)
            def _():
                for m in range(2 * tiles):
                    wo_copy(m).start()

            for_unit(n, lambda copy: copy.wait())

            @pl.when(k == 0)
            def _():
                product(n, k, [0, depth], [lambda: None])

            @pl.when(lax.rem(k, 3) == 1)
            def _():
                values(n, i, k)

            for blocks in range(1, pl.cdiv(nc, WIDE) + 1):
                pl.when(follows & (lax.div(i, WIDE) == blocks - 1))(functools.partial(attention, n, i, k, blocks))

        for blocks in range(1, pl.cdiv(nc, WIDE) + 1):
            pl.when((k == units) & (lax.div(i, WIDE) == blocks - 1))(functools.partial(attention, None, i, k, blocks))

        @pl.when(k == units + 1)
        def _():
            @pl.when(i > 0)
            def _():
                for j in range(batch):
                    d2d_copy(i - 1, j).wait_send()

            @pl.when(i + 1 < nc)
            def _():
                for r in range(ch // GROUP):
                    x_copy(i + 1, r).wait()
                turn_by(i + 1)

            def theirs(n, wide):
                at = n * wide if isinstance(n, int) else pl.multiple_of(n * wide, wide)
                part = _dot(seen[...], wo[:, pl.ds(pl.multiple_of(other + at, 128), wide)], 1, 0)
                stage[:, :, pl.ds(at, wide)] = part.astype(BF16).reshape(batch, sub, wide)

            @pl.when(i == 0)
            def _():
                def first(n, _):
                    wo_copy(n).wait()
                    theirs(n, tile)
                    norm(n)

                lax.fori_loop(0, tiles, first, None)

            @pl.when(i > 0)
            def _():
                theirs(0, half)
                for r in range(ch // GROUP):
                    norm(r)

            for j in range(batch):
                d2d_copy(i, j).start()

        @pl.when(k == units + 2)
        def _():
            def ours(n, wide):
                at = n * wide if isinstance(n, int) else pl.multiple_of(n * wide, wide)
                part = _dot(seen[...], wo[:, pl.ds(pl.multiple_of(mine + at, 128), wide)], 1, 0)
                acc[lax.rem(i, 2), :, :, pl.ds(at, wide)] = part.reshape(batch, sub, wide)

            @pl.when(i == 0)
            def _():
                def first(n, _):
                    wo_copy(tiles + n).wait()
                    ours(n, tile)

                lax.fori_loop(0, tiles, first, None)

            pl.when(i > 0)(lambda: ours(0, half))

            @pl.when(i == 0)
            def _():
                for n in range(units, units + AHEAD):
                    for_unit(n, start)

        @pl.when((k == units + 3) & (i + 2 < nc))
        def _():
            for r in range(ch // GROUP):
                x_copy(i + 2, r).start()

    def valid(s):
        return (s >= 0) & (s < pieces)

    def sum_of(s):
        return acc.at[lax.rem(lax.div(s, batch), 2), lax.rem(s, batch)]

    def pair(s):
        at, ours = lax.rem(s, 2 * batch), sum_of(s)
        d2d_copy(lax.div(s, batch), lax.rem(s, batch)).wait_recv()

        @pl.when(inner)
        def _():
            ours[...] = ours[...] + d2d[at].astype(F32)

        @pl.when(jnp.logical_not(inner))
        def _():
            @pl.when(s >= nb)
            def _():
                up_copy(s - nb).wait_send()

            sendb[lax.rem(s, nb)] = (ours[...] + d2d[at].astype(F32)).astype(BF16)
            up_copy(s).start()

    def relay(s):
        up_copy(s).wait_recv()

        @pl.when(s >= nb)
        def _():
            cross_copy(s - nb).wait_send()

        sendb[lax.rem(s, nb)] = (sum_of(s)[...] + up[lax.rem(s, ring)].astype(F32)).astype(BF16)
        cross_copy(s).start()

    def sent(s):
        out_copies(s, lambda copy: copy.wait_send())
        pl.when(s < split)(lambda: local_copy(s).wait())

    def finish(s):
        b = lax.rem(s, nb)
        cross_copy(s).wait_recv()
        xres_copy(s).wait()

        @pl.when(s >= nb)
        def _():
            sent(s - nb)

        total = sendb[b].astype(F32) + cross[lax.rem(s, cring)].astype(F32)
        y = (xres[lax.rem(s, nx)].astype(F32) + total).astype(BF16)

        @pl.when(s < split)
        def _():
            resb[b] = y
            local_copy(s).start()

        @pl.when(s >= split)
        def _():
            y_ref[rows(s), pl.ds(mine, half)] = y

        out_copies(s, start)

    def arrived(s):
        b = lax.rem(s, ring)
        finished(s, lambda at, _: remote(at, at, part_send.at[0], res_recv.at[b], away).wait_recv())
        onward_copy(s, start)

    for r in range(ch // GROUP):
        x_copy(0, r).start()
    for n in range(AHEAD):
        for_unit(n, start)
    barrier = pltpu.get_barrier_semaphore()
    pl.semaphore_signal(barrier, inc=1, device_id=partner, device_id_type=MESH)

    @pl.when(z < zs - 1)
    def _():
        pl.semaphore_signal(barrier, inc=1, device_id=above, device_id_type=MESH)

    @pl.when(z > 0)
    def _():
        pl.semaphore_signal(barrier, inc=1, device_id=below, device_id_type=MESH)

    def clear(h, _):
        keys[h] = jnp.zeros(keys.shape[1:], BF16)
        vals[h, :HEAD, :] = jnp.zeros((HEAD, vals.shape[2]), BF16)
        vals[h, HEAD:, :] = jnp.ones((vals.shape[1] - HEAD, vals.shape[2]), BF16)

    lax.fori_loop(0, heads, clear, None)
    for n in range(depth // 128):
        gain[:, n * 128 : (n + 1) * 128] = gain_ref[n : n + 1, :].astype(F32)
    turn_by(0)
    for r in range(ch // GROUP):
        x_copy(0, r).wait()
        norm(r)
    for r in range(ch // GROUP):
        x_copy(1, r).start()
    pl.semaphore_wait(barrier, 1 + jnp.where(z < zs - 1, 1, 0) + jnp.where(z > 0, 1, 0))

    def served(g, stage, do):
        s = g - lag1 - LAGS[stage]
        pl.when(valid(s))(functools.partial(do, s))

    def serve(g):
        pl.when(jnp.logical_not(inner))(lambda: served(g, 3, arrived))

        @pl.when(inner)
        def _():
            served(g, 2, finish)
            served(g + 2, 2, lambda s: xres_copy(s).start())

        served(g, 0, pair)

    homes = [
        pltpu.make_async_copy(early.at[pl.ds(r * GROUP, GROUP), :], y_ref.at[pl.ds(r * GROUP, GROUP), :], home_sem.at[r])
        for r in range(early.shape[0] // GROUP)
    ]

    def theirs_arrived(which, y):
        at = y.at[:, pl.ds(other, half)]
        remote(at, at, part_send.at[which], part_recv.at[which], partner).wait_recv()

    def slot(g, _):
        i, k = lax.div(g, per), lax.rem(g, per)
        pl.when(lax.rem(g, 2) == 0)(lambda: serve(lax.div(g, 2)))
        pl.when((lax.rem(g, 2) == 1) & inner)(lambda: served(lax.div(g, 2), 1, relay))
        pl.when(i < nc)(lambda: compute(i, k))

        @pl.when(g == max(nc * per, 2 * (split + last_lag)))
        def _():
            theirs_arrived(0, early)
            for copy in homes:
                copy.start()

    lax.fori_loop(0, 2 * (pieces + last_lag), slot, None)

    for j in range(batch):
        d2d_copy(nc - 1, j).wait_send()
    for s in range(pieces - nb, pieces):
        up_copy(s).wait_send()

    @pl.when(inner)
    def _():
        for s in range(pieces - nb, pieces):
            sent(s)

    rest = y_ref.at[early.shape[0] :, :]
    theirs_arrived(1, rest)
    for which, y in enumerate((early, rest)):
        ours = y.at[:, pl.ds(mine, half)]
        pl.when(jnp.logical_not(inner))(remote(ours, ours, part_send.at[which], part_recv.at[which], partner).wait_send)
    for copy in homes:
        copy.wait()


def _placed(y_in, y_out, sem):
    size = y_in.shape[0] // sem.shape[0]
    copies = [pltpu.make_async_copy(y_in.at[pl.ds(r, size), :], y_out.at[pl.ds(r, size), :], sem.at[r // size]) for r in range(0, y_in.shape[0], size)]
    for copy in copies:
        copy.start()
    for copy in copies:
        copy.wait()


def _tables(nc, ch):
    rate = THETA ** (-np.arange(HEAD // 2) / (HEAD // 2))
    sign = np.repeat([-1.0, 1.0], HEAD // 2)

    def both(place):
        angle = np.tile(place[:, None] * rate, (1, 2))
        return np.stack([np.cos(angle), np.sin(angle) * sign]).astype(np.float32)

    return both(np.arange(nc) * ch), both(np.arange(ch))


def solution(mesh, ch=128, tile=1792, copy_rows=128):
    names = mesh.axis_names
    zs = mesh.shape["tp"] // 2

    def step(x, gain, wq, wk, wv, wo):
        n, d = x.shape
        heads = wq.shape[1] // HEAD
        nc, half = n // ch, d // 2
        per = 3 * (heads // 2) + 7
        sub = 2 * ch // per
        base, fine = _tables(nc, ch)
        cfg = dict(ch=ch, sub=sub, per=per, heads=heads, nc=nc, half=half, zs=zs, tile=min(tile, half), names=names)
        wide, batch = min(tile, half), per // 2
        nb, ring, cring, nx = 4, 10, 6, 3
        dma = pltpu.SemaphoreType.DMA
        hbm, vmem = pl.BlockSpec(memory_space=pl.ANY), pl.BlockSpec(memory_space=pltpu.VMEM)
        _, y = pl.pallas_call(
            functools.partial(_kernel, cfg),
            out_shape=[jax.ShapeDtypeStruct((heads * HEAD, d), BF16), pltpu.VMEM((n, d), BF16)],
            in_specs=[hbm, vmem, vmem, vmem, hbm, hbm, hbm, hbm],
            out_specs=[hbm, vmem],
            scratch_shapes=[
                pltpu.VMEM((heads, n, HEAD), BF16),
                pltpu.VMEM((heads, HEAD + 8, n), BF16),
                pltpu.VMEM((AHEAD + 1, d, 2 * HEAD), BF16),
                pltpu.VMEM((2, ch, 2 * HEAD), F32),
                pltpu.VMEM((ch, d), BF16),
                pltpu.VMEM((2, batch, sub, half), F32),
                pltpu.VMEM((batch, sub, half), BF16),
                pltpu.VMEM((ch, heads * HEAD), BF16),
                pltpu.VMEM((2 * batch, sub, half), BF16),
                pltpu.VMEM((ring, sub, half), BF16),
                pltpu.VMEM((cring, sub, half), BF16),
                pltpu.VMEM((nb, sub, half), BF16),
                pltpu.VMEM((nb, sub, half), BF16),
                pltpu.VMEM((nx, sub, half), BF16),
                pltpu.VMEM((ch, HEAD), F32),
                pltpu.VMEM((ch, HEAD), F32),
                pltpu.VMEM((1, d), F32),
                dma((AHEAD + 1, 2)), dma((2 * half // wide,)), dma((ch // GROUP,)), dma((nx,)),
                dma((batch,)), dma((2 * batch,)), dma((ring,)), dma((cring,)), dma((ring,)),
                dma((nb,)), dma((nb,)), dma((nb,)), dma((nb,)), dma((2,)), dma((2,)),
                dma((heads * HEAD // GROUP,)),
            ],
            compiler_params=pltpu.CompilerParams(collective_id=0, has_side_effects=True, vmem_limit_bytes=KERNEL_VMEM),
            name="attention_half",
        )(x, gain.reshape(d // 128, 128), jnp.asarray(base), jnp.asarray(fine), wq, wk, wv, wo)
        return pl.pallas_call(
            _placed,
            out_shape=jax.ShapeDtypeStruct((n, d), BF16),
            in_specs=[vmem],
            out_specs=hbm,
            scratch_shapes=[dma((n // copy_rows,))],
            compiler_params=pltpu.CompilerParams(vmem_limit_bytes=2**20),
            name="placed",
        )(pltpu.with_memory_space_constraint(y, pltpu.VMEM))

    tokens, columns = P("dp", None), P(None, "tp")
    return jax.shard_map(
        step,
        mesh=mesh,
        in_specs=(tokens, P(None), columns, columns, columns, P("tp", None)),
        out_specs=tokens,
        check_vma=False,
    )
```

```python
import functools

import jax
import jax.numpy as jnp
import numpy as np
from jax import lax
from jax.experimental import pallas as pl
from jax.experimental.pallas import tpu as pltpu
from jax.sharding import PartitionSpec as P

HEAD = 128
THETA = 10000
LOG2E = 1.4426950408889634
HIDDEN = -2e30
MESH = pl.DeviceIdType.MESH
BF16, F32 = jnp.bfloat16, jnp.float32
LAGS = (0, 3, 6, 12)
GROUP = 64
KERNEL_VMEM = 37_600_000
WIDE = 4
AHEAD = 2


def _dot(a, b, ca, cb):
    return lax.dot_general(a, b, (((ca,), (cb,)), ((), ())), preferred_element_type=F32)


def _kernel(cfg, x_hbm, gain_ref, base_ref, fine_ref, wq_hbm, wk_hbm, wv_hbm, wo_hbm, early, y_ref,
            keys, vals, wbuf, zbuf, abuf, acc, stage, seen, d2d, up, cross, sendb, resb, xres, rotc, rots, gain,
            w_sem, wo_sem, x_sem, xres_sem, d2d_send, d2d_recv, up_recv, cross_recv, res_recv,
            send_a, send_b, send_c, send_l, part_send, part_recv, home_sem):
    ch, sub, per, heads, nc, half, zs, tile, names = (cfg[k] for k in ("ch", "sub", "per", "heads", "nc", "half", "zs", "tile", "names"))
    depth = 2 * half
    units = 3 * (heads // 2) + 2
    batch = per // 2
    pieces = nc * batch
    e = HEAD**-0.5 * LOG2E
    lag1 = (units + 4) // 2
    last_lag = lag1 + LAGS[3]
    ring, cring, nb, nx = up.shape[0], cross.shape[0], sendb.shape[0], xres.shape[0]
    wo, split = y_ref.at[: early.shape[0], :], early.shape[0] // sub
    xbuf = y_ref.at[(nc - 1) * ch :, :]

    dpi, t = lax.axis_index(names[0]), lax.axis_index(names[1])
    core, z = lax.rem(t, 2), lax.div(t, 2)
    inner = (z > 0) & (z < zs - 1)
    partner, above, below = (dpi, t + 1 - 2 * core), (dpi, t + 2), (dpi, t - 2)
    toward = (dpi, jnp.where(z < zs // 2, t + 2, t - 2))
    away = (dpi, jnp.where(z < zs // 2, t - 2, t + 2))
    mine = pl.multiple_of(core * half, 128)
    other = pl.multiple_of((1 - core) * half, 128)

    def rows(s):
        return pl.ds(pl.multiple_of(s * sub, sub), sub)

    def finished(s, act):
        cols = pl.ds(mine, half)
        pl.when(s < split)(lambda: act(early.at[rows(s), cols], 0))
        pl.when(s >= split)(lambda: act(y_ref.at[rows(s), cols], 1))

    def remote(src, dst, send, recv, device):
        return pltpu.make_async_remote_copy(src_ref=src, dst_ref=dst, send_sem=send, recv_sem=recv, device_id=device, device_id_type=MESH)

    def x_copy(i, r):
        at = pl.ds(r * GROUP, GROUP)
        return pltpu.make_async_copy(x_hbm.at[pl.ds(pl.multiple_of(i * ch + r * GROUP, GROUP), GROUP), :], xbuf.at[at, :], x_sem.at[r])

    def for_unit(n, act):
        k, at = lax.rem(n, units), lax.rem(n, AHEAD + 1)
        group, kind = lax.div(k, 3), lax.rem(k, 3)

        def columns(w, h, wide):
            return w.at[:, pl.ds(pl.multiple_of(h * HEAD, HEAD), wide * HEAD)]

        @pl.when((kind == 0) & (2 * group + 1 < heads))
        def _():
            act(pltpu.make_async_copy(columns(wv_hbm, 2 * group, 2), wbuf.at[at], w_sem.at[at, 0]))

        @pl.when((kind == 0) & (2 * group + 1 == heads))
        def _():
            act(pltpu.make_async_copy(columns(wv_hbm, 2 * group, 1), wbuf.at[at, :, :HEAD], w_sem.at[at, 0]))

        @pl.when(kind > 0)
        def _():
            h = 2 * group + kind - 1
            act(pltpu.make_async_copy(columns(wq_hbm, h, 1), wbuf.at[at, :, :HEAD], w_sem.at[at, 0]))
            act(pltpu.make_async_copy(columns(wk_hbm, h, 1), wbuf.at[at, :, HEAD:], w_sem.at[at, 1]))

    tiles = half // tile

    def wo_copy(m):
        at = jnp.where(m < tiles, other + m * tile, mine + (m - tiles) * tile)
        part = pl.ds(pl.multiple_of(at, 128), tile)
        return pltpu.make_async_copy(wo_hbm.at[:, part], wo.at[:, part], wo_sem.at[m])

    def xres_copy(s):
        b = lax.rem(s, nx)
        return pltpu.make_async_copy(x_hbm.at[rows(s), pl.ds(mine, half)], xres.at[b], xres_sem.at[b])

    def d2d_copy(c, k):
        at = lax.rem(c, 2) * batch + k
        return remote(stage.at[k], d2d.at[at], d2d_send.at[k], d2d_recv.at[at], partner)

    def up_copy(s):
        b, r = lax.rem(s, nb), lax.rem(s, ring)
        return remote(sendb.at[b], up.at[r], send_a.at[b], up_recv.at[r], toward)

    def cross_copy(s):
        b, r = lax.rem(s, nb), lax.rem(s, cring)
        return remote(sendb.at[b], cross.at[r], send_a.at[b], cross_recv.at[r], toward)

    def out_copies(s, act):
        b = lax.rem(s, nb)

        def both(at, which):
            src = at if which else resb.at[b]
            act(remote(src, at, send_b.at[b], res_recv.at[lax.rem(s, ring)], away))
            act(remote(src, at, send_c.at[b], part_recv.at[which], partner))

        finished(s, both)

    def local_copy(s):
        b = lax.rem(s, nb)
        return pltpu.make_async_copy(resb.at[b], early.at[rows(s), pl.ds(mine, half)], send_l.at[b])

    def onward_copy(s, act):
        finished(s, lambda at, which: act(remote(at, at, part_send.at[which], part_recv.at[which], partner)))

    def start(copy):
        copy.start()

    def turn_by(i):
        bc, bs = base_ref[0, pl.ds(i, 1), :], base_ref[1, pl.ds(i, 1), :]
        rotc[...] = bc * fine_ref[0] - bs * fine_ref[1]
        rots[...] = bs * fine_ref[0] + bc * fine_ref[1]

    def norm(r):
        at = pl.ds(pl.multiple_of(r * GROUP, GROUP), GROUP)
        cols = [slice(c, c + 128) for c in range(0, depth, 128)]
        sums = [None] * 4
        for n, c in enumerate(cols):
            wide = xbuf[at, c].astype(F32)
            sums[n % 4] = wide * wide if sums[n % 4] is None else sums[n % 4] + wide * wide
        total = functools.reduce(jnp.add, [s for s in sums if s is not None])
        scale = lax.rsqrt(jnp.sum(total, -1, keepdims=True) * (1 / depth) + 1e-6)
        scale = jnp.broadcast_to(scale, (GROUP, 128))
        for c in cols:
            abuf[at, c] = (xbuf[at, c].astype(F32) * scale * gain[:, c]).astype(BF16)

    def turned(v):
        v = v.astype(BF16).astype(F32)
        return (v * rotc[...] + pltpu.roll(v, HEAD // 2, 1) * rots[...]).astype(BF16)

    def product(n, k, cuts, between):
        if n is None:
            for do in between:
                do()
            return
        at, total = lax.rem(n, AHEAD + 1), None
        for lo, hi, do in zip(cuts, cuts[1:], between):
            if lo < hi:
                part = _dot(abuf[:, lo:hi], wbuf[at, lo:hi, :], 1, 0)
                total = part if total is None else total + part
            do()
        zbuf[lax.rem(k, 2)] = total

    def cut(parts):
        lead = 1 / 7 if parts > 1 else 1
        ends = [0, lead] + [lead + (1 - lead) * (j + 1) / max(parts - 1, 1) for j in range(parts - 1)]
        return [min(round(f * depth / 256) * 256, depth) for f in ends]

    def attention(n, i, k, blocks):
        h = jnp.where(lax.rem(k, 3) == 2, 2 * lax.div(k, 3), 2 * lax.div(k, 3) - 1)
        here = pl.ds(pl.multiple_of(i * ch, ch), ch)
        wide, last = WIDE * ch, blocks - 1
        state = {}

        def scores(j):
            at = slice((last - j) * wide, (last - j + 1) * wide)
            s = _dot(keys[h, at, :], state["q"], 1, 1)
            if j == 0:
                gap = lax.broadcasted_iota(jnp.int32, (wide, ch), 1) - lax.broadcasted_iota(jnp.int32, (wide, ch), 0)
                s = jnp.where(gap >= last * wide - i * ch, s, HIDDEN)
            state["s", j], state["v", j] = s, vals[h, :, at]

        def lead():
            z = zbuf[lax.rem(k + 1, 2)]
            state["q"] = turned(z[:, :HEAD])
            keys[h, here, :] = turned(z[:, HEAD:])
            scores(0)

        def block(j):
            if j + 1 < blocks:
                scores(j + 1)
            s = state.pop(("s", j))
            top = s.max(axis=0, keepdims=True)
            if j:
                top = jnp.maximum(state["top"], top)
            weights = jnp.exp2((s - top) * e).astype(BF16)
            mix = _dot(state.pop(("v", j)), weights, 1, 0)
            if j:
                mix = state["mix"] * jnp.exp2((state["top"] - top) * e) + mix
            state["top"], state["mix"] = top, mix
            if j == last:
                out = mix[:HEAD] * (1 / mix[HEAD : HEAD + 1])
                seen[:, pl.ds(pl.multiple_of(h * HEAD, HEAD), HEAD)] = out.T.astype(BF16)

        product(n, k, cut(blocks + 1), [lead, *(functools.partial(block, j) for j in range(blocks))])

    def values(n, i, k):
        def post():
            z, here = zbuf[lax.rem(k + 1, 2)], pl.ds(pl.multiple_of(i * ch, ch), ch)
            for m in (1, 0):
                h = jnp.minimum(2 * lax.div(k, 3) + m, heads - 1)
                vals[h, :HEAD, here] = z[:, m * HEAD : (m + 1) * HEAD].astype(BF16).T

        product(n, k, [0, depth], [post])

    def compute(i, k):
        n = i * units + k
        follows = (k > 1) & (lax.rem(k, 3) != 1)

        @pl.when(k < units)
        def _():
            @pl.when((n + AHEAD < nc * units) & ((n + AHEAD < units) | (n >= units)))
            def _():
                for_unit(n + AHEAD, start)

            @pl.when(n == units - AHEAD)
            def _():
                for m in range(2 * tiles):
                    wo_copy(m).start()

            for_unit(n, lambda copy: copy.wait())

            @pl.when(k == 0)
            def _():
                product(n, k, [0, depth], [lambda: None])

            @pl.when(lax.rem(k, 3) == 1)
            def _():
                values(n, i, k)

            for blocks in range(1, pl.cdiv(nc, WIDE) + 1):
                pl.when(follows & (lax.div(i, WIDE) == blocks - 1))(functools.partial(attention, n, i, k, blocks))

        for blocks in range(1, pl.cdiv(nc, WIDE) + 1):
            pl.when((k == units) & (lax.div(i, WIDE) == blocks - 1))(functools.partial(attention, None, i, k, blocks))

        @pl.when(k == units + 1)
        def _():
            @pl.when(i == 0)
            def _():
                for n in range(units, units + AHEAD):
                    for_unit(n, start)

            @pl.when(i > 0)
            def _():
                for j in range(batch):
                    d2d_copy(i - 1, j).wait_send()

            @pl.when(i + 1 < nc)
            def _():
                for r in range(ch // GROUP):
                    x_copy(i + 1, r).wait()
                turn_by(i + 1)

            def theirs(n, wide):
                at = n * wide if isinstance(n, int) else pl.multiple_of(n * wide, wide)
                part = _dot(seen[...], wo[:, pl.ds(pl.multiple_of(other + at, 128), wide)], 1, 0)
                stage[:, :, pl.ds(at, wide)] = part.astype(BF16).reshape(batch, sub, wide)

            @pl.when(i == 0)
            def _():
                def first(n, _):
                    wo_copy(n).wait()
                    theirs(n, tile)
                    norm(n)

                lax.fori_loop(0, tiles, first, None)

            @pl.when(i > 0)
            def _():
                theirs(0, half)
                for r in range(ch // GROUP):
                    norm(r)

            for j in range(batch):
                d2d_copy(i, j).start()

        @pl.when(k == units + 2)
        def _():
            def ours(n, wide):
                at = n * wide if isinstance(n, int) else pl.multiple_of(n * wide, wide)
                part = _dot(seen[...], wo[:, pl.ds(pl.multiple_of(mine + at, 128), wide)], 1, 0)
                acc[lax.rem(i, 2), :, :, pl.ds(at, wide)] = part.reshape(batch, sub, wide)

            @pl.when(i == 0)
            def _():
                def first(n, _):
                    wo_copy(tiles + n).wait()
                    ours(n, tile)

                lax.fori_loop(0, tiles, first, None)

            pl.when(i > 0)(lambda: ours(0, half))


        @pl.when((k == units + 3) & (i + 2 < nc))
        def _():
            for r in range(ch // GROUP):
                x_copy(i + 2, r).start()

    def valid(s):
        return (s >= 0) & (s < pieces)

    def sum_of(s):
        return acc.at[lax.rem(lax.div(s, batch), 2), lax.rem(s, batch)]

    def pair(s):
        at, ours = lax.rem(s, 2 * batch), sum_of(s)
        d2d_copy(lax.div(s, batch), lax.rem(s, batch)).wait_recv()

        @pl.when(inner)
        def _():
            ours[...] = ours[...] + d2d[at].astype(F32)

        @pl.when(jnp.logical_not(inner))
        def _():
            @pl.when(s >= nb)
            def _():
                up_copy(s - nb).wait_send()

            sendb[lax.rem(s, nb)] = (ours[...] + d2d[at].astype(F32)).astype(BF16)
            up_copy(s).start()

    def relay(s):
        up_copy(s).wait_recv()

        @pl.when(s >= nb)
        def _():
            cross_copy(s - nb).wait_send()

        sendb[lax.rem(s, nb)] = (sum_of(s)[...] + up[lax.rem(s, ring)].astype(F32)).astype(BF16)
        cross_copy(s).start()

    def sent(s):
        out_copies(s, lambda copy: copy.wait_send())
        pl.when(s < split)(lambda: local_copy(s).wait())

    def finish(s):
        b = lax.rem(s, nb)
        cross_copy(s).wait_recv()
        xres_copy(s).wait()

        @pl.when(s >= nb)
        def _():
            sent(s - nb)

        total = sendb[b].astype(F32) + cross[lax.rem(s, cring)].astype(F32)
        y = (xres[lax.rem(s, nx)].astype(F32) + total).astype(BF16)

        @pl.when(s < split)
        def _():
            resb[b] = y
            local_copy(s).start()

        @pl.when(s >= split)
        def _():
            y_ref[rows(s), pl.ds(mine, half)] = y

        out_copies(s, start)

    def arrived(s):
        b = lax.rem(s, ring)
        finished(s, lambda at, _: remote(at, at, part_send.at[0], res_recv.at[b], away).wait_recv())
        onward_copy(s, start)

    for r in range(ch // GROUP):
        x_copy(0, r).start()
    for n in range(AHEAD):
        for_unit(n, start)
    barrier = pltpu.get_barrier_semaphore()
    pl.semaphore_signal(barrier, inc=1, device_id=partner, device_id_type=MESH)

    @pl.when(z < zs - 1)
    def _():
        pl.semaphore_signal(barrier, inc=1, device_id=above, device_id_type=MESH)

    @pl.when(z > 0)
    def _():
        pl.semaphore_signal(barrier, inc=1, device_id=below, device_id_type=MESH)

    def clear(h, _):
        keys[h] = jnp.zeros(keys.shape[1:], BF16)
        vals[h, :HEAD, :] = jnp.zeros((HEAD, vals.shape[2]), BF16)
        vals[h, HEAD:, :] = jnp.ones((vals.shape[1] - HEAD, vals.shape[2]), BF16)

    lax.fori_loop(0, heads, clear, None)
    for n in range(depth // 128):
        gain[:, n * 128 : (n + 1) * 128] = gain_ref[n : n + 1, :].astype(F32)
    turn_by(0)
    for r in range(ch // GROUP):
        x_copy(0, r).wait()
        norm(r)
    for r in range(ch // GROUP):
        x_copy(1, r).start()
    pl.semaphore_wait(barrier, 1 + jnp.where(z < zs - 1, 1, 0) + jnp.where(z > 0, 1, 0))

    def served(g, stage, do):
        s = g - lag1 - LAGS[stage]
        pl.when(valid(s))(functools.partial(do, s))

    def serve(g):
        pl.when(jnp.logical_not(inner))(lambda: served(g, 3, arrived))

        @pl.when(inner)
        def _():
            served(g, 2, finish)
            served(g + 2, 2, lambda s: xres_copy(s).start())
            served(g, 1, relay)

        served(g, 0, pair)

    homes = [
        pltpu.make_async_copy(early.at[pl.ds(r * GROUP, GROUP), :], y_ref.at[pl.ds(r * GROUP, GROUP), :], home_sem.at[r])
        for r in range(early.shape[0] // GROUP)
    ]

    def theirs_arrived(which, y):
        at = y.at[:, pl.ds(other, half)]
        remote(at, at, part_send.at[which], part_recv.at[which], partner).wait_recv()

    def slot(g, _):
        i, k = lax.div(g, per), lax.rem(g, per)
        pl.when(lax.rem(g, 2) == 0)(lambda: serve(lax.div(g, 2)))
        pl.when(i < nc)(lambda: compute(i, k))

        @pl.when(g == max(nc * per, 2 * (split + last_lag)))
        def _():
            theirs_arrived(0, early)
            for copy in homes:
                copy.start()

    lax.fori_loop(0, 2 * (pieces + last_lag), slot, None)

    for j in range(batch):
        d2d_copy(nc - 1, j).wait_send()
    for s in range(pieces - nb, pieces):
        up_copy(s).wait_send()

    @pl.when(inner)
    def _():
        for s in range(pieces - nb, pieces):
            sent(s)

    rest = y_ref.at[early.shape[0] :, :]
    theirs_arrived(1, rest)
    for which, y in enumerate((early, rest)):
        ours = y.at[:, pl.ds(mine, half)]
        pl.when(jnp.logical_not(inner))(remote(ours, ours, part_send.at[which], part_recv.at[which], partner).wait_send)
    for copy in homes:
        copy.wait()


def _placed(y_in, y_out, sem):
    size = y_in.shape[0] // sem.shape[0]
    copies = [pltpu.make_async_copy(y_in.at[pl.ds(r, size), :], y_out.at[pl.ds(r, size), :], sem.at[r // size]) for r in range(0, y_in.shape[0], size)]
    for copy in copies:
        copy.start()
    for copy in copies:
        copy.wait()


def _tables(nc, ch):
    rate = THETA ** (-np.arange(HEAD // 2) / (HEAD // 2))
    sign = np.repeat([-1.0, 1.0], HEAD // 2)

    def both(place):
        angle = np.tile(place[:, None] * rate, (1, 2))
        return np.stack([np.cos(angle), np.sin(angle) * sign]).astype(np.float32)

    return both(np.arange(nc) * ch), both(np.arange(ch))


def solution(mesh, ch=128, tile=1792, copy_rows=128):
    names = mesh.axis_names
    zs = mesh.shape["tp"] // 2

    def step(x, gain, wq, wk, wv, wo):
        n, d = x.shape
        heads = wq.shape[1] // HEAD
        nc, half = n // ch, d // 2
        per = 3 * (heads // 2) + 7
        sub = 2 * ch // per
        base, fine = _tables(nc, ch)
        cfg = dict(ch=ch, sub=sub, per=per, heads=heads, nc=nc, half=half, zs=zs, tile=min(tile, half), names=names)
        wide, batch = min(tile, half), per // 2
        nb, ring, cring, nx = 6, 13, 8, 4
        dma = pltpu.SemaphoreType.DMA
        hbm, vmem = pl.BlockSpec(memory_space=pl.ANY), pl.BlockSpec(memory_space=pltpu.VMEM)
        _, y = pl.pallas_call(
            functools.partial(_kernel, cfg),
            out_shape=[jax.ShapeDtypeStruct((heads * HEAD, d), BF16), pltpu.VMEM((n, d), BF16)],
            in_specs=[hbm, vmem, vmem, vmem, hbm, hbm, hbm, hbm],
            out_specs=[hbm, vmem],
            scratch_shapes=[
                pltpu.VMEM((heads, n, HEAD), BF16),
                pltpu.VMEM((heads, HEAD + 8, n), BF16),
                pltpu.VMEM((AHEAD + 1, d, 2 * HEAD), BF16),
                pltpu.VMEM((2, ch, 2 * HEAD), F32),
                pltpu.VMEM((ch, d), BF16),
                pltpu.VMEM((2, batch, sub, half), F32),
                pltpu.VMEM((batch, sub, half), BF16),
                pltpu.VMEM((ch, heads * HEAD), BF16),
                pltpu.VMEM((2 * batch, sub, half), BF16),
                pltpu.VMEM((ring, sub, half), BF16),
                pltpu.VMEM((cring, sub, half), BF16),
                pltpu.VMEM((nb, sub, half), BF16),
                pltpu.VMEM((nb, sub, half), BF16),
                pltpu.VMEM((nx, sub, half), BF16),
                pltpu.VMEM((ch, HEAD), F32),
                pltpu.VMEM((ch, HEAD), F32),
                pltpu.VMEM((1, d), F32),
                dma((AHEAD + 1, 2)), dma((2 * half // wide,)), dma((ch // GROUP,)), dma((nx,)),
                dma((batch,)), dma((2 * batch,)), dma((ring,)), dma((cring,)), dma((ring,)),
                dma((nb,)), dma((nb,)), dma((nb,)), dma((nb,)), dma((2,)), dma((2,)),
                dma((heads * HEAD // GROUP,)),
            ],
            compiler_params=pltpu.CompilerParams(collective_id=0, has_side_effects=True, vmem_limit_bytes=KERNEL_VMEM),
            name="attention_half",
        )(x, gain.reshape(d // 128, 128), jnp.asarray(base), jnp.asarray(fine), wq, wk, wv, wo)
        return pl.pallas_call(
            _placed,
            out_shape=jax.ShapeDtypeStruct((n, d), BF16),
            in_specs=[vmem],
            out_specs=hbm,
            scratch_shapes=[dma((n // copy_rows,))],
            compiler_params=pltpu.CompilerParams(vmem_limit_bytes=2**20),
            name="placed",
        )(pltpu.with_memory_space_constraint(y, pltpu.VMEM))

    tokens, columns = P("dp", None), P(None, "tp")
    return jax.shard_map(
        step,
        mesh=mesh,
        in_specs=(tokens, P(None), columns, columns, columns, P("tp", None)),
        out_specs=tokens,
        check_vma=False,
    )
```

```python
import functools

import jax
import jax.numpy as jnp
import numpy as np
from jax import lax
from jax.experimental import pallas as pl
from jax.experimental.pallas import tpu as pltpu
from jax.sharding import PartitionSpec as P

HEAD = 128
THETA = 10000
LOG2E = 1.4426950408889634
HIDDEN = -2e30
MESH = pl.DeviceIdType.MESH
BF16, F32 = jnp.bfloat16, jnp.float32
LAGS = (0, 2, 5, 9)
GROUP = 64
KERNEL_VMEM = 37_600_000
WIDE = 4
AHEAD = 3


def _dot(a, b, ca, cb):
    return lax.dot_general(a, b, (((ca,), (cb,)), ((), ())), preferred_element_type=F32)


def _kernel(cfg, x_hbm, gain_ref, base_ref, fine_ref, wq_hbm, wk_hbm, wv_hbm, wo_hbm, early, y_ref,
            keys, vals, wbuf, zbuf, abuf, acc, stage, seen, d2d, up, cross, sendb, resb, xres, rotc, rots, gain,
            w_sem, wo_sem, x_sem, xres_sem, d2d_send, d2d_recv, up_recv, cross_recv, res_recv,
            send_a, send_b, send_c, send_l, part_send, part_recv, home_sem):
    ch, sub, per, heads, nc, half, zs, tile, names = (cfg[k] for k in ("ch", "sub", "per", "heads", "nc", "half", "zs", "tile", "names"))
    depth = 2 * half
    units = 3 * (heads // 2) + 2
    batch = per // 2
    pieces = nc * batch
    e = HEAD**-0.5 * LOG2E
    lag1 = (units + 4) // 2
    last_lag = lag1 + LAGS[3]
    ring, cring, nb, nx = up.shape[0], cross.shape[0], sendb.shape[0], xres.shape[0]
    wo, split = y_ref.at[: early.shape[0], :], early.shape[0] // sub
    xbuf = y_ref.at[(nc - 1) * ch :, :]

    dpi, t = lax.axis_index(names[0]), lax.axis_index(names[1])
    core, z = lax.rem(t, 2), lax.div(t, 2)
    inner = (z > 0) & (z < zs - 1)
    partner, above, below = (dpi, t + 1 - 2 * core), (dpi, t + 2), (dpi, t - 2)
    toward = (dpi, jnp.where(z < zs // 2, t + 2, t - 2))
    away = (dpi, jnp.where(z < zs // 2, t - 2, t + 2))
    mine = pl.multiple_of(core * half, 128)
    other = pl.multiple_of((1 - core) * half, 128)

    def rows(s):
        return pl.ds(pl.multiple_of(s * sub, sub), sub)

    def finished(s, act):
        cols = pl.ds(mine, half)
        pl.when(s < split)(lambda: act(early.at[rows(s), cols], 0))
        pl.when(s >= split)(lambda: act(y_ref.at[rows(s), cols], 1))

    def remote(src, dst, send, recv, device):
        return pltpu.make_async_remote_copy(src_ref=src, dst_ref=dst, send_sem=send, recv_sem=recv, device_id=device, device_id_type=MESH)

    def x_copy(i, r):
        at = pl.ds(r * GROUP, GROUP)
        return pltpu.make_async_copy(x_hbm.at[pl.ds(pl.multiple_of(i * ch + r * GROUP, GROUP), GROUP), :], xbuf.at[at, :], x_sem.at[r])

    def for_unit(n, act):
        k, at = lax.rem(n, units), lax.rem(n, AHEAD + 1)
        group, kind = lax.div(k, 3), lax.rem(k, 3)

        def columns(w, h, wide):
            return w.at[:, pl.ds(pl.multiple_of(h * HEAD, HEAD), wide * HEAD)]

        @pl.when((kind == 0) & (2 * group + 1 < heads))
        def _():
            act(pltpu.make_async_copy(columns(wv_hbm, 2 * group, 2), wbuf.at[at], w_sem.at[at, 0]))

        @pl.when((kind == 0) & (2 * group + 1 == heads))
        def _():
            act(pltpu.make_async_copy(columns(wv_hbm, 2 * group, 1), wbuf.at[at, :, :HEAD], w_sem.at[at, 0]))

        @pl.when(kind > 0)
        def _():
            h = 2 * group + kind - 1
            act(pltpu.make_async_copy(columns(wq_hbm, h, 1), wbuf.at[at, :, :HEAD], w_sem.at[at, 0]))
            act(pltpu.make_async_copy(columns(wk_hbm, h, 1), wbuf.at[at, :, HEAD:], w_sem.at[at, 1]))

    tiles = half // tile

    def wo_copy(m):
        at = jnp.where(m < tiles, other + m * tile, mine + (m - tiles) * tile)
        part = pl.ds(pl.multiple_of(at, 128), tile)
        return pltpu.make_async_copy(wo_hbm.at[:, part], wo.at[:, part], wo_sem.at[m])

    def xres_copy(s):
        b = lax.rem(s, nx)
        return pltpu.make_async_copy(x_hbm.at[rows(s), pl.ds(mine, half)], xres.at[b], xres_sem.at[b])

    def d2d_copy(c, k):
        at = lax.rem(c, 2) * batch + k
        return remote(stage.at[k], d2d.at[at], d2d_send.at[k], d2d_recv.at[at], partner)

    def up_copy(s):
        b, r = lax.rem(s, nb), lax.rem(s, ring)
        return remote(sendb.at[b], up.at[r], send_a.at[b], up_recv.at[r], toward)

    def cross_copy(s):
        b, r = lax.rem(s, nb), lax.rem(s, cring)
        return remote(sendb.at[b], cross.at[r], send_a.at[b], cross_recv.at[r], toward)

    def out_copies(s, act):
        b = lax.rem(s, nb)

        def both(at, which):
            src = at if which else resb.at[b]
            act(remote(src, at, send_b.at[b], res_recv.at[lax.rem(s, ring)], away))
            act(remote(src, at, send_c.at[b], part_recv.at[which], partner))

        finished(s, both)

    def local_copy(s):
        b = lax.rem(s, nb)
        return pltpu.make_async_copy(resb.at[b], early.at[rows(s), pl.ds(mine, half)], send_l.at[b])

    def onward_copy(s, act):
        finished(s, lambda at, which: act(remote(at, at, part_send.at[which], part_recv.at[which], partner)))

    def start(copy):
        copy.start()

    def turn_by(i):
        bc, bs = base_ref[0, pl.ds(i, 1), :], base_ref[1, pl.ds(i, 1), :]
        rotc[...] = bc * fine_ref[0] - bs * fine_ref[1]
        rots[...] = bs * fine_ref[0] + bc * fine_ref[1]

    def ready(i):
        for r in range(ch // GROUP):
            x_copy(i, r).wait()
        turn_by(i)

    def norm(r):
        at = pl.ds(pl.multiple_of(r * GROUP, GROUP), GROUP)
        cols = [slice(c, c + 128) for c in range(0, depth, 128)]
        sums = [None] * 4
        for n, c in enumerate(cols):
            wide = xbuf[at, c].astype(F32)
            sums[n % 4] = wide * wide if sums[n % 4] is None else sums[n % 4] + wide * wide
        total = functools.reduce(jnp.add, [s for s in sums if s is not None])
        scale = lax.rsqrt(jnp.sum(total, -1, keepdims=True) * (1 / depth) + 1e-6)
        scale = jnp.broadcast_to(scale, (GROUP, 128))
        for c in cols:
            abuf[at, c] = (xbuf[at, c].astype(F32) * scale * gain[:, c]).astype(BF16)

    def turned(v):
        v = v.astype(BF16).astype(F32)
        return (v * rotc[...] + pltpu.roll(v, HEAD // 2, 1) * rots[...]).astype(BF16)

    def product(n, k, cuts, between):
        if n is None:
            for do in between:
                do()
            return
        at, total = lax.rem(n, AHEAD + 1), None
        for lo, hi, do in zip(cuts, cuts[1:], between):
            if lo < hi:
                part = _dot(abuf[:, lo:hi], wbuf[at, lo:hi, :], 1, 0)
                total = part if total is None else total + part
            do()
        zbuf[lax.rem(k, 2)] = total

    def cut(parts):
        lead = 1 / 7 if parts > 1 else 1
        ends = [0, lead] + [lead + (1 - lead) * (j + 1) / max(parts - 1, 1) for j in range(parts - 1)]
        return [min(round(f * depth / 256) * 256, depth) for f in ends]

    def attention(n, i, k, blocks):
        h = jnp.where(lax.rem(k, 3) == 2, 2 * lax.div(k, 3), 2 * lax.div(k, 3) - 1)
        here = pl.ds(pl.multiple_of(i * ch, ch), ch)
        wide, last = WIDE * ch, blocks - 1
        state = {}

        def scores(j):
            at = slice((last - j) * wide, (last - j + 1) * wide)
            s = _dot(keys[h, at, :], state["q"], 1, 1)
            if j == 0:
                gap = lax.broadcasted_iota(jnp.int32, (wide, ch), 1) - lax.broadcasted_iota(jnp.int32, (wide, ch), 0)
                s = jnp.where(gap >= last * wide - i * ch, s, HIDDEN)
            state["s", j], state["v", j] = s, vals[h, :, at]

        def lead():
            z = zbuf[lax.rem(k + 1, 2)]
            state["q"] = turned(z[:, :HEAD])
            keys[h, here, :] = turned(z[:, HEAD:])
            scores(0)

        def block(j):
            if j + 1 < blocks:
                scores(j + 1)
            s = state.pop(("s", j))
            top = s.max(axis=0, keepdims=True)
            if j:
                top = jnp.maximum(state["top"], top)
            weights = jnp.exp2((s - top) * e).astype(BF16)
            mix = _dot(state.pop(("v", j)), weights, 1, 0)
            if j:
                mix = state["mix"] * jnp.exp2((state["top"] - top) * e) + mix
            state["top"], state["mix"] = top, mix
            if j == last:
                out = mix[:HEAD] * (1 / mix[HEAD : HEAD + 1])
                seen[:, pl.ds(pl.multiple_of(h * HEAD, HEAD), HEAD)] = out.T.astype(BF16)

        product(n, k, cut(blocks + 1), [lead, *(functools.partial(block, j) for j in range(blocks))])

    def values(n, i, k):
        def post():
            z, here = zbuf[lax.rem(k + 1, 2)], pl.ds(pl.multiple_of(i * ch, ch), ch)
            for m in (1, 0):
                h = jnp.minimum(2 * lax.div(k, 3) + m, heads - 1)
                vals[h, :HEAD, here] = z[:, m * HEAD : (m + 1) * HEAD].astype(BF16).T

        product(n, k, [0, depth], [post])

    def compute(i, k):
        n = i * units + k
        follows = (k > 1) & (lax.rem(k, 3) != 1)

        @pl.when(k < units)
        def _():
            @pl.when((n + AHEAD < nc * units) & ((n + AHEAD < units) | (n >= units)))
            def _():
                for_unit(n + AHEAD, start)

            @pl.when(n == units - AHEAD)
            def _():
                for m in range(2 * tiles):
                    wo_copy(m).start()

            for_unit(n, lambda copy: copy.wait())

            @pl.when(k == 0)
            def _():
                product(n, k, [0, depth], [lambda: None])

            @pl.when(lax.rem(k, 3) == 1)
            def _():
                values(n, i, k)

            for blocks in range(1, pl.cdiv(nc, WIDE) + 1):
                pl.when(follows & (lax.div(i, WIDE) == blocks - 1))(functools.partial(attention, n, i, k, blocks))

        for blocks in range(1, pl.cdiv(nc, WIDE) + 1):
            pl.when((k == units) & (lax.div(i, WIDE) == blocks - 1))(functools.partial(attention, None, i, k, blocks))

        @pl.when(k == units + 1)
        def _():
            @pl.when(i > 0)
            def _():
                for j in range(batch):
                    d2d_copy(i - 1, j).wait_send()

            pl.when((i > 0) & (i + 1 < nc))(lambda: ready(i + 1))

            def theirs(n, wide):
                at = n * wide if isinstance(n, int) else pl.multiple_of(n * wide, wide)
                part = _dot(seen[...], wo[:, pl.ds(pl.multiple_of(other + at, 128), wide)], 1, 0)
                stage[:, :, pl.ds(at, wide)] = part.astype(BF16).reshape(batch, sub, wide)

            @pl.when(i == 0)
            def _():
                def first(n, _):
                    wo_copy(n).wait()
                    theirs(n, tile)

                lax.fori_loop(0, tiles, first, None)

            @pl.when(i > 0)
            def _():
                theirs(0, half)
                for r in range(ch // GROUP):
                    norm(r)

            for j in range(batch):
                d2d_copy(i, j).start()

        @pl.when(k == units + 2)
        def _():
            def ours(n, wide):
                at = n * wide if isinstance(n, int) else pl.multiple_of(n * wide, wide)
                part = _dot(seen[...], wo[:, pl.ds(pl.multiple_of(mine + at, 128), wide)], 1, 0)
                acc[lax.rem(i, 2), :, :, pl.ds(at, wide)] = part.reshape(batch, sub, wide)

            @pl.when(i == 0)
            def _():
                def first(n, _):
                    wo_copy(tiles + n).wait()
                    ours(n, tile)

                lax.fori_loop(0, tiles, first, None)

            pl.when(i > 0)(lambda: ours(0, half))

            @pl.when(i == 0)
            def _():
                for n in range(units, units + AHEAD):
                    for_unit(n, start)

        @pl.when((k == units + 3) & (i == 0))
        def _():
            ready(1)
            lax.fori_loop(0, ch // GROUP, lambda r, _: norm(r), None)

        @pl.when((k == units + 3) & (i + 2 < nc))
        def _():
            for r in range(ch // GROUP):
                x_copy(i + 2, r).start()

    def valid(s):
        return (s >= 0) & (s < pieces)

    def sum_of(s):
        return acc.at[lax.rem(lax.div(s, batch), 2), lax.rem(s, batch)]

    def pair(s):
        at, ours = lax.rem(s, 2 * batch), sum_of(s)
        d2d_copy(lax.div(s, batch), lax.rem(s, batch)).wait_recv()

        @pl.when(inner)
        def _():
            ours[...] = ours[...] + d2d[at].astype(F32)

        @pl.when(jnp.logical_not(inner))
        def _():
            @pl.when(s >= nb)
            def _():
                up_copy(s - nb).wait_send()

            sendb[lax.rem(s, nb)] = (ours[...] + d2d[at].astype(F32)).astype(BF16)
            up_copy(s).start()

    def relay(s):
        up_copy(s).wait_recv()

        @pl.when(s >= nb)
        def _():
            cross_copy(s - nb).wait_send()

        sendb[lax.rem(s, nb)] = (sum_of(s)[...] + up[lax.rem(s, ring)].astype(F32)).astype(BF16)
        cross_copy(s).start()

    def sent(s):
        out_copies(s, lambda copy: copy.wait_send())
        pl.when(s < split)(lambda: local_copy(s).wait())

    def finish(s):
        b = lax.rem(s, nb)
        cross_copy(s).wait_recv()
        xres_copy(s).wait()

        @pl.when(s >= nb)
        def _():
            sent(s - nb)

        total = sendb[b].astype(F32) + cross[lax.rem(s, cring)].astype(F32)
        y = (xres[lax.rem(s, nx)].astype(F32) + total).astype(BF16)

        @pl.when(s < split)
        def _():
            resb[b] = y
            local_copy(s).start()

        @pl.when(s >= split)
        def _():
            y_ref[rows(s), pl.ds(mine, half)] = y

        out_copies(s, start)

    def arrived(s):
        b = lax.rem(s, ring)
        finished(s, lambda at, _: remote(at, at, part_send.at[0], res_recv.at[b], away).wait_recv())
        onward_copy(s, start)

    for r in range(ch // GROUP):
        x_copy(0, r).start()
    for n in range(AHEAD):
        for_unit(n, start)
    barrier = pltpu.get_barrier_semaphore()
    pl.semaphore_signal(barrier, inc=1, device_id=partner, device_id_type=MESH)

    @pl.when(z < zs - 1)
    def _():
        pl.semaphore_signal(barrier, inc=1, device_id=above, device_id_type=MESH)

    @pl.when(z > 0)
    def _():
        pl.semaphore_signal(barrier, inc=1, device_id=below, device_id_type=MESH)

    def clear(h, _):
        keys[h] = jnp.zeros(keys.shape[1:], BF16)
        vals[h, :HEAD, :] = jnp.zeros((HEAD, vals.shape[2]), BF16)
        vals[h, HEAD:, :] = jnp.ones((vals.shape[1] - HEAD, vals.shape[2]), BF16)

    lax.fori_loop(0, heads, clear, None)
    for n in range(depth // 128):
        gain[:, n * 128 : (n + 1) * 128] = gain_ref[n : n + 1, :].astype(F32)
    turn_by(0)
    for r in range(ch // GROUP):
        x_copy(0, r).wait()
        norm(r)
    for r in range(ch // GROUP):
        x_copy(1, r).start()
    pl.semaphore_wait(barrier, 1 + jnp.where(z < zs - 1, 1, 0) + jnp.where(z > 0, 1, 0))

    def served(g, stage, do):
        s = g - lag1 - LAGS[stage]
        pl.when(valid(s))(functools.partial(do, s))

    def serve(g):
        pl.when(jnp.logical_not(inner))(lambda: served(g, 3, arrived))

        @pl.when(inner)
        def _():
            served(g, 2, finish)
            served(g + 2, 2, lambda s: xres_copy(s).start())

        served(g, 0, pair)

    homes = [
        pltpu.make_async_copy(early.at[pl.ds(r * GROUP, GROUP), :], y_ref.at[pl.ds(r * GROUP, GROUP), :], home_sem.at[r])
        for r in range(early.shape[0] // GROUP)
    ]

    def theirs_arrived(which, y):
        at = y.at[:, pl.ds(other, half)]
        remote(at, at, part_send.at[which], part_recv.at[which], partner).wait_recv()

    def slot(g, _):
        i, k = lax.div(g, per), lax.rem(g, per)
        pl.when(lax.rem(g, 2) == 0)(lambda: serve(lax.div(g, 2)))
        pl.when((lax.rem(g, 2) == 1) & inner)(lambda: served(lax.div(g, 2), 1, relay))
        pl.when(i < nc)(lambda: compute(i, k))

        @pl.when(g == max(nc * per, 2 * (split + last_lag)))
        def _():
            theirs_arrived(0, early)
            for copy in homes:
                copy.start()

    lax.fori_loop(0, 2 * (pieces + last_lag), slot, None)

    for j in range(batch):
        d2d_copy(nc - 1, j).wait_send()
    for s in range(pieces - nb, pieces):
        up_copy(s).wait_send()

    @pl.when(inner)
    def _():
        for s in range(pieces - nb, pieces):
            sent(s)

    rest = y_ref.at[early.shape[0] :, :]
    theirs_arrived(1, rest)
    for which, y in enumerate((early, rest)):
        ours = y.at[:, pl.ds(mine, half)]
        pl.when(jnp.logical_not(inner))(remote(ours, ours, part_send.at[which], part_recv.at[which], partner).wait_send)
    for copy in homes:
        copy.wait()


def _placed(y_in, y_out, sem):
    size = y_in.shape[0] // sem.shape[0]
    copies = [pltpu.make_async_copy(y_in.at[pl.ds(r, size), :], y_out.at[pl.ds(r, size), :], sem.at[r // size]) for r in range(0, y_in.shape[0], size)]
    for copy in copies:
        copy.start()
    for copy in copies:
        copy.wait()


def _tables(nc, ch):
    rate = THETA ** (-np.arange(HEAD // 2) / (HEAD // 2))
    sign = np.repeat([-1.0, 1.0], HEAD // 2)

    def both(place):
        angle = np.tile(place[:, None] * rate, (1, 2))
        return np.stack([np.cos(angle), np.sin(angle) * sign]).astype(np.float32)

    return both(np.arange(nc) * ch), both(np.arange(ch))


def solution(mesh, ch=128, tile=1792, copy_rows=128):
    names = mesh.axis_names
    zs = mesh.shape["tp"] // 2

    def step(x, gain, wq, wk, wv, wo):
        n, d = x.shape
        heads = wq.shape[1] // HEAD
        nc, half = n // ch, d // 2
        per = 3 * (heads // 2) + 7
        sub = 2 * ch // per
        base, fine = _tables(nc, ch)
        cfg = dict(ch=ch, sub=sub, per=per, heads=heads, nc=nc, half=half, zs=zs, tile=min(tile, half), names=names)
        wide, batch = min(tile, half), per // 2
        nb, ring, cring, nx = 4, 10, 6, 3
        dma = pltpu.SemaphoreType.DMA
        hbm, vmem = pl.BlockSpec(memory_space=pl.ANY), pl.BlockSpec(memory_space=pltpu.VMEM)
        _, y = pl.pallas_call(
            functools.partial(_kernel, cfg),
            out_shape=[jax.ShapeDtypeStruct((heads * HEAD, d), BF16), pltpu.VMEM((n, d), BF16)],
            in_specs=[hbm, vmem, vmem, vmem, hbm, hbm, hbm, hbm],
            out_specs=[hbm, vmem],
            scratch_shapes=[
                pltpu.VMEM((heads, n, HEAD), BF16),
                pltpu.VMEM((heads, HEAD + 8, n), BF16),
                pltpu.VMEM((AHEAD + 1, d, 2 * HEAD), BF16),
                pltpu.VMEM((2, ch, 2 * HEAD), F32),
                pltpu.VMEM((ch, d), BF16),
                pltpu.VMEM((2, batch, sub, half), F32),
                pltpu.VMEM((batch, sub, half), BF16),
                pltpu.VMEM((ch, heads * HEAD), BF16),
                pltpu.VMEM((2 * batch, sub, half), BF16),
                pltpu.VMEM((ring, sub, half), BF16),
                pltpu.VMEM((cring, sub, half), BF16),
                pltpu.VMEM((nb, sub, half), BF16),
                pltpu.VMEM((nb, sub, half), BF16),
                pltpu.VMEM((nx, sub, half), BF16),
                pltpu.VMEM((ch, HEAD), F32),
                pltpu.VMEM((ch, HEAD), F32),
                pltpu.VMEM((1, d), F32),
                dma((AHEAD + 1, 2)), dma((2 * half // wide,)), dma((ch // GROUP,)), dma((nx,)),
                dma((batch,)), dma((2 * batch,)), dma((ring,)), dma((cring,)), dma((ring,)),
                dma((nb,)), dma((nb,)), dma((nb,)), dma((nb,)), dma((2,)), dma((2,)),
                dma((heads * HEAD // GROUP,)),
            ],
            compiler_params=pltpu.CompilerParams(collective_id=0, has_side_effects=True, vmem_limit_bytes=KERNEL_VMEM),
            name="attention_half",
        )(x, gain.reshape(d // 128, 128), jnp.asarray(base), jnp.asarray(fine), wq, wk, wv, wo)
        return pl.pallas_call(
            _placed,
            out_shape=jax.ShapeDtypeStruct((n, d), BF16),
            in_specs=[vmem],
            out_specs=hbm,
            scratch_shapes=[dma((n // copy_rows,))],
            compiler_params=pltpu.CompilerParams(vmem_limit_bytes=2**20),
            name="placed",
        )(pltpu.with_memory_space_constraint(y, pltpu.VMEM))

    tokens, columns = P("dp", None), P(None, "tp")
    return jax.shard_map(
        step,
        mesh=mesh,
        in_specs=(tokens, P(None), columns, columns, columns, P("tp", None)),
        out_specs=tokens,
        check_vma=False,
    )
```
